256 devices in a mesh: gx: 8 (over z), gy: 8 (over y, core), gz: 4 (over x).
Axes of the slice: x: 4, y: 4, z: 8, core: 2. Of those that a mesh axis runs over, the one named last changes fastest.
Arguments:
- iterate: float32 [64, 128, 512], P('gx', 'gy', 'gz'), may hold values from -6 to 6
- source: float32 [64, 128, 512], P('gx', 'gy', 'gz'), may hold values from -6 to 6
- reaction: float32 [64, 128, 512], P('gx', 'gy', 'gz'), may hold values from 0.05 to 1
- trial_powers: int32 [4], replicated, may hold values from 0 to 5
Outputs:
- newton_dir: float32 [64, 128, 512], P('gx', 'gy', 'gz')
- remnant: float32 [64, 128, 512], P('gx', 'gy', 'gz')
- layer_energies: float32 [4, 64], P(None, 'gx')
- energies: float32 [4], replicated
The draws below stay inside these ranges and needn't reach their ends.
Inputs may be any that keep to these rules, and one draw needn't show every extreme that they name: `trial_powers`: trial k takes the step length 2 to the power minus entry k.
All inputs are finite; a program needn't handle non-finite values.
Results may differ from the reference program's by a relative error of at most 0.0003.
Values sent between devices are 32-bit elements; how exact they have to be, the bound alone decides.
No kernel may reach another device: no remote copies, remote signals or barrier semaphores. Data moves between devices by JAX's collectives and lax.ppermute only.
A program may use at most 128 MiB of HBM per device.

```python
import math
import jax
import jax.numpy as jnp
from jax import lax

ITERS = 4
LEVELS = 4
TRIALS = 4
NX = 64
NY = 128
NZ = 512


def place_ends(array, rng, smallest, high):
    longest = array.shape.index(max(array.shape))
    spots = []
    for shift in (0, 1):
        where = [jax.random.randint(jax.random.fold_in(rng, axis), (), 0, length) for axis, length in enumerate(array.shape)]
        where[longest] = (where[longest] + shift) % array.shape[longest]
        spots.append(tuple(where))
    return array.at[spots[0]].set(smallest).at[spots[1]].set(high)


def level_of(key, extent, split, smallest, largest):
    def one(axis_at, shards_of):
        draws = jax.random.uniform(jax.random.fold_in(jax.random.fold_in(key, 6), axis_at), (shards_of,), jnp.float32, smallest / len(split), largest / len(split))
        return jnp.repeat(jnp.exp(draws), extent[axis_at] // shards_of).reshape((-1,) + (1,) * (len(extent) - axis_at - 1))

    loudness = one(*split[0])
    for cut in split[1:]:
        loudness = loudness * one(*cut)
    return loudness


def noise(rng, shape, spread, limit, split=(), kind=jnp.bfloat16):
    loudness = level_of(rng, shape, split, -0.22, 0.18) if split else 1.0
    entries = jax.random.normal(rng, shape, jnp.float32) * spread * loudness
    return jnp.minimum(jnp.maximum(entries, -limit), limit).astype(kind)


def setup_inputs(seed: int = 0) -> dict:
    key_list = jax.random.split(jax.random.key(seed), 5)
    return {
        "iterate": noise(key_list[0], (NX, NY, NZ), 1.0, 6.0, ((0, 8), (1, 8), (2, 4)), jnp.float32),
        "source": noise(key_list[1], (NX, NY, NZ), 1.0, 6.0, ((0, 8), (1, 8), (2, 4)), jnp.float32),
        "reaction": jnp.clip(jnp.exp(math.log(1.0) - 2.9957323 * jax.random.uniform(key_list[2], (NX, NY, NZ), jnp.float32) ** level_of(key_list[2], (NX, NY, NZ), ((0, 8), (1, 8), (2, 4)), -0.2, 0.2)), 0.05, 1.0),
        "trial_powers": place_ends(jax.random.randint(key_list[3], (TRIALS,), 0, 6), jax.random.fold_in(key_list[3], 1), 0, 5).astype(jnp.int32),
    }


cheb_mid = 1.15
cheb_half = 0.85

def differences(padded):
    along_x = padded[1:, 1:-1, 1:-1] - padded[:-1, 1:-1, 1:-1]
    along_y = padded[1:-1, 1:, 1:-1] - padded[1:-1, :-1, 1:-1]
    along_z = padded[1:-1, 1:-1, 1:] - padded[1:-1, 1:-1, :-1]
    return (along_x, along_y, along_z)

def stiffness(gradient):
    square = gradient * gradient
    return (1.0 + 2.0 * square) / jnp.sqrt(1.0 + square)

def fluxes(gradient):
    return gradient * jnp.sqrt(1.0 + gradient * gradient)

def face_energy(gradient):
    square = 1.0 + gradient * gradient
    return (square * jnp.sqrt(square) - 1.0) / 3.0

def divergence(face_flows):
    return face_flows[0][1:] - face_flows[0][:-1] + (face_flows[1][:, 1:] - face_flows[1][:, :-1]) + (face_flows[2][:, :, 1:] - face_flows[2][:, :, :-1])

def apply_operator(padded, weights, reaction):
    centre = padded[1:-1, 1:-1, 1:-1]
    gradient = differences(padded)
    face_flows = tuple((w * s for w, s in zip(weights, gradient)))
    return reaction * centre - divergence(face_flows)

def diagonal_of(weights, reaction):
    weight_x, weight_y, weight_z = weights
    return reaction + weight_x[1:] + weight_x[:-1] + weight_y[:, 1:] + weight_y[:, :-1] + weight_z[:, :, 1:] + weight_z[:, :, :-1]

def smooth(remnant, inverse, degree, operate):
    cheb_sigma = cheb_mid / cheb_half
    cheb_rho = 1.0 / cheb_sigma
    update = inverse * remnant / cheb_mid
    summed = update
    for sweep_idx in range(1, degree):
        remnant = remnant - operate(update)
        cheb_next = 1.0 / (2.0 * cheb_sigma - cheb_rho)
        update = cheb_next * cheb_rho * update + 2.0 * cheb_next / cheb_half * inverse * remnant
        summed = summed + update
        cheb_rho = cheb_next
    return (summed, remnant, update)

def pair_sum(values, axis_pos):
    old_shape = values.shape
    new_shape = old_shape[:axis_pos] + (old_shape[axis_pos] // 2, 2) + old_shape[axis_pos + 1:]
    return lax.optimization_barrier(jnp.sum(values.reshape(new_shape), axis=axis_pos + 1))

def restrict(values):
    return pair_sum(pair_sum(pair_sum(values, 0), 1), 2)

def prolong(values):
    return jnp.repeat(jnp.repeat(jnp.repeat(values, 2, 0), 2, 1), 2, 2)

def coarsen(weights, reaction):
    weight_x, weight_y, weight_z = weights
    coarse_x = pair_sum(pair_sum(weight_x[::2], 1), 2)
    coarse_y = pair_sum(pair_sum(weight_y[:, ::2], 0), 2)
    coarse_z = pair_sum(pair_sum(weight_z[:, :, ::2], 0), 1)
    return ((coarse_x, coarse_y, coarse_z), restrict(reaction))

def build_levels(weights, reaction):
    levels = [(weights, reaction, 1.0 / diagonal_of(weights, reaction))]
    for level_idx in range(1, LEVELS):
        weights, reaction = coarsen(weights, reaction)
        levels.append((weights, reaction, 1.0 / diagonal_of(weights, reaction)))
    return levels

def vcycle(levels, level_depth, remnant):
    weights, reaction, inverse = levels[level_depth]

    def operate(values):
        return apply_operator(jnp.pad(values, 1), weights, reaction)
    if level_depth == len(levels) - 1:
        summed, _, _ = smooth(remnant, inverse, 3, operate)
        return summed
    summed, remnant, update = smooth(remnant, inverse, 2, operate)
    remnant = remnant - operate(update)
    correction = prolong(vcycle(levels, level_depth + 1, restrict(remnant)))
    summed = summed + correction
    remnant = remnant - operate(correction)
    smoothed, _, _ = smooth(remnant, inverse, 2, operate)
    return summed + smoothed

def reference(iterate, source, reaction, trial_powers):
    gradient = differences(jnp.pad(iterate, 1))
    weights = tuple((stiffness(s) for s in gradient))
    remnant = source - reaction * iterate + divergence(tuple((fluxes(s) for s in gradient)))
    levels = build_levels(weights, reaction)
    newton_dir = jnp.zeros_like(iterate)
    precond_out = vcycle(levels, 0, remnant)
    direction = precond_out
    precond_norm = jnp.sum(remnant * precond_out)
    for iter_idx in range(ITERS):
        image_dir = apply_operator(jnp.pad(direction, 1), weights, reaction)
        step_length = precond_norm / jnp.sum(direction * image_dir)
        newton_dir = newton_dir + step_length * direction
        remnant = remnant - step_length * image_dir
        if iter_idx + 1 < ITERS:
            precond_out = vcycle(levels, 0, remnant)
            norm_next = jnp.sum(remnant * precond_out)
            direction = precond_out + norm_next / precond_norm * direction
            precond_norm = norm_next
    layer_cells = NY * NZ
    layers = []
    for trial_idx in range(TRIALS):
        step_scale = jnp.exp2(-trial_powers[trial_idx].astype(jnp.float32))
        trial_field = iterate + step_scale * newton_dir
        trial_slopes = differences(jnp.pad(trial_field, 1))
        energy_x = face_energy(trial_slopes[0])
        layer_sum = lax.optimization_barrier(jnp.sum(energy_x[:-1], axis=(1, 2)))
        layer_sum = layer_sum.at[-1].add(jnp.sum(energy_x[-1]))
        layer_sum = layer_sum + lax.optimization_barrier(jnp.sum(face_energy(trial_slopes[1]), axis=(1, 2))) + lax.optimization_barrier(jnp.sum(face_energy(trial_slopes[2]), axis=(1, 2)))
        layer_sum = layer_sum + lax.optimization_barrier(jnp.sum(0.5 * reaction * trial_field * trial_field - source * trial_field, axis=(1, 2)))
        layers.append(layer_sum / layer_cells)
    layer_energies = jnp.stack(layers)
    energies = lax.optimization_barrier(jnp.sum(layer_energies, axis=1)) / NX
    return (newton_dir, remnant, layer_energies, energies)
```

```python
import jax
import jax.numpy as jnp
from jax import lax
from jax.experimental import pallas as pl
from jax.experimental.pallas import tpu as pltpu
from jax.sharding import Mesh
from jax.sharding import PartitionSpec as P

ITERS = 4
TRIALS = 4
ALL = ("gx", "gy_0", "gy_1", "gz")
GY = ("gy_0", "gy_1")
NGX, NGY, NGZ = 8, 8, 4
NDEV = 256
NZB = 32
NX, NY, NZ = 64, 128, 512
M = 12
B = 16
NB = 40
F32 = jnp.float32
INTERPRET = False

THETA = 1.15
DELTA = 0.85
SIGMA = THETA / DELTA
RHO0 = 1.0 / SIGMA
RHO1 = 1.0 / (2.0 * SIGMA - RHO0)
RHO2 = 1.0 / (2.0 * SIGMA - RHO1)
C1U = RHO1 * RHO0
C1R = 2.0 * RHO1 / DELTA
C2U = RHO2 * RHO1
C2R = 2.0 * RHO2 / DELTA


def roll(v, shift, axis):
    return pltpu.roll(v, shift % v.shape[axis], axis)


def up_z(v, s=1):
    return roll(v, -s, 0)


def dn_z(v, s=1):
    return roll(v, s, 0)


def up_x(v, s=1):
    return roll(v, -s, 1)


def dn_x(v, s=1):
    return roll(v, s, 1)


def ziota():
    return lax.broadcasted_iota(jnp.int32, (NB, 128), 0)


def xiota():
    return lax.broadcasted_iota(jnp.int32, (NB, 128), 1)


def even(iota, s):
    return (iota // s) % 2 == 0


def sum_z(v, s):
    return v + jnp.where(even(ziota(), s), up_z(v, s), dn_z(v, s))


def sum_x(v, s):
    return v + jnp.where(even(xiota(), s), up_x(v, s), dn_x(v, s))


def odd_z(v, s):
    return jnp.where(even(ziota(), s), up_z(v, s), v)


def odd_x(v, s):
    return jnp.where(even(xiota(), s), up_x(v, s), v)


class Level:
    def __init__(self, wx, wy, wz, c, dinv, s):
        self.wx, self.wy, self.wz, self.c, self.dinv, self.s = wx, wy, wz, c, dinv, s

    def y_flux(self, y, low, high):
        return self.wy[y] * (high - low)

    def apply(self, y, u, high, flux_low):
        s = self.s
        flux_y = self.wy[y] * (high - u)
        flux_x = self.wx[y] * (up_x(u, s) - u)
        flux_z = self.wz[y] * (up_z(u, s) - u)
        image = self.c[y] * u - ((flux_x - dn_x(flux_x, s)) + (flux_y - flux_low) + (flux_z - dn_z(flux_z, s)))
        return image, flux_y


def sweep(level, lo, hi, field, store):
    first = field(lo)
    flux = level.y_flux(lo - 1, field(lo - 1), first)

    def row(y, carry):
        u, flux_low = carry
        high = field(y + 1)
        image, flux_y = level.apply(y, u, high, flux_low)
        store(y, u, image)
        return high, flux_y

    lax.fori_loop(lo, hi, row, (first, flux))


def smooth_down(level, lo, hi, r, r1, u1, x, finish):
    def start(y):
        return level.dinv[y] * r[y] / THETA

    def first(y, u, image):
        rest = r[y] - image
        r1[y] = rest
        after = C1U * u + C1R * (level.dinv[y] * rest)
        u1[y] = after
        x[y] = u + after

    sweep(level, lo, hi, start, first)
    sweep(level, lo + 1, hi - 1, lambda y: u1[y], lambda y, u, image: finish(y, r1[y] - image))


def smooth_up(level, lo, hi, e, r2, r3, u, x, finish):
    def first(y, own, image):
        rest = r2[y] - image
        r3[y] = rest
        u[y] = level.dinv[y] * rest / THETA

    sweep(level, lo, hi, e, first)

    def second(y, own, image):
        rest = r3[y] - image
        after = C1U * own + C1R * (level.dinv[y] * rest)
        finish(y, (x[y] + e(y)) + (own + after))

    sweep(level, lo + 1, hi - 1, lambda y: u[y], second)


def down(fine, mid, r, r1, u1, x, r2, b1, r1m, u1m, xm, r2m, b2):
    def keep(y, rest):
        r2[y] = rest

    smooth_down(fine, 3, 37, r, r1, u1, x, keep)

    def restrict(y, carry):
        b1[y] = sum_x(sum_z(r2[2 * y] + r2[2 * y + 1], 1), 1)
        return carry

    lax.fori_loop(2, 18, restrict, 0)

    def keep_mid(y, rest):
        r2m[y] = rest

    smooth_down(mid, 3, 17, b1, r1m, u1m, xm, keep_mid)
    for k in range(4):
        b2[k] = sum_x(sum_z(r2m[2 * k + 6] + r2m[2 * k + 7], 2), 2)


def setup_kernel(pos, it, src, rea, wx, wy, wz, c, dinv, wx1, wy1, wz1, c1, dinv1, r, x, r2, xm, r2m, pay, r1, u1, b1, r1m, u1m):
    gy, zb = pos[0], pos[1]
    zg = ziota() + (zb * B - M)
    lane = xiota()
    inside_zx = (zg >= 0) & (zg < NZ) & (lane < NX)

    def weight(g):
        square = g * g
        root = jnp.sqrt(1.0 + square)
        return (1.0 + 2.0 * square) / root, g * root

    def row(y, carry):
        flow_low, wy_low, wym_low = carry
        yg = gy * B - M + y
        here, high = it[y], it[y + 1]
        w_x, p_x = weight(up_x(here) - here)
        w_y, p_y = weight(high - here)
        w_z, p_z = weight(up_z(here) - here)
        inside = inside_zx & (yg >= 0) & (yg < NY)
        rest = src[y] - rea[y] * here + ((p_x - dn_x(p_x)) + (p_y - flow_low) + (p_z - dn_z(p_z)))
        r[y] = jnp.where(inside, rest, 0.0)
        outer = rea[y] + jnp.where(lane == 0, dn_x(w_x), 0.0) + jnp.where(lane == NX - 1, w_x, 0.0)
        outer = outer + jnp.where(zg == 0, dn_z(w_z), 0.0) + jnp.where(zg == NZ - 1, w_z, 0.0)
        outer = outer + jnp.where(yg == 0, wy_low, 0.0) + jnp.where(yg == NY - 1, w_y, 0.0)
        outer = jnp.where(inside, outer, 0.0)
        m_x = jnp.where(inside & (lane < NX - 1), w_x, 0.0)
        m_y = jnp.where(inside & (yg < NY - 1), w_y, 0.0)
        m_z = jnp.where(inside & (zg < NZ - 1), w_z, 0.0)
        wx[y], wy[y], wz[y], c[y] = m_x, m_y, m_z, outer
        diagonal = outer + m_x + dn_x(m_x) + m_y + wym_low + m_z + dn_z(m_z)
        good = diagonal > 0.0
        dinv[y] = jnp.where(good, 1.0 / jnp.where(good, diagonal, 1.0), 0.0)
        return p_y, w_y, m_y

    zero = jnp.zeros((NB, 128), F32)
    lax.fori_loop(0, NB - 1, row, (zero, zero, zero))
    for ref in (wx, wy, wz, c, dinv, r):
        ref[NB - 1] = zero

    def row1(y, low):
        a, b = 2 * y, 2 * y + 1
        m_x = sum_z(odd_x(wx[a] + wx[b], 1), 1)
        m_y = sum_x(sum_z(wy[b], 1), 1)
        m_z = sum_x(odd_z(wz[a] + wz[b], 1), 1)
        m_c = sum_x(sum_z(c[a] + c[b], 1), 1)
        wx1[y], wy1[y], wz1[y], c1[y] = m_x, m_y, m_z, m_c
        diagonal = m_c + m_x + dn_x(m_x, 2) + m_y + low + m_z + dn_z(m_z, 2)
        good = diagonal > 0.0
        dinv1[y] = jnp.where(good, 1.0 / jnp.where(good, diagonal, 1.0), 0.0)
        return m_y

    lax.fori_loop(0, NB // 2, row1, zero)
    fine = Level(wx, wy, wz, c, dinv, 1)
    mid = Level(wx1, wy1, wz1, c1, dinv1, 2)

    class Part:
        def __setitem__(self, k, value):
            pay[k] = value

    down(fine, mid, r, r1, u1, x, r2, b1, r1m, u1m, xm, r2m, Part())
    for k in range(4):
        a, b = 2 * k + 6, 2 * k + 7
        pay[4 + k] = sum_z(odd_x(wx1[a] + wx1[b], 2), 2)
        pay[8 + k] = sum_x(sum_z(wy1[b], 2), 2)
        pay[12 + k] = sum_x(odd_z(wz1[a] + wz1[b], 2), 2)
        pay[16 + k] = sum_x(sum_z(c1[a] + c1[b], 2), 2)


def lane_ids():
    return lax.broadcasted_iota(jnp.int32, (16, NDEV), 1)


def next_z(v):
    return jnp.where(lane_ids() < 224, roll(v, -32, 1), roll(v, 223, 1))


def prev_z(v):
    lanes = lane_ids()
    return jnp.where(lanes >= 32, roll(v, 32, 1), jnp.where(lanes == 0, 0.0, roll(v, -223, 1)))


def next_y(v):
    return roll(v, -4, 1)


def prev_y(v):
    return roll(v, 4, 1)


def coarse_apply(n, s, u, wx, wy, wz, c):
    flux_y = [[None] * n for _ in range(n)]
    flux_z = [[None] * n for _ in range(n)]
    for y in range(n):
        for z in range(n):
            here = u[y][z]
            high_y = u[y + 1][z] if y + 1 < n else next_y(u[0][z])
            high_z = u[y][z + 1] if z + 1 < n else next_z(u[y][0])
            flux_y[y][z] = wy(y, z) * (high_y - here)
            flux_z[y][z] = wz(y, z) * (high_z - here)
    image = [[None] * n for _ in range(n)]
    for y in range(n):
        for z in range(n):
            here = u[y][z]
            flux_x = wx(y, z) * (roll(here, -s, 0) - here)
            low_y = flux_y[y - 1][z] if y else prev_y(flux_y[n - 1][z])
            low_z = flux_z[y][z - 1] if z else prev_z(flux_z[y][n - 1])
            image[y][z] = c(y, z) * here - (
                (flux_x - roll(flux_x, s, 0)) + (flux_y[y][z] - low_y) + (flux_z[y][z] - low_z)
            )
    return image


def planes(n, f):
    return [[f(y, z) for z in range(n)] for y in range(n)]


def pair_x(v):
    iota = lax.broadcasted_iota(jnp.int32, (16, NDEV), 0)
    return v + jnp.where(even(iota, 1), roll(v, -1, 0), roll(v, 1, 0))


def odd_pair_x(v):
    iota = lax.broadcasted_iota(jnp.int32, (16, NDEV), 0)
    return jnp.where(even(iota, 1), roll(v, -1, 0), v)


def inverse_diagonal(n, s, wx, wy, wz, c):
    def one(y, z):
        low_y = wy(y - 1, z) if y else prev_y(wy(n - 1, z))
        low_z = wz(y, z - 1) if z else prev_z(wz(y, n - 1))
        diagonal = c(y, z) + wx(y, z) + roll(wx(y, z), s, 0) + wy(y, z) + low_y + wz(y, z) + low_z
        return 1.0 / diagonal

    return planes(n, one)


def coefficients_kernel(got, k2, k3):
    for f in range(4):
        k2[f] = got[f].T

    def field(f):
        return lambda y, z: k2[f, pl.ds((y * 4 + z) * 16, 16), :]

    wx, wy, wz, c = (field(f) for f in range(4))
    inverse = inverse_diagonal(4, 1, wx, wy, wz, c)
    for y in range(4):
        for z in range(4):
            k2[4, pl.ds((y * 4 + z) * 16, 16), :] = inverse[y][z]
    for y in range(2):
        for z in range(2):
            a, b, e, f = (2 * y, 2 * z), (2 * y, 2 * z + 1), (2 * y + 1, 2 * z), (2 * y + 1, 2 * z + 1)
            at = pl.ds((y * 2 + z) * 16, 16)
            k3[0, at, :] = odd_pair_x((wx(*a) + wx(*b)) + (wx(*e) + wx(*f)))
            k3[1, at, :] = pair_x(wy(*e) + wy(*f))
            k3[2, at, :] = pair_x(wz(*b) + wz(*f))
            k3[3, at, :] = pair_x((c(*a) + c(*b)) + (c(*e) + c(*f)))

    def field3(f):
        return lambda y, z: k3[f, pl.ds((y * 2 + z) * 16, 16), :]

    inverse = inverse_diagonal(2, 2, *(field3(f) for f in range(4)))
    for y in range(2):
        for z in range(2):
            k3[4, pl.ds((y * 2 + z) * 16, 16), :] = inverse[y][z]


def combine(n, f, *lists):
    return planes(n, lambda y, z: f(*(a[y][z] for a in lists)))


def coarse_solve(got, k2, k3, b2t):
    b2t[...] = got.T

    def field(ref, n, f):
        return lambda y, z: ref[f, pl.ds((y * n + z) * 16, 16), :]

    a2 = tuple(field(k2, 4, f) for f in range(4))
    dinv = planes(4, field(k2, 4, 4))
    a3 = tuple(field(k3, 2, f) for f in range(4))
    dinv3 = planes(2, field(k3, 2, 4))
    r = planes(4, lambda y, z: b2t[pl.ds((y * 4 + z) * 16, 16), :])
    u = combine(4, lambda d, b: d * b / THETA, dinv, r)
    r = combine(4, lambda a, b: a - b, r, coarse_apply(4, 1, u, *a2))
    u1 = combine(4, lambda u, d, r: C1U * u + C1R * (d * r), u, dinv, r)
    x = combine(4, lambda a, b: a + b, u, u1)
    r = combine(4, lambda a, b: a - b, r, coarse_apply(4, 1, u1, *a2))
    r3 = planes(
        2,
        lambda y, z: pair_x(
            (r[2 * y][2 * z] + r[2 * y][2 * z + 1]) + (r[2 * y + 1][2 * z] + r[2 * y + 1][2 * z + 1])
        ),
    )
    u = combine(2, lambda d, b: d * b / THETA, dinv3, r3)
    x3 = u
    for cu, cr in ((C1U, C1R), (C2U, C2R)):
        r3 = combine(2, lambda a, b: a - b, r3, coarse_apply(2, 2, u, *a3))
        u = combine(2, lambda u, d, r: cu * u + cr * (d * r), u, dinv3, r3)
        x3 = combine(2, lambda a, b: a + b, x3, u)
    e = planes(4, lambda y, z: x3[y // 2][z // 2])
    x = combine(4, lambda a, b: a + b, x, e)
    r = combine(4, lambda a, b: a - b, r, coarse_apply(4, 1, e, *a2))
    u = combine(4, lambda d, b: d * b / THETA, dinv, r)
    r = combine(4, lambda a, b: a - b, r, coarse_apply(4, 1, u, *a2))
    u1 = combine(4, lambda u, d, r: C1U * u + C1R * (d * r), u, dinv, r)
    return combine(4, lambda x, a, b: x + (a + b), x, u, u1)


def place_coarse(pos, x2, e2):
    gy, zb = pos[0], pos[1]
    lanes = lane_ids()
    picked = {}
    for dy in (-1, 0, 1):
        for dz in (-1, 0, 1):
            at_y = jnp.clip(gy + dy, 0, NGY - 1)
            at_z = jnp.clip(zb + dz, 0, NZB - 1)
            picked[dy, dz] = lanes == ((at_z % NGX) * NGY + at_y) * NGZ + at_z // NGX
    spread = lax.broadcasted_iota(jnp.int32, (16, 128), 1) // 4 == lax.broadcasted_iota(jnp.int32, (16, 128), 0)
    rows = ziota() // 4
    for y2 in range(1, 9):
        dy, y = (y2 - 3) // 4, (y2 - 3) % 4
        plane = jnp.zeros((NB, 128), F32)
        for z2 in range(1, 9):
            dz, z = (z2 - 3) // 4, (z2 - 3) % 4
            column = jnp.sum(jnp.where(picked[dy, dz], x2[y][z], 0.0), axis=1, keepdims=True)
            line = jnp.sum(jnp.where(spread, column, 0.0), axis=0, keepdims=True)
            plane = jnp.where(rows == z2, line, plane)
        e2[y2] = plane


def up_kernel(pos, got, k2, k3, wx, wy, wz, c, dinv, wx1, wy1, wz1, c1, dinv1, x, r2, xm, r2m, out, b2t, e2, r3m, um, x1, r3, u):
    place_coarse(pos, coarse_solve(got[...], k2, k3, b2t), e2)
    fine = Level(wx, wy, wz, c, dinv, 1)
    mid = Level(wx1, wy1, wz1, c1, dinv1, 2)

    def keep(y, value):
        x1[y] = value

    smooth_up(mid, 4, 16, lambda y: e2[y // 2], r2m, r3m, um, xm, keep)

    def result(y, value):
        out[y - M] = dn_z(value, -M)[:B]

    smooth_up(fine, 11, 29, lambda y: x1[y // 2], r2, r3, u, x, result)


def image_kernel(z, r, wx, wy, wz, c, w, dots):
    fine = Level(wx, wy, wz, c, None, 1)

    def keep(y, u, image):
        w[y] = image

    sweep(fine, 2, 38, lambda y: z[y], keep)
    own = (ziota() >= M) & (ziota() < M + B)

    def row(y, carry):
        a, b = carry
        here = jnp.where(own, z[y], 0.0)
        return a + r[y] * here, b + here * w[y]

    zero = jnp.zeros((NB, 128), F32)
    a, b = lax.fori_loop(M, M + B, row, (zero, zero))
    lane = lax.broadcasted_iota(jnp.int32, (8, 128), 1)
    dots[...] = jnp.where(lane == 0, jnp.sum(a), jnp.where(lane == 1, jnp.sum(b), 0.0))


def step_sizes(got, old, scal, first):
    total = jnp.sum(got[...], axis=0, keepdims=True)
    lane = lax.broadcasted_iota(jnp.int32, (1, 128), 1)

    def pick(v, k):
        return jnp.sum(jnp.where(lane == k, v, 0.0))

    one = jnp.ones((1, 128), F32)
    gamma, delta = pick(total, 0) * one, pick(total, 1) * one
    if first:
        beta = jnp.zeros((1, 128), F32)
        alpha = gamma / delta
    else:
        was = old[0:1]
        gamma_old, alpha_old = pick(was, 0) * one, pick(was, 1) * one
        beta = gamma / gamma_old
        alpha = gamma / (delta - beta * gamma / alpha_old)
    if scal is not None:
        scal[...] = jnp.broadcast_to(jnp.where(lane == 0, gamma, alpha), (8, 128))
    return alpha, beta


def update_kernel(first, got, old, z, w, r, q, p, d, wx, wy, wz, c, dinv, wx1, wy1, wz1, c1, dinv1,
                  scal, r_o, q_o, p_o, d_o, x, r2, xm, r2m, pay, r1, u1, b1, r1m, u1m):
    alpha, beta = step_sizes(got, old, scal, first)

    def row(y, carry):
        q_y = w[y] if first else w[y] + beta * q[y]
        q_o[y] = q_y
        r_o[y] = r[y] - alpha * q_y
        return carry

    lax.fori_loop(2, 38, row, 0)

    def row_d(y, carry):
        p_y = z[y] if first else z[y] + beta * p[y]
        p_o[y] = p_y
        d_o[y] = alpha * p_y if first else d[y] + alpha * p_y
        return carry

    lax.fori_loop(M - 1, M + B + 1, row_d, 0)
    fine = Level(wx, wy, wz, c, dinv, 1)
    mid = Level(wx1, wy1, wz1, c1, dinv1, 2)
    down(fine, mid, r_o, r1, u1, x, r2, b1, r1m, u1m, xm, r2m, pay)


def finish_kernel(pos, steps, got, old, z, w, r, q, p, d, it, src, rea, d_out, r_out, layers, d_all):
    alpha, beta = step_sizes(got, old, None, False)
    gy, zb = pos[0], pos[1]

    def row_d(y, carry):
        d_all[y] = d[y] + alpha * (z[y] + beta * p[y])
        return carry

    lax.fori_loop(M - 1, M + B + 1, row_d, 0)

    def row(y, carry):
        r_out[y - M] = dn_z(r[y] - alpha * (w[y] + beta * q[y]), -M)[:B]
        d_out[y - M] = dn_z(d_all[y], -M)[:B]
        return carry

    lax.fori_loop(M, M + B, row, 0)
    zi = ziota()
    own = (zi >= M) & (zi < M + B)
    own_z = own | ((zi == M + B) & (zb == NZB - 1))
    lane = lax.broadcasted_iota(jnp.int32, (1, 128), 1)

    def energy(g):
        square = 1.0 + g * g
        return (square * jnp.sqrt(square) - 1.0) / 3.0

    zero = jnp.zeros((NB, 128), F32)
    for k in range(TRIALS):
        step = steps[k]

        def trial(y):
            return it[y] + step * d_all[y]

        def row(y, carry):
            low, acc_x, acc = carry
            v = trial(y)
            acc_x = acc_x + jnp.where(own, energy(v - dn_x(v)), 0.0)
            part = energy(v - low) + (0.5 * rea[y] * v * v - src[y] * v)
            acc = acc + jnp.where(own, part, 0.0) + jnp.where(own_z, energy(v - dn_z(v)), 0.0)
            return v, acc_x, acc

        v, acc_x, acc = lax.fori_loop(M, M + B, row, (trial(M - 1), zero, zero))
        last = own & (gy == NGY - 1)
        acc = acc + jnp.where(last, energy(trial(M + B) - v), 0.0)
        sum_of_x = jnp.sum(acc_x, axis=0, keepdims=True)
        top = jnp.where(lane == NX - 1, jnp.broadcast_to(roll(jnp.broadcast_to(sum_of_x, (8, 128)), -1, 1)[0:1], (1, 128)), 0.0)
        layers[k] = jnp.broadcast_to(sum_of_x + top + jnp.sum(acc, axis=0, keepdims=True), (8, 128))


VM = pl.BlockSpec(memory_space=pltpu.VMEM)
SM = pl.BlockSpec(memory_space=pltpu.SMEM)


def call(kernel, n_scalar, outs, scratch, name):
    def run(*args):
        return pl.pallas_call(
            kernel,
            in_specs=[SM] * n_scalar + [VM] * (len(args) - n_scalar),
            out_specs=[VM] * len(outs),
            out_shape=[jax.ShapeDtypeStruct(s, F32) for s in outs],
            scratch_shapes=[pltpu.VMEM(s, F32) for s in scratch],
            interpret=INTERPRET,
            name=name,
        )(*args)

    return run


FINE = (NB, NB, 128)
MID = (NB // 2, NB, 128)
DOWN_SCRATCH = [FINE, FINE, MID, MID, MID]


def shift_pairs(dy, dz):
    pairs = []
    for gy in range(NGY):
        for zb in range(NZB):
            ty, tz = gy + dy, zb + dz
            if 0 <= ty < NGY and 0 <= tz < NZB:
                source = ((zb % NGX) * NGY + gy) * NGZ + zb // NGX
                target = ((tz % NGX) * NGY + ty) * NGZ + tz // NGX
                pairs.append((source, target))
    return pairs


def exchange(own):
    ax = own.ndim - 2
    low = lax.ppermute(lax.slice_in_dim(own, B - M, B, axis=ax), ALL, shift_pairs(0, 1))
    high = lax.ppermute(lax.slice_in_dim(own, 0, M, axis=ax), ALL, shift_pairs(0, -1))
    own = jnp.concatenate([low, own, high], axis=ax)
    ax = own.ndim - 3
    low = lax.ppermute(lax.slice_in_dim(own, B - M, B, axis=ax), ALL, shift_pairs(1, 0))
    high = lax.ppermute(lax.slice_in_dim(own, 0, M, axis=ax), ALL, shift_pairs(-1, 0))
    return jnp.concatenate([low, own, high], axis=ax)


def to_everyone(x):
    copies = jnp.broadcast_to(x, (NDEV, *x.shape))
    return lax.all_to_all(copies, ALL, split_axis=0, concat_axis=0, tiled=True)


def compact(pay):
    kept = pay[:, M : M + B : 4, 0:NX:4]
    return kept.reshape(-1, 256)


def on_device(iterate, source, reaction, trial_powers):
    gx = lax.axis_index("gx")
    gy = lax.axis_index(GY)
    zb = lax.axis_index("gz") * NGX + gx
    pos = jnp.stack([gy, zb]).astype(jnp.int32)
    steps = jnp.exp2(-trial_powers.astype(F32))
    fields = jnp.stack([iterate, source, reaction])
    fields = fields.reshape(3, 8, 16, 8, 16).transpose(3, 1, 0, 2, 4).reshape(8, 8, 3, 256)
    fields = lax.all_to_all(fields, "gx", split_axis=0, concat_axis=0, tiled=True)
    fields = fields.reshape(NX, 3 * 256).T.reshape(3, 16, 16, NX)
    fields = exchange(jnp.pad(fields, ((0, 0), (0, 0), (0, 0), (0, 128 - NX))))
    it, src, rea = fields[0], fields[1], fields[2]
    coefs_and_rest = call(
        setup_kernel, 1, [FINE] * 5 + [MID] * 5 + [FINE] * 3 + [MID] * 2 + [(20, NB, 128)], DOWN_SCRATCH, "setup"
    )(pos, it, src, rea)
    fine, mid = coefs_and_rest[:5], coefs_and_rest[5:10]
    r, x, r2, xm, r2m, pay = coefs_and_rest[10:]
    got = to_everyone(compact(pay))
    k2, k3 = call(coefficients_kernel, 0, [(5, 256, NDEV), (5, 64, NDEV)], [], "coefficients")(
        got[:, 1:].transpose(1, 0, 2)
    )
    got = got[:, 0]
    up = call(up_kernel, 1, [(B, B, 128)], [(256, NDEV), (NB // 4, NB, 128), MID, MID, MID, FINE, FINE], "up")
    image = call(image_kernel, 0, [FINE, (8, 128)], [], "image")
    q = p = d = r
    scal = jnp.zeros((8, 128), F32)
    for i in range(ITERS):
        (z,) = up(pos, got, k2, k3, *fine, *mid, x, r2, xm, r2m)
        z = exchange(z)
        w, dots = image(z, r, *fine[:4])
        dots = to_everyone(dots[0:1])[:, 0]
        if i + 1 < ITERS:
            update = call(
                lambda *refs, first=i == 0: update_kernel(first, *refs), 0,
                [(8, 128)] + [FINE] * 6 + [MID] * 2 + [(4, NB, 128)], DOWN_SCRATCH, "update",
            )
            scal, r, q, p, d, x, r2, xm, r2m, pay = update(dots, scal, z, w, r, q, p, d, *fine, *mid)
            got = to_everyone(compact(pay))[:, 0]
    own = (B, B, 128)
    d_own, r_own, layers = call(finish_kernel, 2, [own, own, (TRIALS, 8, 128)], [FINE], "finish")(
        pos, steps, dots, scal, z, w, r, q, p, d, it, src, rea
    )
    both = jnp.stack([d_own, r_own])[..., :NX].reshape(512, NX).T
    both = lax.all_to_all(both.reshape(8, 8, 512), "gx", split_axis=0, concat_axis=0, tiled=True)
    both = both.reshape(8, 8, 2, 16, 16).transpose(2, 1, 3, 0, 4).reshape(2, 8, 16, 128)
    layers = to_everyone(layers[:, 0, :NX].reshape(2, 128)).sum(axis=0).reshape(TRIALS, NX) / (NY * NZ)
    energies = jnp.sum(layers, axis=1) / NX
    mine = lax.dynamic_slice_in_dim(layers, gx * 8, 8, axis=1)
    return both[0], both[1], mine, energies


def solution(mesh):
    torus = Mesh(mesh.devices.reshape(8, 4, 2, 4), ALL)
    placed = P("gx", GY, "gz")
    return jax.shard_map(
        on_device,
        mesh=torus,
        in_specs=(placed, placed, placed, P()),
        out_specs=(placed, placed, P(None, "gx"), P()),
        check_vma=False,
    )
```

```python
import functools

import jax
import jax.numpy as jnp
from jax import lax
from jax.experimental import pallas as pl
from jax.experimental.pallas import tpu as pltpu
from jax.sharding import Mesh
from jax.sharding import PartitionSpec as P

ITERS = 4
TRIALS = 4
ALL = ("gx", "gy_0", "gy_1", "gz")
GY = ("gy_0", "gy_1")
NGX, NGY, NGZ = 8, 8, 4
NDEV = 256
NZB = 32
NX, NY, NZ = 64, 128, 512
M = 12
B = 16
NB = 40
F32 = jnp.float32
INTERPRET = False
LIMIT = 26 * 1024 * 1024

THETA = 1.15
DELTA = 0.85
SIGMA = THETA / DELTA
RHO0 = 1.0 / SIGMA
RHO1 = 1.0 / (2.0 * SIGMA - RHO0)
RHO2 = 1.0 / (2.0 * SIGMA - RHO1)
C1U = RHO1 * RHO0
C1R = 2.0 * RHO1 / DELTA
C2U = RHO2 * RHO1
C2R = 2.0 * RHO2 / DELTA


def roll(v, shift, axis):
    return pltpu.roll(v, shift % v.shape[axis], axis)


def up_z(v, s=1):
    return roll(v, -s, 0)


def dn_z(v, s=1):
    return roll(v, s, 0)


def up_x(v, s=1):
    return roll(v, -s, 1)


def dn_x(v, s=1):
    return roll(v, s, 1)


def ziota():
    return lax.broadcasted_iota(jnp.int32, (NB, 128), 0)


def xiota():
    return lax.broadcasted_iota(jnp.int32, (NB, 128), 1)


def even(iota, s):
    return (iota // s) % 2 == 0


def sum_z(v, s):
    return v + jnp.where(even(ziota(), s), up_z(v, s), dn_z(v, s))


def sum_x(v, s):
    return v + jnp.where(even(xiota(), s), up_x(v, s), dn_x(v, s))


def odd_z(v, s):
    return jnp.where(even(ziota(), s), up_z(v, s), v)


def odd_x(v, s):
    return jnp.where(even(xiota(), s), up_x(v, s), v)


class Level:
    def __init__(self, wx, wy, wz, c, dinv, s):
        self.wx, self.wy, self.wz, self.c, self.dinv, self.s = wx, wy, wz, c, dinv, s

    def y_flux(self, y, low, high):
        return self.wy[y] * (high - low)

    def apply(self, y, u, high, flux_low):
        s = self.s
        flux_y = self.wy[y] * (high - u)
        flux_x = self.wx[y] * (up_x(u, s) - u)
        flux_z = self.wz[y] * (up_z(u, s) - u)
        image = self.c[y] * u - ((flux_x - dn_x(flux_x, s)) + (flux_y - flux_low) + (flux_z - dn_z(flux_z, s)))
        return image, flux_y


def rows(lo, hi, body, carry, step=4):
    def group(start, carry):
        stores = []
        for k in range(step):
            carry, more = body(start + k, carry)
            stores += more
        for ref, at, value in stores:
            ref[at] = value
        return carry

    count = (hi - lo) // step
    if count:
        carry = lax.fori_loop(0, count, lambda i, carry: group(lo + i * step, carry), carry)
    for y in range(lo + count * step, hi):
        carry, stores = body(y, carry)
        for ref, at, value in stores:
            ref[at] = value
    return carry


def sweep(level, lo, hi, field, store):
    first = field(lo)
    flux = level.y_flux(lo - 1, field(lo - 1), first)

    def row(y, carry):
        u, flux_low = carry
        high = field(y + 1)
        image, flux_y = level.apply(y, u, high, flux_low)
        return (high, flux_y), store(y, u, image)

    rows(lo, hi, row, (first, flux))


def smooth_down(level, lo, hi, r, r1, u1, x, r2):
    def start(y):
        return level.dinv[y] * r[y] * (1.0 / THETA)

    def first(y, u, image):
        rest = r[y] - image
        after = C1U * u + C1R * (level.dinv[y] * rest)
        return [(r1, y, rest), (u1, y, after), (x, y, u + after)]

    sweep(level, lo, hi, start, first)
    sweep(level, lo + 1, hi - 1, lambda y: u1[y], lambda y, u, image: [(r2, y, r1[y] - image)])


def smooth_up(level, lo, hi, e, r2, r3, u, x, finish):
    def first(y, own, image):
        rest = r2[y] - image
        return [(r3, y, rest), (u, y, level.dinv[y] * rest * (1.0 / THETA))]

    sweep(level, lo, hi, e, first)

    def second(y, own, image):
        rest = r3[y] - image
        after = C1U * own + C1R * (level.dinv[y] * rest)
        return finish(y, (x[y] + e(y)) + (own + after))

    sweep(level, lo + 1, hi - 1, lambda y: u[y], second)


def down(fine, mid, r, x, r2, xm, r2m, r1, u1, b1, r1m, u1m):
    smooth_down(fine, 3, 37, r, r1, u1, x, r2)
    rows(2, 18, lambda y, c: (c, [(b1, y, sum_x(sum_z(r2[2 * y] + r2[2 * y + 1], 1), 1))]), 0)
    smooth_down(mid, 3, 17, b1, r1m, u1m, xm, r2m)
    return to_line([sum_x(sum_z(r2m[2 * k + 6] + r2m[2 * k + 7], 2), 2) for k in range(4)])


def to_line(rows):
    spread = lax.broadcasted_iota(jnp.int32, (128, 256), 1) % 16 * 4 == lax.broadcasted_iota(jnp.int32, (128, 256), 0)
    spread = jnp.where(spread, 1.0, 0.0)
    at = lax.broadcasted_iota(jnp.int32, (NB, 256), 1) // 16
    z = lax.broadcasted_iota(jnp.int32, (NB, 256), 0)
    line = jnp.zeros((1, 256), F32)
    for y in range(4):
        wide = jnp.dot(rows[y], spread, precision=lax.Precision.HIGHEST, preferred_element_type=F32)
        mine = (at // 4 == y) & (z == M + 4 * (at % 4))
        line = line + jnp.sum(jnp.where(mine, wide, 0.0), axis=0, keepdims=True)
    return line


def levels_of(coef, coef1):
    return Level(*(coef.at[k] for k in range(5)), 1), Level(*(coef1.at[k] for k in range(5)), 2)


def cycle_of(cycle, cycle1):
    return cycle.at[0], cycle.at[1], cycle1.at[0], cycle1.at[1]


def setup_kernel(pos, fields, coef, coef1, rq, cycle, cycle1, kept, pay, *scratch):
    it, src, rea, r = fields.at[0], fields.at[1], fields.at[2], rq.at[0]
    fine, mid = levels_of(coef, coef1)
    wx, wy, wz, c, dinv = fine.wx, fine.wy, fine.wz, fine.c, fine.dinv
    wx1, wy1, wz1, c1, dinv1 = mid.wx, mid.wy, mid.wz, mid.c, mid.dinv
    for k in range(3):
        kept[k] = fields[k, M - 1 : M + B + 1]
    gy, zb = pos[0], pos[1]
    zg = ziota() + (zb * B - M)
    lane = xiota()
    inside_zx = (zg >= 0) & (zg < NZ) & (lane < NX)

    def weight(g):
        square = g * g
        root = jnp.sqrt(1.0 + square)
        return (1.0 + 2.0 * square) / root, g * root

    def row(y, carry):
        flow_low, wy_low, wym_low = carry
        yg = gy * B - M + y
        here, high = it[y], it[y + 1]
        w_x, p_x = weight(up_x(here) - here)
        w_y, p_y = weight(high - here)
        w_z, p_z = weight(up_z(here) - here)
        inside = inside_zx & (yg >= 0) & (yg < NY)
        rest = src[y] - rea[y] * here + ((p_x - dn_x(p_x)) + (p_y - flow_low) + (p_z - dn_z(p_z)))
        outer = rea[y] + jnp.where(lane == 0, dn_x(w_x), 0.0) + jnp.where(lane == NX - 1, w_x, 0.0)
        outer = outer + jnp.where(zg == 0, dn_z(w_z), 0.0) + jnp.where(zg == NZ - 1, w_z, 0.0)
        outer = outer + jnp.where(yg == 0, wy_low, 0.0) + jnp.where(yg == NY - 1, w_y, 0.0)
        outer = jnp.where(inside, outer, 0.0)
        m_x = jnp.where(inside & (lane < NX - 1), w_x, 0.0)
        m_y = jnp.where(inside & (yg < NY - 1), w_y, 0.0)
        m_z = jnp.where(inside & (zg < NZ - 1), w_z, 0.0)
        diagonal = outer + m_x + dn_x(m_x) + m_y + wym_low + m_z + dn_z(m_z)
        good = diagonal > 0.0
        inverse = jnp.where(good, 1.0 / jnp.where(good, diagonal, 1.0), 0.0)
        stores = [(r, y, jnp.where(inside, rest, 0.0)), (wx, y, m_x), (wy, y, m_y), (wz, y, m_z), (c, y, outer)]
        return (p_y, w_y, m_y), stores + [(dinv, y, inverse)]

    zero = jnp.zeros((NB, 128), F32)
    rows(0, NB - 1, row, (zero, zero, zero), 2)
    for ref in (wx, wy, wz, c, dinv, r):
        ref[NB - 1] = zero

    def row1(y, low):
        a, b = 2 * y, 2 * y + 1
        m_x = sum_z(odd_x(wx[a] + wx[b], 1), 1)
        m_y = sum_x(sum_z(wy[b], 1), 1)
        m_z = sum_x(odd_z(wz[a] + wz[b], 1), 1)
        m_c = sum_x(sum_z(c[a] + c[b], 1), 1)
        diagonal = m_c + m_x + dn_x(m_x, 2) + m_y + low + m_z + dn_z(m_z, 2)
        good = diagonal > 0.0
        inverse = jnp.where(good, 1.0 / jnp.where(good, diagonal, 1.0), 0.0)
        return m_y, [(wx1, y, m_x), (wy1, y, m_y), (wz1, y, m_z), (c1, y, m_c), (dinv1, y, inverse)]

    rows(0, NB // 2, row1, zero, 2)

    pay[:, 0:256] = down(fine, mid, r, *cycle_of(cycle, cycle1), *scratch)
    pair = [(2 * k + 6, 2 * k + 7) for k in range(4)]
    pay[:, 256:512] = to_line([sum_z(odd_x(wx1[a] + wx1[b], 2), 2) for a, b in pair])
    pay[:, 512:768] = to_line([sum_x(sum_z(wy1[b], 2), 2) for a, b in pair])
    pay[:, 768:1024] = to_line([sum_x(odd_z(wz1[a] + wz1[b], 2), 2) for a, b in pair])
    pay[:, 1024:1280] = to_line([sum_x(sum_z(c1[a] + c1[b], 2), 2) for a, b in pair])


def lane_ids():
    return lax.broadcasted_iota(jnp.int32, (16, NDEV), 1)


def next_z(v):
    return jnp.where(lane_ids() < 224, roll(v, -32, 1), roll(v, 223, 1))


def prev_z(v):
    lanes = lane_ids()
    return jnp.where(lanes >= 32, roll(v, 32, 1), jnp.where(lanes == 0, 0.0, roll(v, -223, 1)))


def next_y(v):
    return roll(v, -4, 1)


def prev_y(v):
    return roll(v, 4, 1)


def coarse_apply(n, s, u, wx, wy, wz, c):
    flux_y = [[None] * n for _ in range(n)]
    flux_z = [[None] * n for _ in range(n)]
    for y in range(n):
        for z in range(n):
            here = u[y][z]
            high_y = u[y + 1][z] if y + 1 < n else next_y(u[0][z])
            high_z = u[y][z + 1] if z + 1 < n else next_z(u[y][0])
            flux_y[y][z] = wy(y, z) * (high_y - here)
            flux_z[y][z] = wz(y, z) * (high_z - here)
    image = [[None] * n for _ in range(n)]
    for y in range(n):
        for z in range(n):
            here = u[y][z]
            flux_x = wx(y, z) * (roll(here, -s, 0) - here)
            low_y = flux_y[y - 1][z] if y else prev_y(flux_y[n - 1][z])
            low_z = flux_z[y][z - 1] if z else prev_z(flux_z[y][n - 1])
            image[y][z] = c(y, z) * here - (
                (flux_x - roll(flux_x, s, 0)) + (flux_y[y][z] - low_y) + (flux_z[y][z] - low_z)
            )
    return image


def planes(n, f):
    return [[f(y, z) for z in range(n)] for y in range(n)]


def pair_x(v):
    iota = lax.broadcasted_iota(jnp.int32, (16, NDEV), 0)
    return v + jnp.where(even(iota, 1), roll(v, -1, 0), roll(v, 1, 0))


def odd_pair_x(v):
    iota = lax.broadcasted_iota(jnp.int32, (16, NDEV), 0)
    return jnp.where(even(iota, 1), roll(v, -1, 0), v)


def inverse_diagonal(n, s, wx, wy, wz, c):
    def one(y, z):
        low_y = wy(y - 1, z) if y else prev_y(wy(n - 1, z))
        low_z = wz(y, z - 1) if z else prev_z(wz(y, n - 1))
        diagonal = c(y, z) + wx(y, z) + roll(wx(y, z), s, 0) + wy(y, z) + low_y + wz(y, z) + low_z
        return 1.0 / diagonal

    return planes(n, one)


def coefficients(got, k2, k3):
    for f in range(4):
        k2[f] = got[:, 256 * (f + 1) : 256 * (f + 2)].T

    def field(f):
        return lambda y, z: k2[f, pl.ds((y * 4 + z) * 16, 16), :]

    wx, wy, wz, c = (field(f) for f in range(4))
    inverse = inverse_diagonal(4, 1, wx, wy, wz, c)
    for y in range(4):
        for z in range(4):
            k2[4, pl.ds((y * 4 + z) * 16, 16), :] = inverse[y][z]
    for y in range(2):
        for z in range(2):
            a, b, e, f = (2 * y, 2 * z), (2 * y, 2 * z + 1), (2 * y + 1, 2 * z), (2 * y + 1, 2 * z + 1)
            at = pl.ds((y * 2 + z) * 16, 16)
            k3[0, at, :] = odd_pair_x((wx(*a) + wx(*b)) + (wx(*e) + wx(*f)))
            k3[1, at, :] = pair_x(wy(*e) + wy(*f))
            k3[2, at, :] = pair_x(wz(*b) + wz(*f))
            k3[3, at, :] = pair_x((c(*a) + c(*b)) + (c(*e) + c(*f)))

    def field3(f):
        return lambda y, z: k3[f, pl.ds((y * 2 + z) * 16, 16), :]

    inverse = inverse_diagonal(2, 2, *(field3(f) for f in range(4)))
    for y in range(2):
        for z in range(2):
            k3[4, pl.ds((y * 2 + z) * 16, 16), :] = inverse[y][z]


def combine(n, f, *lists):
    return planes(n, lambda y, z: f(*(a[y][z] for a in lists)))


def coarse_solve(k2, k3, b2t):
    def field(ref, n, f):
        return lambda y, z: ref[f, pl.ds((y * n + z) * 16, 16), :]

    a2 = tuple(field(k2, 4, f) for f in range(4))
    dinv = planes(4, field(k2, 4, 4))
    a3 = tuple(field(k3, 2, f) for f in range(4))
    dinv3 = planes(2, field(k3, 2, 4))
    r = planes(4, lambda y, z: b2t[pl.ds((y * 4 + z) * 16, 16), :])
    u = combine(4, lambda d, b: d * b / THETA, dinv, r)
    r = combine(4, lambda a, b: a - b, r, coarse_apply(4, 1, u, *a2))
    u1 = combine(4, lambda u, d, r: C1U * u + C1R * (d * r), u, dinv, r)
    x = combine(4, lambda a, b: a + b, u, u1)
    r = combine(4, lambda a, b: a - b, r, coarse_apply(4, 1, u1, *a2))
    r3 = planes(
        2,
        lambda y, z: pair_x(
            (r[2 * y][2 * z] + r[2 * y][2 * z + 1]) + (r[2 * y + 1][2 * z] + r[2 * y + 1][2 * z + 1])
        ),
    )
    u = combine(2, lambda d, b: d * b / THETA, dinv3, r3)
    x3 = u
    for cu, cr in ((C1U, C1R), (C2U, C2R)):
        r3 = combine(2, lambda a, b: a - b, r3, coarse_apply(2, 2, u, *a3))
        u = combine(2, lambda u, d, r: cu * u + cr * (d * r), u, dinv3, r3)
        x3 = combine(2, lambda a, b: a + b, x3, u)
    e = planes(4, lambda y, z: x3[y // 2][z // 2])
    x = combine(4, lambda a, b: a + b, x, e)
    r = combine(4, lambda a, b: a - b, r, coarse_apply(4, 1, e, *a2))
    u = combine(4, lambda d, b: d * b / THETA, dinv, r)
    r = combine(4, lambda a, b: a - b, r, coarse_apply(4, 1, u, *a2))
    u1 = combine(4, lambda u, d, r: C1U * u + C1R * (d * r), u, dinv, r)
    return combine(4, lambda x, a, b: x + (a + b), x, u, u1)


def place_coarse(pos, x2, e2):
    gy, zb = pos[0], pos[1]
    lanes = lane_ids()
    picked = {}
    for dy in (-1, 0, 1):
        for dz in (-1, 0, 1):
            at_y = jnp.clip(gy + dy, 0, NGY - 1)
            at_z = jnp.clip(zb + dz, 0, NZB - 1)
            picked[dy, dz] = lanes == ((at_z % NGX) * NGY + at_y) * NGZ + at_z // NGX
    spread = lax.broadcasted_iota(jnp.int32, (16, 128), 1) // 4 == lax.broadcasted_iota(jnp.int32, (16, 128), 0)
    rows = ziota() // 4
    for y2 in range(1, 9):
        dy, y = (y2 - 3) // 4, (y2 - 3) % 4
        plane = jnp.zeros((NB, 128), F32)
        for z2 in range(1, 9):
            dz, z = (z2 - 3) // 4, (z2 - 3) % 4
            column = jnp.sum(jnp.where(picked[dy, dz], x2[y][z], 0.0), axis=1, keepdims=True)
            line = jnp.sum(jnp.where(spread, column, 0.0), axis=0, keepdims=True)
            plane = jnp.where(rows == z2, line, plane)
        e2[y2] = plane


def up(pos, k2, k3, b2t, fine, mid, x, r2, xm, r2m, out, e2, r3, u, x1, r3m, um):
    place_coarse(pos, coarse_solve(k2, k3, b2t), e2)
    smooth_up(mid, 4, 16, lambda y: e2[y // 2], r2m, r3m, um, xm, lambda y, value: [(x1, y, value)])

    def result(y, value):
        return [(out, y - M, dn_z(value, -M)[:B])]

    smooth_up(fine, 11, 29, lambda y: x1[y // 2], r2, r3, u, x, result)


def first_kernel(pos, got, coef, coef1, cycle, cycle1, out, k2, k3, b2t, *scratch):
    fine, mid = levels_of(coef, coef1)
    coefficients(got, k2, k3)
    b2t[...] = got[:, 0:256].T
    up(pos, k2, k3, b2t, fine, mid, *cycle_of(cycle, cycle1), out, *scratch)


def image_kernel(last, centre, low, high, rq, coef, coef1, z_kept, w, pay, z, *scratch):
    fine, mid = levels_of(coef, coef1)
    z[0:M] = low[...]
    z[M : M + B] = centre[...]
    z[M + B : NB] = high[...]
    z_kept[...] = z[M - 1 : M + B + 1]
    lo, hi = (M, M + B) if last else (2, 38)
    sweep(fine, lo, hi, lambda y: z[y], lambda y, u, image: [(w, y, image)])
    own = (ziota() >= M) & (ziota() < M + B)

    def row(y, carry):
        a, b = carry
        here = jnp.where(own, z[y], 0.0)
        return (a + rq[0, y] * here, b + here * w[y]), []

    zero = jnp.zeros((NB, 128), F32)
    a, b = rows(M, M + B, row, (zero, zero))
    lane = lax.broadcasted_iota(jnp.int32, (1, 128), 1)
    pay[:, 0:128] = jnp.where(lane == 0, jnp.sum(a), jnp.where(lane == 1, jnp.sum(b), 0.0))
    if not last:
        cycle, cycle1 = scratch[:2]
        pay[:, 128:384] = down(fine, mid, w, *cycle_of(cycle, cycle1), *scratch[2:])


def step_sizes(got, old, scal, first):
    total = jnp.sum(got[:, 0:128], axis=0, keepdims=True)
    lane = lax.broadcasted_iota(jnp.int32, (1, 128), 1)

    def pick(v, k):
        return jnp.sum(jnp.where(lane == k, v, 0.0))

    one = jnp.ones((1, 128), F32)
    gamma, delta = pick(total, 0) * one, pick(total, 1) * one
    if first:
        beta = jnp.zeros((1, 128), F32)
        alpha = gamma / delta
    else:
        was = old[0:1]
        gamma_old, alpha_old = pick(was, 0) * one, pick(was, 1) * one
        beta = gamma / gamma_old
        alpha = gamma / (delta - beta * gamma / alpha_old)
    if scal is not None:
        scal[...] = jnp.broadcast_to(jnp.where(lane == 0, gamma, alpha), (8, 128))
    return alpha, beta


def step_kernel(first, pos, got, old, z, w, b2_was, rq, *refs):
    pd, refs = (None, refs) if first else (refs[0], refs[1:])
    coef, coef1, k2, k3, scal, rq_o, pd_o, out, pay, b2q, b2t, cycle, cycle1, e2, *scratch = refs
    fine, mid = levels_of(coef, coef1)
    alpha, beta = step_sizes(got, old, scal, first)

    def row(y, carry):
        q = w[y] if first else w[y] + beta * rq[1, y]
        return carry, [(rq_o, (1, y), q), (rq_o, (0, y), rq[0, y] - alpha * q)]

    rows(2, 38, row, 0)

    def row_d(y, carry):
        p = z[y] if first else z[y] + beta * pd[0, y]
        return carry, [(pd_o, (0, y), p), (pd_o, (1, y), alpha * p if first else pd[1, y] + alpha * p)]

    rows(0, B + 2, row_d, 0)
    x, r2, xm, r2m = cycle_of(cycle, cycle1)
    pay[...] = down(fine, mid, rq_o.at[0], x, r2, xm, r2m, *scratch)
    alpha2 = jnp.concatenate([alpha, alpha], axis=1)
    if first:
        b2q[...] = got[:, 128:384].T
        b2t[...] = b2_was[...] - alpha2 * b2q[...]
    else:
        beta2 = jnp.concatenate([beta, beta], axis=1)
        b2q[...] = got[:, 128:384].T + beta2 * b2_was[...]
        b2t[...] = got[:, 384:640].T - alpha2 * b2q[...]
    up(pos, k2, k3, b2t, fine, mid, x, r2, xm, r2m, out, e2, *scratch)


def finish_kernel(pos, steps, got, old, z, w, rq, pd, kept, d_out, r_out, layers, d_all):
    alpha, beta = step_sizes(got, old, None, False)
    gy, zb = pos[0], pos[1]
    rows(0, B + 2, lambda y, c: (c, [(d_all, y, pd[1, y] + alpha * (z[y] + beta * pd[0, y]))]), 0)

    def row(y, carry):
        r = rq[0, y + M] - alpha * (w[y + M] + beta * rq[1, y + M])
        return carry, [(r_out, y, dn_z(r, -M)[:B]), (d_out, y, dn_z(d_all[y + 1], -M)[:B])]

    rows(0, B, row, 0)
    zi = ziota()
    own = (zi >= M) & (zi < M + B)
    own_z = own | ((zi == M + B) & (zb == NZB - 1))
    lane = lax.broadcasted_iota(jnp.int32, (1, 128), 1)

    def energy(g):
        square = 1.0 + g * g
        return (square * jnp.sqrt(square) - 1.0) / 3.0

    zero = jnp.zeros((NB, 128), F32)
    for k in range(TRIALS):
        step = steps[k]

        def trial(y):
            return kept[0, y] + step * d_all[y]

        def row(y, carry):
            low, acc_x, acc = carry
            v = trial(y)
            acc_x = acc_x + jnp.where(own, energy(v - dn_x(v)), 0.0)
            part = energy(v - low) + (0.5 * kept[2, y] * v * v - kept[1, y] * v)
            acc = acc + jnp.where(own, part, 0.0) + jnp.where(own_z, energy(v - dn_z(v)), 0.0)
            return (v, acc_x, acc), []

        v, acc_x, acc = rows(1, B + 1, row, (trial(0), zero, zero), 2)
        last = own & (gy == NGY - 1)
        acc = acc + jnp.where(last, energy(trial(B + 1) - v), 0.0)
        sum_of_x = jnp.sum(acc_x, axis=0, keepdims=True)
        top = jnp.where(lane == NX - 1, jnp.broadcast_to(roll(jnp.broadcast_to(sum_of_x, (8, 128)), -1, 1)[0:1], (1, 128)), 0.0)
        layers[k] = jnp.broadcast_to(sum_of_x + top + jnp.sum(acc, axis=0, keepdims=True), (8, 128))


VM = pl.BlockSpec(memory_space=pltpu.VMEM)
SM = pl.BlockSpec(memory_space=pltpu.SMEM)


def call(kernel, n_scalar, outs, scratch, name, aliases={}):
    def run(*args):
        return pl.pallas_call(
            kernel,
            in_specs=[SM] * n_scalar + [VM] * (len(args) - n_scalar),
            out_specs=[VM] * len(outs),
            out_shape=[jax.ShapeDtypeStruct(s, F32) for s in outs],
            scratch_shapes=[pltpu.VMEM(s, F32) for s in scratch],
            input_output_aliases=aliases,
            compiler_params=pltpu.CompilerParams(vmem_limit_bytes=LIMIT),
            interpret=INTERPRET,
            name=name,
        )(*args)

    return run


FINE = (NB, NB, 128)
MID = (NB // 2, NB, 128)
KEPT = (B + 2, NB, 128)
SCRATCH = [FINE, FINE, MID, MID, MID]
CYCLE = [(2, *FINE), (2, *MID)]
COEFS = [(5, *FINE), (5, *MID)]
COARSE = (NB // 4, NB, 128)
PLANES = (256, NDEV)


def shift_pairs(dy, dz):
    pairs = []
    for gy in range(NGY):
        for zb in range(NZB):
            ty, tz = gy + dy, zb + dz
            if 0 <= ty < NGY and 0 <= tz < NZB:
                source = ((zb % NGX) * NGY + gy) * NGZ + zb // NGX
                target = ((tz % NGX) * NGY + ty) * NGZ + tz // NGX
                pairs.append((source, target))
    return pairs


def exchange_z(own):
    low = lax.ppermute(own, ALL, shift_pairs(0, 1))
    high = lax.ppermute(own, ALL, shift_pairs(0, -1))
    return jnp.concatenate([low[..., B - M :, :], own, high[..., :M, :]], axis=-2)


def exchange_y(own):
    low = lax.ppermute(own[..., B - M :, :, :], ALL, shift_pairs(1, 0))
    high = lax.ppermute(own[..., :M, :, :], ALL, shift_pairs(-1, 0))
    return low, high


def to_everyone(x):
    copies = jnp.broadcast_to(x, (NDEV, *x.shape))
    return lax.all_to_all(copies, ALL, split_axis=0, concat_axis=0, tiled=True)


def to_everyone_by_axes(line):
    n = line.shape[1]
    copies = jnp.broadcast_to(line, (NGX, 1, n))
    got = lax.all_to_all(copies, "gx", split_axis=0, concat_axis=0, tiled=True)
    copies = jnp.broadcast_to(got.reshape(NGX, n), (NDEV // NGX, NGX, n))
    got = lax.all_to_all(copies, (*GY, "gz"), split_axis=0, concat_axis=0, tiled=True)
    return got.transpose(1, 0, 2).reshape(NDEV, n)


def on_device(iterate, source, reaction, trial_powers):
    gx = lax.axis_index("gx")
    gy = lax.axis_index(GY)
    zb = lax.axis_index("gz") * NGX + gx
    pos = jnp.stack([gy, zb]).astype(jnp.int32)
    steps = jnp.exp2(-trial_powers.astype(F32))
    fields = jnp.stack([iterate, source, reaction])
    fields = fields.reshape(3, 8, 16, 8, 16).transpose(3, 1, 0, 2, 4).reshape(8, 8, 3, 256)
    fields = lax.all_to_all(fields, "gx", split_axis=0, concat_axis=0, tiled=True)
    fields = fields.reshape(NX, 3 * 256).T.reshape(3, 16, 16, NX)
    fields = exchange_z(jnp.pad(fields, ((0, 0), (0, 0), (0, 0), (0, 128 - NX))))
    low, high = exchange_y(fields)
    fields = jnp.concatenate([low, fields, high], axis=1)
    coef, coef1, rq, cycle, cycle1, kept, pay = call(
        setup_kernel, 1, COEFS + [(2, *FINE)] + CYCLE + [(3, *KEPT), (1, 1280)], SCRATCH, "setup"
    )(pos, fields)
    own = (B, B, 128)
    z, k2, k3, b2 = call(
        first_kernel, 1, [own, (5, 256, NDEV), (5, 64, NDEV), PLANES], [COARSE] + SCRATCH, "first"
    )(pos, to_everyone_by_axes(pay), coef, coef1, cycle, cycle1)
    scal = jnp.zeros((8, 128), F32)
    pd = None
    for i in range(ITERS):
        first, last = i == 0, i + 1 == ITERS
        centre = exchange_z(z)
        low, high = exchange_y(centre)
        z, w, line = call(
            functools.partial(image_kernel, last), 0, [KEPT, FINE, (1, 128 if last else 384)],
            [FINE] + ([] if last else CYCLE + SCRATCH), "image",
        )(centre, low, high, rq, coef, coef1)
        if last:
            break
        if not first:
            line = jnp.concatenate([line, pay], axis=1)
        got = to_everyone(line)[:, 0]
        state = (rq,) if first else (rq, pd)
        scal, rq, pd, z, pay, b2 = call(
            functools.partial(step_kernel, first), 1,
            [(8, 128), (2, *FINE), (2, *KEPT), own, (1, 256), PLANES], [PLANES] + CYCLE + [COARSE] + SCRATCH, "step",
            {6: 1} if first else {6: 1, 7: 2},
        )(pos, got, scal, z, w, b2, *state, coef, coef1, k2, k3)
    dots = to_everyone(line)[:, 0]
    d_own, r_own, layers = call(finish_kernel, 2, [own, own, (TRIALS, 8, 128)], [KEPT], "finish")(
        pos, steps, dots, scal, z, w, rq, pd, kept
    )
    both = jnp.stack([d_own, r_own])[..., :NX].reshape(512, NX).T
    both = lax.all_to_all(both.reshape(8, 8, 512), "gx", split_axis=0, concat_axis=0, tiled=True)
    both = both.reshape(8, 8, 2, 16, 16).transpose(2, 1, 3, 0, 4).reshape(2, 8, 16, 128)
    layers = to_everyone(layers[:, 0, :NX].reshape(1, 256)).sum(axis=0).reshape(TRIALS, NX) / (NY * NZ)
    energies = jnp.sum(layers, axis=1) / NX
    mine = lax.dynamic_slice_in_dim(layers, gx * 8, 8, axis=1)
    return both[0], both[1], mine, energies


def solution(mesh):
    torus = Mesh(mesh.devices.reshape(8, 4, 2, 4), ALL)
    placed = P("gx", GY, "gz")
    return jax.shard_map(
        on_device,
        mesh=torus,
        in_specs=(placed, placed, placed, P()),
        out_specs=(placed, placed, P(None, "gx"), P()),
        check_vma=False,
    )
```

```python
import functools

import jax
import jax.numpy as jnp
from jax import lax
from jax.experimental import pallas as pl
from jax.experimental.pallas import tpu as pltpu
from jax.sharding import Mesh
from jax.sharding import PartitionSpec as P

ITERS = 4
TRIALS = 4
ALL = ("gx", "gy_0", "gy_1", "gz")
GY = ("gy_0", "gy_1")
NGX, NGY, NGZ = 8, 8, 4
NDEV = 256
NZB = 32
NX, NY, NZ = 64, 128, 512
M = 12
B = 16
NB = 40
F32 = jnp.float32
INTERPRET = False
H = 20
LIMIT = 26 * 1024 * 1024

THETA = 1.15
DELTA = 0.85
SIGMA = THETA / DELTA
RHO0 = 1.0 / SIGMA
RHO1 = 1.0 / (2.0 * SIGMA - RHO0)
RHO2 = 1.0 / (2.0 * SIGMA - RHO1)
C1U = RHO1 * RHO0
C1R = 2.0 * RHO1 / DELTA
C2U = RHO2 * RHO1
C2R = 2.0 * RHO2 / DELTA


def roll(v, shift, axis):
    return pltpu.roll(v, shift % v.shape[axis], axis)


def up_z(v, s=1):
    return roll(v, -s, 0)


def dn_z(v, s=1):
    return roll(v, s, 0)


def up_x(v, s=1):
    return roll(v, -s, 1)


def dn_x(v, s=1):
    return roll(v, s, 1)


def swap(v):
    return roll(v, NX, 1)


def ziota():
    return lax.broadcasted_iota(jnp.int32, (NB, 128), 0)


def xiota():
    return lax.broadcasted_iota(jnp.int32, (NB, 128), 1)


def even(iota, s):
    return (iota // s) % 2 == 0


def sum_z(v, s):
    return v + jnp.where(even(ziota(), s), up_z(v, s), dn_z(v, s))


def sum_x(v, s):
    return v + jnp.where(even(xiota(), s), up_x(v, s), dn_x(v, s))


def odd_z(v, s):
    return jnp.where(even(ziota(), s), up_z(v, s), v)


def odd_x(v, s):
    return jnp.where(even(xiota(), s), up_x(v, s), v)


class Level:
    def __init__(self, wx, wy, wz, c, dinv, s):
        self.wx, self.wy, self.wz, self.c, self.dinv, self.s = wx, wy, wz, c, dinv, s

    def y_flux(self, y, low, high):
        return self.wy[y] * (high - low)

    def apply(self, y, u, high, flux_low):
        s = self.s
        flux_y = self.wy[y] * (high - u)
        flux_x = self.wx[y] * (up_x(u, s) - u)
        flux_z = self.wz[y] * (up_z(u, s) - u)
        image = self.c[y] * u - ((flux_x - dn_x(flux_x, s)) + (flux_y - flux_low) + (flux_z - dn_z(flux_z, s)))
        return image, flux_y


def rows(lo, hi, body, carry, step=4):
    def group(start, carry):
        stores = []
        for k in range(step):
            carry, more = body(start + k, carry)
            stores += more
        for ref, at, value in stores:
            ref[at] = value
        return carry

    count = (hi - lo) // step
    if count:
        carry = lax.fori_loop(0, count, lambda i, carry: group(lo + i * step, carry), carry)
    for y in range(lo + count * step, hi):
        carry, stores = body(y, carry)
        for ref, at, value in stores:
            ref[at] = value
    return carry


def sweep(level, lo, n, field, store):
    first = field(lo)
    flux = level.y_flux(lo - 1, field(lo - 1), first)

    def row(y, carry):
        u, flux_low = carry
        high = field(y + 1)
        image, flux_y = level.apply(y, u, high, flux_low)
        return (high, flux_y), store(y, u, image)

    u, flux_low = rows(lo, n - 1, row, (first, flux))
    image, _ = level.apply(n - 1, u, swap(u), flux_low)
    for ref, at, value in store(n - 1, u, image):
        ref[at] = value


def smooth_down(level, lo, n, r, r1, u1, x, r2):
    def start(y):
        return level.dinv[y] * r[y] * (1.0 / THETA)

    def first(y, u, image):
        rest = r[y] - image
        after = C1U * u + C1R * (level.dinv[y] * rest)
        return [(r1, y, rest), (u1, y, after), (x, y, u + after)]

    sweep(level, lo, n, start, first)
    sweep(level, lo + 1, n, lambda y: u1[y], lambda y, u, image: [(r2, y, r1[y] - image)])


def smooth_up(level, lo, n, e, r2, r3, u, x, finish):
    def first(y, own, image):
        rest = r2[y] - image
        return [(r3, y, rest), (u, y, level.dinv[y] * rest * (1.0 / THETA))]

    sweep(level, lo, n, e, first)

    def second(y, own, image):
        rest = r3[y] - image
        after = C1U * own + C1R * (level.dinv[y] * rest)
        return finish(y, (x[y] + e(y)) + (own + after))

    sweep(level, lo + 1, n, lambda y: u[y], second)


def down(fine, mid, r, x, r2, xm, r2m, r1, u1, b1, r1m, u1m):
    smooth_down(fine, 3, H, r, r1, u1, x, r2)
    rows(2, H // 2, lambda y, c: (c, [(b1, y, sum_x(sum_z(r2[2 * y] + r2[2 * y + 1], 1), 1))]), 0)
    smooth_down(mid, 3, H // 2, b1, r1m, u1m, xm, r2m)
    return to_line([sum_x(sum_z(r2m[2 * k + 6] + r2m[2 * k + 7], 2), 2) for k in range(2)])


def to_line(folded):
    to = lax.broadcasted_iota(jnp.int32, (128, 256), 1)
    spread = to % 16 * 4 + to // 128 * NX == lax.broadcasted_iota(jnp.int32, (128, 256), 0)
    spread = jnp.where(spread, 1.0, 0.0)
    at = lax.broadcasted_iota(jnp.int32, (NB, 256), 1) // 16
    y = at // 4
    z = lax.broadcasted_iota(jnp.int32, (NB, 256), 0) == M + 4 * (at % 4)
    line = jnp.zeros((1, 256), F32)
    for k in range(2):
        wide = jnp.dot(folded[k], spread, precision=lax.Precision.HIGHEST, preferred_element_type=F32)
        line = line + jnp.sum(jnp.where(((y == k) | (y == 3 - k)) & z, wide, 0.0), axis=0, keepdims=True)
    return line


def levels_of(coef, coef1):
    return Level(*(coef.at[k] for k in range(5)), 1), Level(*(coef1.at[k] for k in range(5)), 2)


def cycle_of(cycle, cycle1):
    return cycle.at[0], cycle.at[1], cycle1.at[0], cycle1.at[1]


def setup_kernel(pos, fields, coef, coef1, rq, cycle, cycle1, kept, pay, *scratch):
    it, src, rea, r = fields.at[0], fields.at[1], fields.at[2], rq.at[0]
    fine, mid = levels_of(coef, coef1)
    wx, wy, wz, c, dinv = fine.wx, fine.wy, fine.wz, fine.c, fine.dinv
    wx1, wy1, wz1, c1, dinv1 = mid.wx, mid.wy, mid.wz, mid.c, mid.dinv
    for k in range(3):
        kept[k] = fields[k, M - 1 : H]
    gy, zb = pos[0], pos[1]
    zg = ziota() + (zb * B - M)
    lane = xiota()
    xg = lane % NX
    inside_z = (zg >= 0) & (zg < NZ)
    at_edge = ((lane < NX) & (gy == 0)) | ((lane >= NX) & (gy == NGY - 1))

    def weight(g):
        square = g * g
        root = jnp.sqrt(1.0 + square)
        return (1.0 + 2.0 * square) / root, g * root

    def row(y, carry, high=None):
        here, flow_low, wy_low, wym_low = carry
        high = it[y + 1] if high is None else high
        w_x, p_x = weight(jnp.where(xg == NX - 1, 0.0, up_x(here)) - here)
        w_0, p_0 = weight(here)
        w_y, p_y = weight(high - here)
        w_z, p_z = weight(up_z(here) - here)
        inside = inside_z & jnp.logical_not(at_edge & (y < M))
        low_x = jnp.where(xg == 0, p_0, dn_x(p_x))
        rest = src[y] - rea[y] * here + ((p_x - low_x) + (p_y - flow_low) + (p_z - dn_z(p_z)))
        outer = rea[y] + jnp.where(xg == 0, w_0, 0.0) + jnp.where(xg == NX - 1, w_x, 0.0)
        outer = outer + jnp.where(zg == 0, dn_z(w_z), 0.0) + jnp.where(zg == NZ - 1, w_z, 0.0)
        outer = outer + jnp.where(at_edge & (y == M), wy_low, 0.0)
        outer = jnp.where(inside, outer, 0.0)
        m_x = jnp.where(inside & (xg < NX - 1), w_x, 0.0)
        m_y = jnp.where(inside, w_y, 0.0)
        m_z = jnp.where(inside & (zg < NZ - 1), w_z, 0.0)
        diagonal = outer + m_x + dn_x(m_x) + m_y + wym_low + m_z + dn_z(m_z)
        good = diagonal > 0.0
        inverse = jnp.where(good, 1.0 / jnp.where(good, diagonal, 1.0), 0.0)
        stores = [(r, y, jnp.where(inside, rest, 0.0)), (wx, y, m_x), (wy, y, m_y), (wz, y, m_z), (c, y, outer)]
        return (high, p_y, w_y, m_y), stores + [(dinv, y, inverse)]

    zero = jnp.zeros((NB, 128), F32)
    carry = rows(1, H - 1, row, (it[1], zero, zero, zero), 2)
    for ref, at, value in row(H - 1, carry, swap(carry[0]))[1]:
        ref[at] = value
    for ref in (wx, wy, wz, c, dinv, r):
        ref[0] = zero

    def row1(y, low):
        a, b = 2 * y, 2 * y + 1
        m_x = sum_z(odd_x(wx[a] + wx[b], 1), 1)
        m_y = sum_x(sum_z(wy[b], 1), 1)
        m_z = sum_x(odd_z(wz[a] + wz[b], 1), 1)
        m_c = sum_x(sum_z(c[a] + c[b], 1), 1)
        diagonal = m_c + m_x + dn_x(m_x, 2) + m_y + low + m_z + dn_z(m_z, 2)
        good = diagonal > 0.0
        inverse = jnp.where(good, 1.0 / jnp.where(good, diagonal, 1.0), 0.0)
        return m_y, [(wx1, y, m_x), (wy1, y, m_y), (wz1, y, m_z), (c1, y, m_c), (dinv1, y, inverse)]

    rows(0, H // 2, row1, zero, 2)

    pay[:, 0:256] = down(fine, mid, r, *cycle_of(cycle, cycle1), *scratch)
    pair = [(2 * k + 6, 2 * k + 7) for k in range(2)]
    pay[:, 256:512] = to_line([sum_z(odd_x(wx1[a] + wx1[b], 2), 2) for a, b in pair])
    half = lane < NX
    pay[:, 512:768] = to_line([sum_x(sum_z(jnp.where(half, wy1[b], wy1[b - 2]), 2), 2) for a, b in pair])
    pay[:, 768:1024] = to_line([sum_x(odd_z(wz1[a] + wz1[b], 2), 2) for a, b in pair])
    pay[:, 1024:1280] = to_line([sum_x(sum_z(c1[a] + c1[b], 2), 2) for a, b in pair])


def lane_ids():
    return lax.broadcasted_iota(jnp.int32, (16, NDEV), 1)


def next_z(v):
    return jnp.where(lane_ids() < 224, roll(v, -32, 1), roll(v, 223, 1))


def prev_z(v):
    lanes = lane_ids()
    return jnp.where(lanes >= 32, roll(v, 32, 1), jnp.where(lanes == 0, 0.0, roll(v, -223, 1)))


def next_y(v):
    return roll(v, -4, 1)


def prev_y(v):
    return roll(v, 4, 1)


def coarse_apply(n, s, u, wx, wy, wz, c):
    flux_y = [[None] * n for _ in range(n)]
    flux_z = [[None] * n for _ in range(n)]
    for y in range(n):
        for z in range(n):
            here = u[y][z]
            high_y = u[y + 1][z] if y + 1 < n else next_y(u[0][z])
            high_z = u[y][z + 1] if z + 1 < n else next_z(u[y][0])
            flux_y[y][z] = wy(y, z) * (high_y - here)
            flux_z[y][z] = wz(y, z) * (high_z - here)
    image = [[None] * n for _ in range(n)]
    for y in range(n):
        for z in range(n):
            here = u[y][z]
            flux_x = wx(y, z) * (roll(here, -s, 0) - here)
            low_y = flux_y[y - 1][z] if y else prev_y(flux_y[n - 1][z])
            low_z = flux_z[y][z - 1] if z else prev_z(flux_z[y][n - 1])
            image[y][z] = c(y, z) * here - (
                (flux_x - roll(flux_x, s, 0)) + (flux_y[y][z] - low_y) + (flux_z[y][z] - low_z)
            )
    return image


def planes(n, f):
    return [[f(y, z) for z in range(n)] for y in range(n)]


def pair_x(v):
    iota = lax.broadcasted_iota(jnp.int32, (16, NDEV), 0)
    return v + jnp.where(even(iota, 1), roll(v, -1, 0), roll(v, 1, 0))


def odd_pair_x(v):
    iota = lax.broadcasted_iota(jnp.int32, (16, NDEV), 0)
    return jnp.where(even(iota, 1), roll(v, -1, 0), v)


def inverse_diagonal(n, s, wx, wy, wz, c):
    def one(y, z):
        low_y = wy(y - 1, z) if y else prev_y(wy(n - 1, z))
        low_z = wz(y, z - 1) if z else prev_z(wz(y, n - 1))
        diagonal = c(y, z) + wx(y, z) + roll(wx(y, z), s, 0) + wy(y, z) + low_y + wz(y, z) + low_z
        return 1.0 / diagonal

    return planes(n, one)


def coefficients(got, k2, k3):
    for f in range(4):
        k2[f] = got[:, 256 * (f + 1) : 256 * (f + 2)].T

    def field(f):
        return lambda y, z: k2[f, pl.ds((y * 4 + z) * 16, 16), :]

    wx, wy, wz, c = (field(f) for f in range(4))
    inverse = inverse_diagonal(4, 1, wx, wy, wz, c)
    for y in range(4):
        for z in range(4):
            k2[4, pl.ds((y * 4 + z) * 16, 16), :] = inverse[y][z]
    for y in range(2):
        for z in range(2):
            a, b, e, f = (2 * y, 2 * z), (2 * y, 2 * z + 1), (2 * y + 1, 2 * z), (2 * y + 1, 2 * z + 1)
            at = pl.ds((y * 2 + z) * 16, 16)
            k3[0, at, :] = odd_pair_x((wx(*a) + wx(*b)) + (wx(*e) + wx(*f)))
            k3[1, at, :] = pair_x(wy(*e) + wy(*f))
            k3[2, at, :] = pair_x(wz(*b) + wz(*f))
            k3[3, at, :] = pair_x((c(*a) + c(*b)) + (c(*e) + c(*f)))

    def field3(f):
        return lambda y, z: k3[f, pl.ds((y * 2 + z) * 16, 16), :]

    inverse = inverse_diagonal(2, 2, *(field3(f) for f in range(4)))
    for y in range(2):
        for z in range(2):
            k3[4, pl.ds((y * 2 + z) * 16, 16), :] = inverse[y][z]


def combine(n, f, *lists):
    return planes(n, lambda y, z: f(*(a[y][z] for a in lists)))


def coarse_solve(k2, k3, b2t):
    def field(ref, n, f):
        return lambda y, z: ref[f, pl.ds((y * n + z) * 16, 16), :]

    a2 = tuple(field(k2, 4, f) for f in range(4))
    dinv = planes(4, field(k2, 4, 4))
    a3 = tuple(field(k3, 2, f) for f in range(4))
    dinv3 = planes(2, field(k3, 2, 4))
    r = planes(4, lambda y, z: b2t[pl.ds((y * 4 + z) * 16, 16), :])
    u = combine(4, lambda d, b: d * b / THETA, dinv, r)
    r = combine(4, lambda a, b: a - b, r, coarse_apply(4, 1, u, *a2))
    u1 = combine(4, lambda u, d, r: C1U * u + C1R * (d * r), u, dinv, r)
    x = combine(4, lambda a, b: a + b, u, u1)
    r = combine(4, lambda a, b: a - b, r, coarse_apply(4, 1, u1, *a2))
    r3 = planes(
        2,
        lambda y, z: pair_x(
            (r[2 * y][2 * z] + r[2 * y][2 * z + 1]) + (r[2 * y + 1][2 * z] + r[2 * y + 1][2 * z + 1])
        ),
    )
    u = combine(2, lambda d, b: d * b / THETA, dinv3, r3)
    x3 = u
    for cu, cr in ((C1U, C1R), (C2U, C2R)):
        r3 = combine(2, lambda a, b: a - b, r3, coarse_apply(2, 2, u, *a3))
        u = combine(2, lambda u, d, r: cu * u + cr * (d * r), u, dinv3, r3)
        x3 = combine(2, lambda a, b: a + b, x3, u)
    e = planes(4, lambda y, z: x3[y // 2][z // 2])
    x = combine(4, lambda a, b: a + b, x, e)
    r = combine(4, lambda a, b: a - b, r, coarse_apply(4, 1, e, *a2))
    u = combine(4, lambda d, b: d * b / THETA, dinv, r)
    r = combine(4, lambda a, b: a - b, r, coarse_apply(4, 1, u, *a2))
    u1 = combine(4, lambda u, d, r: C1U * u + C1R * (d * r), u, dinv, r)
    return combine(4, lambda x, a, b: x + (a + b), x, u, u1)


def place_coarse(pos, x2, e2):
    gy, zb = pos[0], pos[1]
    lanes = lane_ids()
    picked = {}
    for dy in (-1, 0, 1):
        for dz in (-1, 0, 1):
            at_y = jnp.clip(gy + dy, 0, NGY - 1)
            at_z = jnp.clip(zb + dz, 0, NZB - 1)
            picked[dy, dz] = lanes == ((at_z % NGX) * NGY + at_y) * NGZ + at_z // NGX
    lane = lax.broadcasted_iota(jnp.int32, (16, 128), 1)
    spread = lane % NX // 4 == lax.broadcasted_iota(jnp.int32, (16, 128), 0)
    rows_z = ziota() // 4

    def column(y2, z2):
        mine = picked[(y2 - 3) // 4, (z2 - 3) // 4]
        return jnp.sum(jnp.where(mine, x2[(y2 - 3) % 4][(z2 - 3) % 4], 0.0), axis=1, keepdims=True)

    for k in range(1, 5):
        plane = jnp.zeros((NB, 128), F32)
        for z2 in range(1, 9):
            both = jnp.where(lane < NX, column(k, z2), column(9 - k, z2))
            line = jnp.sum(jnp.where(spread, both, 0.0), axis=0, keepdims=True)
            plane = jnp.where(rows_z == z2, line, plane)
        e2[k] = plane


def up(pos, k2, k3, b2t, fine, mid, x, r2, xm, r2m, out, e2, r3, u, x1, r3m, um):
    place_coarse(pos, coarse_solve(k2, k3, b2t), e2)
    smooth_up(mid, 4, H // 2, lambda y: e2[y // 2], r2m, r3m, um, xm, lambda y, value: [(x1, y, value)])

    def result(y, value):
        return [(out, y - M, dn_z(value, -M)[:B])]

    smooth_up(fine, M - 1, H, lambda y: x1[y // 2], r2, r3, u, x, result)


def first_kernel(pos, got, coef, coef1, cycle, cycle1, out, k2, k3, b2t, *scratch):
    fine, mid = levels_of(coef, coef1)
    coefficients(got, k2, k3)
    b2t[...] = got[:, 0:256].T
    up(pos, k2, k3, b2t, fine, mid, *cycle_of(cycle, cycle1), out, *scratch)


def image_kernel(last, centre, *refs):
    if last:
        before, after, edge, rq, coef, coef1, z_kept, w, pay, z, *scratch = refs
        z[M - 1] = edge[0]
        blank = jnp.zeros((8, 128), F32)
        for k in range(8):
            z[M + k] = roll(jnp.concatenate([before[k], centre[k], after[k], blank], axis=0), 4, 0)
    else:
        low, high, rq, coef, coef1, z_kept, w, pay, z, *scratch = refs
        half = xiota() < NX
        z[M:H] = centre[...]
        for k in range(4):
            z[k] = jnp.where(half, low[k + 4], high[k + 4])
        for k in range(4, M):
            z[k] = swap(jnp.where(half, high[11 - k], low[11 - k]))
    fine, mid = levels_of(coef, coef1)
    z_kept[...] = z[M - 1 : H]
    sweep(fine, M if last else 2, H, lambda y: z[y], lambda y, u, image: [(w, y, image)])
    own = (ziota() >= M) & (ziota() < M + B)

    def row(y, carry):
        a, b = carry
        here = jnp.where(own, z[y], 0.0)
        return (a + rq[0, y] * here, b + here * w[y]), []

    zero = jnp.zeros((NB, 128), F32)
    a, b = rows(M, H, row, (zero, zero))
    lane = lax.broadcasted_iota(jnp.int32, (1, 128), 1)
    pay[:, 0:128] = jnp.where(lane == 0, jnp.sum(a), jnp.where(lane == 1, jnp.sum(b), 0.0))
    if not last:
        cycle, cycle1 = scratch[:2]
        pay[:, 128:384] = down(fine, mid, w, *cycle_of(cycle, cycle1), *scratch[2:])


def step_sizes(got, old, scal, first):
    total = jnp.sum(got[:, 0:128], axis=0, keepdims=True)
    lane = lax.broadcasted_iota(jnp.int32, (1, 128), 1)

    def pick(v, k):
        return jnp.sum(jnp.where(lane == k, v, 0.0))

    one = jnp.ones((1, 128), F32)
    gamma, delta = pick(total, 0) * one, pick(total, 1) * one
    if first:
        beta = jnp.zeros((1, 128), F32)
        alpha = gamma / delta
    else:
        was = old[0:1]
        gamma_old, alpha_old = pick(was, 0) * one, pick(was, 1) * one
        beta = gamma / gamma_old
        alpha = gamma / (delta - beta * gamma / alpha_old)
    if scal is not None:
        scal[...] = jnp.broadcast_to(jnp.where(lane == 0, gamma, alpha), (8, 128))
    return alpha, beta


def step_kernel(first, pos, got, old, z, w, b2_was, rq, *refs):
    pd, refs = (None, refs) if first else (refs[0], refs[1:])
    coef, coef1, k2, k3, scal, rq_o, pd_o, out, pay, b2q, b2t, cycle, cycle1, e2, *scratch = refs
    fine, mid = levels_of(coef, coef1)
    alpha, beta = step_sizes(got, old, scal, first)

    def row(y, carry):
        q = w[y] if first else w[y] + beta * rq[1, y]
        return carry, [(rq_o, (1, y), q), (rq_o, (0, y), rq[0, y] - alpha * q)]

    rows(2, H, row, 0)

    def row_d(y, carry):
        p = z[y] if first else z[y] + beta * pd[0, y]
        return carry, [(pd_o, (0, y), p), (pd_o, (1, y), alpha * p if first else pd[1, y] + alpha * p)]

    rows(0, 9, row_d, 0)
    x, r2, xm, r2m = cycle_of(cycle, cycle1)
    pay[...] = down(fine, mid, rq_o.at[0], x, r2, xm, r2m, *scratch)
    alpha2 = jnp.concatenate([alpha, alpha], axis=1)
    if first:
        b2q[...] = got[:, 128:384].T
        b2t[...] = b2_was[...] - alpha2 * b2q[...]
    else:
        beta2 = jnp.concatenate([beta, beta], axis=1)
        b2q[...] = got[:, 128:384].T + beta2 * b2_was[...]
        b2t[...] = got[:, 384:640].T - alpha2 * b2q[...]
    up(pos, k2, k3, b2t, fine, mid, x, r2, xm, r2m, out, e2, *scratch)


def finish_kernel(pos, steps, got, old, z, w, rq, pd, kept, d_out, r_out, layers, d_all):
    alpha, beta = step_sizes(got, old, None, False)
    gy, zb = pos[0], pos[1]
    rows(0, 9, lambda y, c: (c, [(d_all, y, pd[1, y] + alpha * (z[y] + beta * pd[0, y]))]), 0)

    def row(y, carry):
        r = rq[0, y + M] - alpha * (w[y + M] + beta * rq[1, y + M])
        return carry, [(r_out, y, dn_z(r, -M)[:B]), (d_out, y, dn_z(d_all[y + 1], -M)[:B])]

    rows(0, 8, row, 0)
    zi = ziota()
    own = (zi >= M) & (zi < M + B)
    own_z = own | ((zi == M + B) & (zb == NZB - 1))
    lane = xiota()
    x = lane % NX
    edge = own & ((lane < NX) | (gy == NGY - 1))

    def energy(g):
        square = 1.0 + g * g
        return (square * jnp.sqrt(square) - 1.0) / 3.0

    zero = jnp.zeros((NB, 128), F32)
    for k in range(TRIALS):
        step = steps[k]

        def trial(y):
            return kept[0, y] + step * d_all[y]

        def part(y, low, acc, outer):
            v = trial(y)
            acc = acc + jnp.where(outer, energy(v - low), 0.0) + jnp.where(own_z, energy(v - dn_z(v)), 0.0)
            inner = energy(v - jnp.where(x == 0, 0.0, dn_x(v))) + jnp.where(x == NX - 1, energy(v), 0.0)
            inner = inner + (0.5 * kept[2, y] * v * v - kept[1, y] * v)
            return v, acc + jnp.where(own, inner, 0.0)

        def row(y, carry):
            return part(y, *carry, own), []

        v, acc = rows(2, 9, row, part(1, trial(0), zero, edge), 2)
        acc = acc + jnp.where(own & (lane < NX), energy(swap(v) - v), 0.0)
        total = jnp.broadcast_to(jnp.sum(acc, axis=0, keepdims=True), (8, 128))
        layers[k] = total + swap(total)


VM = pl.BlockSpec(memory_space=pltpu.VMEM)
SM = pl.BlockSpec(memory_space=pltpu.SMEM)


def call(kernel, n_scalar, outs, scratch, name, aliases={}):
    def run(*args):
        return pl.pallas_call(
            kernel,
            in_specs=[SM] * n_scalar + [VM] * (len(args) - n_scalar),
            out_specs=[VM] * len(outs),
            out_shape=[jax.ShapeDtypeStruct(s, F32) for s in outs],
            scratch_shapes=[pltpu.VMEM(s, F32) for s in scratch],
            input_output_aliases=aliases,
            compiler_params=pltpu.CompilerParams(vmem_limit_bytes=LIMIT),
            interpret=INTERPRET,
            name=name,
        )(*args)

    return run


FINE = (H, NB, 128)
MID = (H // 2, NB, 128)
KEPT = (9, NB, 128)
SCRATCH = [FINE, FINE, MID, MID, MID]
CYCLE = [(2, *FINE), (2, *MID)]
COEFS = [(5, *FINE), (5, *MID)]
COARSE = (H // 4, NB, 128)
PLANES = (256, NDEV)


def shift_pairs(dy, dz):
    pairs = []
    for gy in range(NGY):
        for zb in range(NZB):
            ty, tz = gy + dy, zb + dz
            if 0 <= ty < NGY and 0 <= tz < NZB:
                source = ((zb % NGX) * NGY + gy) * NGZ + zb // NGX
                target = ((tz % NGX) * NGY + ty) * NGZ + tz // NGX
                pairs.append((source, target))
    return pairs


def exchange_z(own):
    low = lax.ppermute(own, ALL, shift_pairs(0, 1))
    high = lax.ppermute(own, ALL, shift_pairs(0, -1))
    return jnp.concatenate([low[..., B - M :, :], own, high[..., :M, :]], axis=-2)


def exchange_y(own):
    return lax.ppermute(own, ALL, shift_pairs(1, 0)), lax.ppermute(own, ALL, shift_pairs(-1, 0))


def exchange_faces(own):
    low = lax.ppermute(own[:, 8:], ALL, shift_pairs(0, 1))
    high = lax.ppermute(own[:, :8], ALL, shift_pairs(0, -1))
    below, above = exchange_y(own[:1])
    edge = jnp.concatenate([below[..., NX:], above[..., :NX]], axis=-1)
    return own, low, high, jnp.pad(edge, ((0, 0), (M, M), (0, 0)))


def unfold_margin(own, low, high):
    outer = jnp.concatenate([low[..., 4:, :, :NX], high[..., 4:, :, NX:]], axis=-1)
    inner = jnp.concatenate([low[..., ::-1, :, NX:], high[..., ::-1, :, :NX]], axis=-1)
    return jnp.concatenate([outer, inner, own], axis=-3)


def to_everyone(x):
    copies = jnp.broadcast_to(x, (NDEV, *x.shape))
    return lax.all_to_all(copies, ALL, split_axis=0, concat_axis=0, tiled=True)


def to_everyone_by_axes(line):
    n = line.shape[1]
    copies = jnp.broadcast_to(line, (NGX, 1, n))
    got = lax.all_to_all(copies, "gx", split_axis=0, concat_axis=0, tiled=True)
    copies = jnp.broadcast_to(got.reshape(NGX, n), (NDEV // NGX, NGX, n))
    got = lax.all_to_all(copies, (*GY, "gz"), split_axis=0, concat_axis=0, tiled=True)
    return got.transpose(1, 0, 2).reshape(NDEV, n)


def on_device(iterate, source, reaction, trial_powers):
    gx = lax.axis_index("gx")
    gy = lax.axis_index(GY)
    zb = lax.axis_index("gz") * NGX + gx
    pos = jnp.stack([gy, zb]).astype(jnp.int32)
    pos, steps = lax.optimization_barrier((pos, jnp.exp2(-trial_powers.astype(F32))))
    fields = jnp.stack([iterate, source, reaction])
    fields = fields.reshape(3, 8, 16, 8, 16).transpose(3, 1, 0, 2, 4).reshape(8, 8, 3, 256)
    fields = lax.all_to_all(fields, "gx", split_axis=0, concat_axis=0, tiled=True)
    fields = fields.reshape(NX, 3 * 256).T.reshape(3, 16, 16, NX)
    fields = jnp.concatenate([fields[:, :8], fields[:, :7:-1]], axis=-1)
    fields = exchange_z(fields)
    fields = unfold_margin(fields, *exchange_y(fields))
    coef, coef1, rq, cycle, cycle1, kept, pay = call(
        setup_kernel, 1, COEFS + [(2, *FINE)] + CYCLE + [(3, *KEPT), (1, 1280)], SCRATCH, "setup"
    )(pos, fields)
    own = (8, B, 128)
    z, k2, k3, b2 = call(
        first_kernel, 1, [own, (5, 256, NDEV), (5, 64, NDEV), PLANES], [COARSE] + SCRATCH, "first"
    )(pos, to_everyone_by_axes(pay), coef, coef1, cycle, cycle1)
    scal = jnp.zeros((8, 128), F32)
    pd = None
    for i in range(ITERS):
        first, last = i == 0, i + 1 == ITERS
        if last:
            around = exchange_faces(z)
        else:
            centre = exchange_z(z)
            around = (centre, *exchange_y(centre))
        z, w, line = call(
            functools.partial(image_kernel, last), 0, [KEPT, FINE, (1, 128 if last else 384)],
            [FINE] + ([] if last else CYCLE + SCRATCH), "image",
        )(*around, rq, coef, coef1)
        if last:
            break
        if not first:
            line = jnp.concatenate([line, pay], axis=1)
        got = to_everyone(line)[:, 0]
        state = (rq,) if first else (rq, pd)
        scal, rq, pd, z, pay, b2 = call(
            functools.partial(step_kernel, first), 1,
            [(8, 128), (2, *FINE), (2, *KEPT), own, (1, 256), PLANES], [PLANES] + CYCLE + [COARSE] + SCRATCH, "step",
            {6: 1} if first else {6: 1, 7: 2},
        )(pos, got, scal, z, w, b2, *state, coef, coef1, k2, k3)
    dots = to_everyone(line)[:, 0]
    d_own, r_own, layers = call(finish_kernel, 2, [own, own, (TRIALS, 8, 128)], [KEPT], "finish")(
        pos, steps, dots, scal, z, w, rq, pd, kept
    )
    both = jnp.stack([d_own, r_own])
    both = jnp.concatenate([both[..., :NX], both[:, ::-1, :, NX:]], axis=1).reshape(512, NX).T
    copies = jnp.broadcast_to(layers[:, 0, :NX].reshape(1, 256), (NDEV, 1, 256))
    copies, both = lax.optimization_barrier((copies, both.reshape(8, 8, 512)))
    layers = lax.all_to_all(copies, ALL, split_axis=0, concat_axis=0, tiled=True)
    both = lax.all_to_all(both, "gx", split_axis=0, concat_axis=0, tiled=True)
    both = both.reshape(8, 8, 2, 16, 16).transpose(2, 1, 3, 0, 4).reshape(2, 8, 16, 128)
    layers = layers.sum(axis=0).reshape(TRIALS, NX) / (NY * NZ)
    energies = jnp.sum(layers, axis=1) / NX
    mine = lax.dynamic_slice_in_dim(layers, gx * 8, 8, axis=1)
    return both[0], both[1], mine, energies


def solution(mesh):
    torus = Mesh(mesh.devices.reshape(8, 4, 2, 4), ALL)
    placed = P("gx", GY, "gz")
    return jax.shard_map(
        on_device,
        mesh=torus,
        in_specs=(placed, placed, placed, P()),
        out_specs=(placed, placed, P(None, "gx"), P()),
        check_vma=False,
    )
```

```python
import functools

import jax
import jax.numpy as jnp
from jax import lax
from jax.experimental import pallas as pl
from jax.experimental.pallas import tpu as pltpu
from jax.sharding import Mesh
from jax.sharding import PartitionSpec as P

ITERS = 4
TRIALS = 4
ALL = ("gx", "gy_0", "gy_1", "gz")
GY = ("gy_0", "gy_1")
NGX, NGY, NGZ = 8, 8, 4
NDEV = 256
NZB = 32
NX, NY, NZ = 64, 128, 512
M = 12
B = 16
NB = 40
F32 = jnp.float32
INTERPRET = False
H = 20
LIMIT = 26 * 1024 * 1024

THETA = 1.15
DELTA = 0.85
SIGMA = THETA / DELTA
RHO0 = 1.0 / SIGMA
RHO1 = 1.0 / (2.0 * SIGMA - RHO0)
RHO2 = 1.0 / (2.0 * SIGMA - RHO1)
C1U = RHO1 * RHO0
C1R = 2.0 * RHO1 / DELTA
C2U = RHO2 * RHO1
C2R = 2.0 * RHO2 / DELTA


def roll(v, shift, axis):
    return pltpu.roll(v, shift % v.shape[axis], axis)


def up_z(v, s=1):
    return roll(v, -s, 0)


def dn_z(v, s=1):
    return roll(v, s, 0)


def up_x(v, s=1):
    return roll(v, -s, 1)


def dn_x(v, s=1):
    return roll(v, s, 1)


def swap(v):
    return roll(v, NX, 1)


def ziota():
    return lax.broadcasted_iota(jnp.int32, (NB, 128), 0)


def xiota():
    return lax.broadcasted_iota(jnp.int32, (NB, 128), 1)


def even(iota, s):
    return (iota // s) % 2 == 0


def sum_z(v, s):
    return v + jnp.where(even(ziota(), s), up_z(v, s), dn_z(v, s))


def sum_x(v, s):
    return v + jnp.where(even(xiota(), s), up_x(v, s), dn_x(v, s))


def odd_z(v, s):
    return jnp.where(even(ziota(), s), up_z(v, s), v)


def odd_x(v, s):
    return jnp.where(even(xiota(), s), up_x(v, s), v)


class Level:
    def __init__(self, wx, wy, wz, c, dinv, s):
        self.wx, self.wy, self.wz, self.c, self.dinv, self.s = wx, wy, wz, c, dinv, s

    def y_flux(self, y, low, high):
        return self.wy[y] * (high - low)

    def apply(self, y, u, high, flux_low):
        s = self.s
        flux_y = self.wy[y] * (high - u)
        flux_x = self.wx[y] * (up_x(u, s) - u)
        flux_z = self.wz[y] * (up_z(u, s) - u)
        image = self.c[y] * u - ((flux_x - dn_x(flux_x, s)) + (flux_y - flux_low) + (flux_z - dn_z(flux_z, s)))
        return image, flux_y


def rows(lo, hi, body, carry, step=4):
    def group(start, carry):
        stores = []
        for k in range(step):
            carry, more = body(start + k, carry)
            stores += more
        for ref, at, value in stores:
            ref[at] = value
        return carry

    count = (hi - lo) // step
    if count:
        carry = lax.fori_loop(0, count, lambda i, carry: group(lo + i * step, carry), carry)
    for y in range(lo + count * step, hi):
        carry, stores = body(y, carry)
        for ref, at, value in stores:
            ref[at] = value
    return carry


def sweep(level, lo, n, field, store):
    first = field(lo)
    flux = level.y_flux(lo - 1, field(lo - 1), first)

    def row(y, carry):
        u, flux_low = carry
        high = field(y + 1)
        image, flux_y = level.apply(y, u, high, flux_low)
        return (high, flux_y), store(y, u, image)

    u, flux_low = rows(lo, n - 1, row, (first, flux))
    image, _ = level.apply(n - 1, u, swap(u), flux_low)
    for ref, at, value in store(n - 1, u, image):
        ref[at] = value


def smooth_down(level, lo, n, r, r1, u1, x, r2):
    def start(y):
        return level.dinv[y] * r[y] * (1.0 / THETA)

    def first(y, u, image):
        rest = r[y] - image
        after = C1U * u + C1R * (level.dinv[y] * rest)
        return [(r1, y, rest), (u1, y, after), (x, y, u + after)]

    sweep(level, lo, n, start, first)
    sweep(level, lo + 1, n, lambda y: u1[y], lambda y, u, image: [(r2, y, r1[y] - image)])


def smooth_up(level, lo, n, e, r2, r3, u, x, finish):
    def first(y, own, image):
        rest = r2[y] - image
        return [(r3, y, rest), (u, y, level.dinv[y] * rest * (1.0 / THETA))]

    sweep(level, lo, n, e, first)

    def second(y, own, image):
        rest = r3[y] - image
        after = C1U * own + C1R * (level.dinv[y] * rest)
        return finish(y, (x[y] + e(y)) + (own + after))

    sweep(level, lo + 1, n, lambda y: u[y], second)


def down(fine, mid, r, x, r2, xm, r2m, r1, u1, b1, r1m, u1m):
    smooth_down(fine, 3, H, r, r1, u1, x, r2)
    rows(2, H // 2, lambda y, c: (c, [(b1, y, sum_x(sum_z(r2[2 * y] + r2[2 * y + 1], 1), 1))]), 0)
    smooth_down(mid, 3, H // 2, b1, r1m, u1m, xm, r2m)
    return to_line([sum_x(sum_z(r2m[2 * k + 6] + r2m[2 * k + 7], 2), 2) for k in range(2)])


def to_line(folded):
    to = lax.broadcasted_iota(jnp.int32, (128, 256), 1)
    spread = to % 16 * 4 + to // 128 * NX == lax.broadcasted_iota(jnp.int32, (128, 256), 0)
    spread = jnp.where(spread, 1.0, 0.0)
    at = lax.broadcasted_iota(jnp.int32, (NB, 256), 1) // 16
    y = at // 4
    z = lax.broadcasted_iota(jnp.int32, (NB, 256), 0) == M + 4 * (at % 4)
    line = jnp.zeros((1, 256), F32)
    for k in range(2):
        wide = jnp.dot(folded[k], spread, precision=lax.Precision.HIGHEST, preferred_element_type=F32)
        line = line + jnp.sum(jnp.where(((y == k) | (y == 3 - k)) & z, wide, 0.0), axis=0, keepdims=True)
    return line


def levels_of(coef, coef1):
    return Level(*(coef.at[k] for k in range(5)), 1), Level(*(coef1.at[k] for k in range(5)), 2)


def cycle_of(cycle, cycle1):
    return cycle.at[0], cycle.at[1], cycle1.at[0], cycle1.at[1]


def setup_kernel(pos, fields, coef, coef1, rq, cycle, cycle1, kept, pay, *scratch):
    it, src, rea, r = fields.at[0], fields.at[1], fields.at[2], rq.at[0]
    fine, mid = levels_of(coef, coef1)
    wx, wy, wz, c, dinv = fine.wx, fine.wy, fine.wz, fine.c, fine.dinv
    wx1, wy1, wz1, c1, dinv1 = mid.wx, mid.wy, mid.wz, mid.c, mid.dinv
    for k in range(3):
        kept[k] = fields[k, M - 1 : H]
    gy, zb = pos[0], pos[1]
    zg = ziota() + (zb * B - M)
    lane = xiota()
    xg = lane % NX
    inside_z = (zg >= 0) & (zg < NZ)
    at_edge = ((lane < NX) & (gy == 0)) | ((lane >= NX) & (gy == NGY - 1))

    def weight(g):
        square = g * g
        root = jnp.sqrt(1.0 + square)
        return (1.0 + 2.0 * square) / root, g * root

    def row(y, carry, high=None):
        here, flow_low, wy_low, wym_low = carry
        high = it[y + 1] if high is None else high
        w_x, p_x = weight(jnp.where(xg == NX - 1, 0.0, up_x(here)) - here)
        w_0, p_0 = weight(here)
        w_y, p_y = weight(high - here)
        w_z, p_z = weight(up_z(here) - here)
        inside = inside_z & jnp.logical_not(at_edge & (y < M))
        low_x = jnp.where(xg == 0, p_0, dn_x(p_x))
        rest = src[y] - rea[y] * here + ((p_x - low_x) + (p_y - flow_low) + (p_z - dn_z(p_z)))
        outer = rea[y] + jnp.where(xg == 0, w_0, 0.0) + jnp.where(xg == NX - 1, w_x, 0.0)
        outer = outer + jnp.where(zg == 0, dn_z(w_z), 0.0) + jnp.where(zg == NZ - 1, w_z, 0.0)
        outer = outer + jnp.where(at_edge & (y == M), wy_low, 0.0)
        outer = jnp.where(inside, outer, 0.0)
        m_x = jnp.where(inside & (xg < NX - 1), w_x, 0.0)
        m_y = jnp.where(inside, w_y, 0.0)
        m_z = jnp.where(inside & (zg < NZ - 1), w_z, 0.0)
        diagonal = outer + m_x + dn_x(m_x) + m_y + wym_low + m_z + dn_z(m_z)
        good = diagonal > 0.0
        inverse = jnp.where(good, 1.0 / jnp.where(good, diagonal, 1.0), 0.0)
        stores = [(r, y, jnp.where(inside, rest, 0.0)), (wx, y, m_x), (wy, y, m_y), (wz, y, m_z), (c, y, outer)]
        return (high, p_y, w_y, m_y), stores + [(dinv, y, inverse)]

    zero = jnp.zeros((NB, 128), F32)
    carry = rows(1, H - 1, row, (it[1], zero, zero, zero), 2)
    for ref, at, value in row(H - 1, carry, swap(carry[0]))[1]:
        ref[at] = value
    for ref in (wx, wy, wz, c, dinv, r):
        ref[0] = zero

    def row1(y, low):
        a, b = 2 * y, 2 * y + 1
        m_x = sum_z(odd_x(wx[a] + wx[b], 1), 1)
        m_y = sum_x(sum_z(wy[b], 1), 1)
        m_z = sum_x(odd_z(wz[a] + wz[b], 1), 1)
        m_c = sum_x(sum_z(c[a] + c[b], 1), 1)
        diagonal = m_c + m_x + dn_x(m_x, 2) + m_y + low + m_z + dn_z(m_z, 2)
        good = diagonal > 0.0
        inverse = jnp.where(good, 1.0 / jnp.where(good, diagonal, 1.0), 0.0)
        return m_y, [(wx1, y, m_x), (wy1, y, m_y), (wz1, y, m_z), (c1, y, m_c), (dinv1, y, inverse)]

    rows(0, H // 2, row1, zero, 2)

    pay[:, 0:256] = down(fine, mid, r, *cycle_of(cycle, cycle1), *scratch)
    pair = [(2 * k + 6, 2 * k + 7) for k in range(2)]
    pay[:, 256:512] = to_line([sum_z(odd_x(wx1[a] + wx1[b], 2), 2) for a, b in pair])
    half = lane < NX
    pay[:, 512:768] = to_line([sum_x(sum_z(jnp.where(half, wy1[b], wy1[b - 2]), 2), 2) for a, b in pair])
    pay[:, 768:1024] = to_line([sum_x(odd_z(wz1[a] + wz1[b], 2), 2) for a, b in pair])
    pay[:, 1024:1280] = to_line([sum_x(sum_z(c1[a] + c1[b], 2), 2) for a, b in pair])


def lane_ids():
    return lax.broadcasted_iota(jnp.int32, (16, NDEV), 1)


def next_z(v):
    lanes = lane_ids()
    ahead = jnp.where(lanes < 224, roll(v, -32, 1), roll(v, -1, 1))
    back = jnp.where(lanes >= 32, roll(v, 32, 1), roll(v, -1, 1))
    return jnp.where(lanes % 2 == 0, ahead, back)


def prev_z(v):
    lanes = lane_ids()
    back = jnp.where(lanes >= 32, roll(v, 32, 1), jnp.where(lanes == 0, 0.0, roll(v, 1, 1)))
    ahead = jnp.where(lanes < 224, roll(v, -32, 1), roll(v, 1, 1))
    return jnp.where(lanes % 2 == 0, back, ahead)


def next_y(v):
    return roll(v, -4, 1)


def prev_y(v):
    return roll(v, 4, 1)


def coarse_apply(n, s, u, wx, wy, wz, c):
    flux_y = [[None] * n for _ in range(n)]
    flux_z = [[None] * n for _ in range(n)]
    for y in range(n):
        for z in range(n):
            here = u[y][z]
            high_y = u[y + 1][z] if y + 1 < n else next_y(u[0][z])
            high_z = u[y][z + 1] if z + 1 < n else next_z(u[y][0])
            flux_y[y][z] = wy(y, z) * (high_y - here)
            flux_z[y][z] = wz(y, z) * (high_z - here)
    image = [[None] * n for _ in range(n)]
    for y in range(n):
        for z in range(n):
            here = u[y][z]
            flux_x = wx(y, z) * (roll(here, -s, 0) - here)
            low_y = flux_y[y - 1][z] if y else prev_y(flux_y[n - 1][z])
            low_z = flux_z[y][z - 1] if z else prev_z(flux_z[y][n - 1])
            image[y][z] = c(y, z) * here - (
                (flux_x - roll(flux_x, s, 0)) + (flux_y[y][z] - low_y) + (flux_z[y][z] - low_z)
            )
    return image


def planes(n, f):
    return [[f(y, z) for z in range(n)] for y in range(n)]


def pair_x(v):
    iota = lax.broadcasted_iota(jnp.int32, (16, NDEV), 0)
    return v + jnp.where(even(iota, 1), roll(v, -1, 0), roll(v, 1, 0))


def odd_pair_x(v):
    iota = lax.broadcasted_iota(jnp.int32, (16, NDEV), 0)
    return jnp.where(even(iota, 1), roll(v, -1, 0), v)


def inverse_diagonal(n, s, wx, wy, wz, c):
    def one(y, z):
        low_y = wy(y - 1, z) if y else prev_y(wy(n - 1, z))
        low_z = wz(y, z - 1) if z else prev_z(wz(y, n - 1))
        diagonal = c(y, z) + wx(y, z) + roll(wx(y, z), s, 0) + wy(y, z) + low_y + wz(y, z) + low_z
        return 1.0 / diagonal

    return planes(n, one)


def coefficients(got, k2, k3):
    for f in range(4):
        k2[f] = got[:, 256 * (f + 1) : 256 * (f + 2)].T

    def field(f):
        return lambda y, z: k2[f, pl.ds((y * 4 + z) * 16, 16), :]

    wx, wy, wz, c = (field(f) for f in range(4))
    inverse = inverse_diagonal(4, 1, wx, wy, wz, c)
    for y in range(4):
        for z in range(4):
            k2[4, pl.ds((y * 4 + z) * 16, 16), :] = inverse[y][z]
    for y in range(2):
        for z in range(2):
            a, b, e, f = (2 * y, 2 * z), (2 * y, 2 * z + 1), (2 * y + 1, 2 * z), (2 * y + 1, 2 * z + 1)
            at = pl.ds((y * 2 + z) * 16, 16)
            k3[0, at, :] = odd_pair_x((wx(*a) + wx(*b)) + (wx(*e) + wx(*f)))
            k3[1, at, :] = pair_x(wy(*e) + wy(*f))
            k3[2, at, :] = pair_x(wz(*b) + wz(*f))
            k3[3, at, :] = pair_x((c(*a) + c(*b)) + (c(*e) + c(*f)))

    def field3(f):
        return lambda y, z: k3[f, pl.ds((y * 2 + z) * 16, 16), :]

    inverse = inverse_diagonal(2, 2, *(field3(f) for f in range(4)))
    for y in range(2):
        for z in range(2):
            k3[4, pl.ds((y * 2 + z) * 16, 16), :] = inverse[y][z]


def combine(n, f, *lists):
    return planes(n, lambda y, z: f(*(a[y][z] for a in lists)))


def coarse_solve(k2, k3, b2t):
    def field(ref, n, f):
        return lambda y, z: ref[f, pl.ds((y * n + z) * 16, 16), :]

    a2 = tuple(field(k2, 4, f) for f in range(4))
    dinv = planes(4, field(k2, 4, 4))
    a3 = tuple(field(k3, 2, f) for f in range(4))
    dinv3 = planes(2, field(k3, 2, 4))
    r = planes(4, lambda y, z: b2t[pl.ds((y * 4 + z) * 16, 16), :])
    u = combine(4, lambda d, b: d * b / THETA, dinv, r)
    r = combine(4, lambda a, b: a - b, r, coarse_apply(4, 1, u, *a2))
    u1 = combine(4, lambda u, d, r: C1U * u + C1R * (d * r), u, dinv, r)
    x = combine(4, lambda a, b: a + b, u, u1)
    r = combine(4, lambda a, b: a - b, r, coarse_apply(4, 1, u1, *a2))
    r3 = planes(
        2,
        lambda y, z: pair_x(
            (r[2 * y][2 * z] + r[2 * y][2 * z + 1]) + (r[2 * y + 1][2 * z] + r[2 * y + 1][2 * z + 1])
        ),
    )
    u = combine(2, lambda d, b: d * b / THETA, dinv3, r3)
    x3 = u
    for cu, cr in ((C1U, C1R), (C2U, C2R)):
        r3 = combine(2, lambda a, b: a - b, r3, coarse_apply(2, 2, u, *a3))
        u = combine(2, lambda u, d, r: cu * u + cr * (d * r), u, dinv3, r3)
        x3 = combine(2, lambda a, b: a + b, x3, u)
    e = planes(4, lambda y, z: x3[y // 2][z // 2])
    x = combine(4, lambda a, b: a + b, x, e)
    r = combine(4, lambda a, b: a - b, r, coarse_apply(4, 1, e, *a2))
    u = combine(4, lambda d, b: d * b / THETA, dinv, r)
    r = combine(4, lambda a, b: a - b, r, coarse_apply(4, 1, u, *a2))
    u1 = combine(4, lambda u, d, r: C1U * u + C1R * (d * r), u, dinv, r)
    return combine(4, lambda x, a, b: x + (a + b), x, u, u1)


def place_coarse(pos, x2, e2):
    gy, zb = pos[0], pos[1]
    lanes = lane_ids()
    picked = {}
    for dy in (-1, 0, 1):
        for dz in (-1, 0, 1):
            at_y = jnp.clip(gy + dy, 0, NGY - 1)
            at_z = jnp.clip(zb + dz, 0, NZB - 1)
            gz, k = at_z // NGX, at_z % NGX
            picked[dy, dz] = lanes == (jnp.where(gz % 2 == 0, k, NGX - 1 - k) * NGY + at_y) * NGZ + gz
    lane = lax.broadcasted_iota(jnp.int32, (16, 128), 1)
    spread = lane % NX // 4 == lax.broadcasted_iota(jnp.int32, (16, 128), 0)
    rows_z = ziota() // 4

    def column(y2, z2):
        mine = picked[(y2 - 3) // 4, (z2 - 3) // 4]
        return jnp.sum(jnp.where(mine, x2[(y2 - 3) % 4][(z2 - 3) % 4], 0.0), axis=1, keepdims=True)

    for k in range(1, 5):
        plane = jnp.zeros((NB, 128), F32)
        for z2 in range(1, 9):
            both = jnp.where(lane < NX, column(k, z2), column(9 - k, z2))
            line = jnp.sum(jnp.where(spread, both, 0.0), axis=0, keepdims=True)
            plane = jnp.where(rows_z == z2, line, plane)
        e2[k] = plane


def up(pos, k2, k3, b2t, fine, mid, x, r2, xm, r2m, out, e2, r3, u, x1, r3m, um):
    place_coarse(pos, coarse_solve(k2, k3, b2t), e2)
    smooth_up(mid, 4, H // 2, lambda y: e2[y // 2], r2m, r3m, um, xm, lambda y, value: [(x1, y, value)])

    def result(y, value):
        return [(out, y - M, dn_z(value, -M)[:B])]

    smooth_up(fine, M - 1, H, lambda y: x1[y // 2], r2, r3, u, x, result)


def first_kernel(pos, got, coef, coef1, cycle, cycle1, out, k2, k3, b2t, *scratch):
    fine, mid = levels_of(coef, coef1)
    coefficients(got, k2, k3)
    b2t[...] = got[:, 0:256].T
    up(pos, k2, k3, b2t, fine, mid, *cycle_of(cycle, cycle1), out, *scratch)


def image_kernel(last, centre, *refs):
    if last:
        before, after, edge, rq, coef, coef1, z_kept, w, pay, z, *scratch = refs
        z[M - 1] = edge[0]
        blank = jnp.zeros((8, 128), F32)
        for k in range(8):
            z[M + k] = roll(jnp.concatenate([before[k], centre[k], after[k], blank], axis=0), 4, 0)
    else:
        low, high, rq, coef, coef1, z_kept, w, pay, z, *scratch = refs
        half = xiota() < NX
        z[M:H] = centre[...]
        for k in range(4):
            z[k] = jnp.where(half, low[k + 4], high[k + 4])
        for k in range(4, M):
            z[k] = swap(jnp.where(half, high[11 - k], low[11 - k]))
    fine, mid = levels_of(coef, coef1)
    z_kept[...] = z[M - 1 : H]
    sweep(fine, M if last else 2, H, lambda y: z[y], lambda y, u, image: [(w, y, image)])
    own = (ziota() >= M) & (ziota() < M + B)

    def row(y, carry):
        a, b = carry
        here = jnp.where(own, z[y], 0.0)
        return (a + rq[0, y] * here, b + here * w[y]), []

    zero = jnp.zeros((NB, 128), F32)
    a, b = rows(M, H, row, (zero, zero))
    lane = lax.broadcasted_iota(jnp.int32, (1, 128), 1)
    pay[:, 0:128] = jnp.where(lane == 0, jnp.sum(a), jnp.where(lane == 1, jnp.sum(b), 0.0))
    if not last:
        cycle, cycle1 = scratch[:2]
        pay[:, 128:384] = down(fine, mid, w, *cycle_of(cycle, cycle1), *scratch[2:])


def step_sizes(got, old, scal, first):
    total = jnp.sum(got[:, 0:128], axis=0, keepdims=True)
    lane = lax.broadcasted_iota(jnp.int32, (1, 128), 1)

    def pick(v, k):
        return jnp.sum(jnp.where(lane == k, v, 0.0))

    one = jnp.ones((1, 128), F32)
    gamma, delta = pick(total, 0) * one, pick(total, 1) * one
    if first:
        beta = jnp.zeros((1, 128), F32)
        alpha = gamma / delta
    else:
        was = old[0:1]
        gamma_old, alpha_old = pick(was, 0) * one, pick(was, 1) * one
        beta = gamma / gamma_old
        alpha = gamma / (delta - beta * gamma / alpha_old)
    if scal is not None:
        scal[...] = jnp.broadcast_to(jnp.where(lane == 0, gamma, alpha), (8, 128))
    return alpha, beta


def step_kernel(first, pos, got, old, z, w, b2_was, rq, *refs):
    pd, refs = (None, refs) if first else (refs[0], refs[1:])
    coef, coef1, k2, k3, scal, rq_o, pd_o, out, pay, b2q, b2t, cycle, cycle1, e2, *scratch = refs
    fine, mid = levels_of(coef, coef1)
    alpha, beta = step_sizes(got, old, scal, first)

    def row(y, carry):
        q = w[y] if first else w[y] + beta * rq[1, y]
        return carry, [(rq_o, (1, y), q), (rq_o, (0, y), rq[0, y] - alpha * q)]

    rows(2, H, row, 0)

    def row_d(y, carry):
        p = z[y] if first else z[y] + beta * pd[0, y]
        return carry, [(pd_o, (0, y), p), (pd_o, (1, y), alpha * p if first else pd[1, y] + alpha * p)]

    rows(0, 9, row_d, 0)
    x, r2, xm, r2m = cycle_of(cycle, cycle1)
    pay[...] = down(fine, mid, rq_o.at[0], x, r2, xm, r2m, *scratch)
    alpha2 = jnp.concatenate([alpha, alpha], axis=1)
    if first:
        b2q[...] = got[:, 128:384].T
        b2t[...] = b2_was[...] - alpha2 * b2q[...]
    else:
        beta2 = jnp.concatenate([beta, beta], axis=1)
        b2q[...] = got[:, 128:384].T + beta2 * b2_was[...]
        b2t[...] = got[:, 384:640].T - alpha2 * b2q[...]
    up(pos, k2, k3, b2t, fine, mid, x, r2, xm, r2m, out, e2, *scratch)


def finish_kernel(pos, steps, got, old, z, w, rq, pd, kept, d_out, r_out, layers, d_all):
    alpha, beta = step_sizes(got, old, None, False)
    gy, zb = pos[0], pos[1]
    rows(0, 9, lambda y, c: (c, [(d_all, y, pd[1, y] + alpha * (z[y] + beta * pd[0, y]))]), 0)

    def row(y, carry):
        r = rq[0, y + M] - alpha * (w[y + M] + beta * rq[1, y + M])
        return carry, [(r_out, y, dn_z(r, -M)[:B]), (d_out, y, dn_z(d_all[y + 1], -M)[:B])]

    rows(0, 8, row, 0)
    zi = ziota()
    own = (zi >= M) & (zi < M + B)
    own_z = own | ((zi == M + B) & (zb == NZB - 1))
    lane = xiota()
    x = lane % NX
    edge = own & ((lane < NX) | (gy == NGY - 1))

    def energy(g):
        square = 1.0 + g * g
        return (square * jnp.sqrt(square) - 1.0) / 3.0

    zero = jnp.zeros((NB, 128), F32)
    for k in range(TRIALS):
        step = steps[k]

        def trial(y):
            return kept[0, y] + step * d_all[y]

        def part(y, low, acc, outer):
            v = trial(y)
            acc = acc + jnp.where(outer, energy(v - low), 0.0) + jnp.where(own_z, energy(v - dn_z(v)), 0.0)
            inner = energy(v - jnp.where(x == 0, 0.0, dn_x(v))) + jnp.where(x == NX - 1, energy(v), 0.0)
            inner = inner + (0.5 * kept[2, y] * v * v - kept[1, y] * v)
            return v, acc + jnp.where(own, inner, 0.0)

        def row(y, carry):
            return part(y, *carry, own), []

        v, acc = rows(2, 9, row, part(1, trial(0), zero, edge), 2)
        acc = acc + jnp.where(own & (lane < NX), energy(swap(v) - v), 0.0)
        total = jnp.broadcast_to(jnp.sum(acc, axis=0, keepdims=True), (8, 128))
        layers[k] = total + swap(total)


VM = pl.BlockSpec(memory_space=pltpu.VMEM)
SM = pl.BlockSpec(memory_space=pltpu.SMEM)


def call(kernel, n_scalar, outs, scratch, name, aliases={}):
    def run(*args):
        return pl.pallas_call(
            kernel,
            in_specs=[SM] * n_scalar + [VM] * (len(args) - n_scalar),
            out_specs=[VM] * len(outs),
            out_shape=[jax.ShapeDtypeStruct(s, F32) for s in outs],
            scratch_shapes=[pltpu.VMEM(s, F32) for s in scratch],
            input_output_aliases=aliases,
            compiler_params=pltpu.CompilerParams(vmem_limit_bytes=LIMIT),
            interpret=INTERPRET,
            name=name,
        )(*args)

    return run


FINE = (H, NB, 128)
MID = (H // 2, NB, 128)
KEPT = (9, NB, 128)
SCRATCH = [FINE, FINE, MID, MID, MID]
CYCLE = [(2, *FINE), (2, *MID)]
COEFS = [(5, *FINE), (5, *MID)]
COARSE = (H // 4, NB, 128)
PLANES = (256, NDEV)


def device_of(gy, zb):
    gz, k = zb // NGX, zb % NGX
    return ((k if gz % 2 == 0 else NGX - 1 - k) * NGY + gy) * NGZ + gz


def shift_pairs(dy, dz):
    pairs = []
    for gy in range(NGY):
        for zb in range(NZB):
            ty, tz = gy + dy, zb + dz
            if 0 <= ty < NGY and 0 <= tz < NZB:
                pairs.append((device_of(gy, zb), device_of(ty, tz)))
    return pairs


def exchange_z(own):
    low = lax.ppermute(own, ALL, shift_pairs(0, 1))
    high = lax.ppermute(own, ALL, shift_pairs(0, -1))
    return jnp.concatenate([low[..., B - M :, :], own, high[..., :M, :]], axis=-2)


def exchange_y(own):
    return lax.ppermute(own, ALL, shift_pairs(1, 0)), lax.ppermute(own, ALL, shift_pairs(-1, 0))


def exchange_faces(own):
    low = lax.ppermute(own[:, 8:], ALL, shift_pairs(0, 1))
    high = lax.ppermute(own[:, :8], ALL, shift_pairs(0, -1))
    below, above = exchange_y(own[:1])
    edge = jnp.concatenate([below[..., NX:], above[..., :NX]], axis=-1)
    return own, low, high, jnp.pad(edge, ((0, 0), (M, M), (0, 0)))


def unfold_margin(own, low, high):
    outer = jnp.concatenate([low[..., 4:, :, :NX], high[..., 4:, :, NX:]], axis=-1)
    inner = jnp.concatenate([low[..., ::-1, :, NX:], high[..., ::-1, :, :NX]], axis=-1)
    return jnp.concatenate([outer, inner, own], axis=-3)


def to_everyone(x):
    copies = jnp.broadcast_to(x, (NDEV, *x.shape))
    return lax.all_to_all(copies, ALL, split_axis=0, concat_axis=0, tiled=True)


def to_everyone_by_axes(line):
    n = line.shape[1]
    copies = jnp.broadcast_to(line, (NGX, 1, n))
    got = lax.all_to_all(copies, "gx", split_axis=0, concat_axis=0, tiled=True)
    copies = jnp.broadcast_to(got.reshape(NGX, n), (NDEV // NGX, NGX, n))
    got = lax.all_to_all(copies, (*GY, "gz"), split_axis=0, concat_axis=0, tiled=True)
    return got.transpose(1, 0, 2).reshape(NDEV, n)


def on_device(iterate, source, reaction, trial_powers):
    gx = lax.axis_index("gx")
    gy = lax.axis_index(GY)
    gz = lax.axis_index("gz")
    down_gx = gz % 2 == 1
    zb = gz * NGX + jnp.where(down_gx, NGX - 1 - gx, gx)
    pos = jnp.stack([gy, zb]).astype(jnp.int32)
    pos, steps = lax.optimization_barrier((pos, jnp.exp2(-trial_powers.astype(F32))))
    fields = jnp.stack([iterate, source, reaction])
    fields = fields.reshape(3, 8, 16, 8, 16).transpose(3, 1, 0, 2, 4).reshape(8, 8, 3, 256)
    fields = jnp.where(down_gx, fields[::-1], fields)
    fields = lax.all_to_all(fields, "gx", split_axis=0, concat_axis=0, tiled=True)
    fields = fields.reshape(NX, 3 * 256).T.reshape(3, 16, 16, NX)
    fields = jnp.concatenate([fields[:, :8], fields[:, :7:-1]], axis=-1)
    fields = exchange_z(fields)
    fields = unfold_margin(fields, *exchange_y(fields))
    coef, coef1, rq, cycle, cycle1, kept, pay = call(
        setup_kernel, 1, COEFS + [(2, *FINE)] + CYCLE + [(3, *KEPT), (1, 1280)], SCRATCH, "setup"
    )(pos, fields)
    own = (8, B, 128)
    z, k2, k3, b2 = call(
        first_kernel, 1, [own, (5, 256, NDEV), (5, 64, NDEV), PLANES], [COARSE] + SCRATCH, "first"
    )(pos, to_everyone_by_axes(pay), coef, coef1, cycle, cycle1)
    scal = jnp.zeros((8, 128), F32)
    pd = None
    for i in range(ITERS):
        first, last = i == 0, i + 1 == ITERS
        if last:
            around = exchange_faces(z)
        else:
            centre = exchange_z(z)
            around = (centre, *exchange_y(centre))
        z, w, line = call(
            functools.partial(image_kernel, last), 0, [KEPT, FINE, (1, 128 if last else 384)],
            [FINE] + ([] if last else CYCLE + SCRATCH), "image",
        )(*around, rq, coef, coef1)
        if last:
            break
        if not first:
            line = jnp.concatenate([line, pay], axis=1)
        got = to_everyone(line)[:, 0]
        state = (rq,) if first else (rq, pd)
        scal, rq, pd, z, pay, b2 = call(
            functools.partial(step_kernel, first), 1,
            [(8, 128), (2, *FINE), (2, *KEPT), own, (1, 256), PLANES], [PLANES] + CYCLE + [COARSE] + SCRATCH, "step",
            {6: 1} if first else {6: 1, 7: 2},
        )(pos, got, scal, z, w, b2, *state, coef, coef1, k2, k3)
    dots = to_everyone(line)[:, 0]
    d_own, r_own, layers = call(finish_kernel, 2, [own, own, (TRIALS, 8, 128)], [KEPT], "finish")(
        pos, steps, dots, scal, z, w, rq, pd, kept
    )
    both = jnp.stack([d_own, r_own])
    both = jnp.concatenate([both[..., :NX], both[:, ::-1, :, NX:]], axis=1).reshape(512, NX).T
    copies = jnp.broadcast_to(layers[:, 0, :NX].reshape(1, 256), (NDEV, 1, 256))
    copies, both = lax.optimization_barrier((copies, both.reshape(8, 8, 512)))
    layers = lax.all_to_all(copies, ALL, split_axis=0, concat_axis=0, tiled=True)
    both = lax.all_to_all(both, "gx", split_axis=0, concat_axis=0, tiled=True)
    both = jnp.where(down_gx, both[::-1], both)
    both = both.reshape(8, 8, 2, 16, 16).transpose(2, 1, 3, 0, 4).reshape(2, 8, 16, 128)
    layers = layers.sum(axis=0).reshape(TRIALS, NX) / (NY * NZ)
    energies = jnp.sum(layers, axis=1) / NX
    mine = lax.dynamic_slice_in_dim(layers, gx * 8, 8, axis=1)
    return both[0], both[1], mine, energies


def solution(mesh):
    torus = Mesh(mesh.devices.reshape(8, 4, 2, 4), ALL)
    placed = P("gx", GY, "gz")
    return jax.shard_map(
        on_device,
        mesh=torus,
        in_specs=(placed, placed, placed, P()),
        out_specs=(placed, placed, P(None, "gx"), P()),
        check_vma=False,
    )
```

```python
import functools

import jax
import jax.numpy as jnp
from jax import lax
from jax.experimental import pallas as pl
from jax.experimental.pallas import tpu as pltpu
from jax.sharding import Mesh
from jax.sharding import PartitionSpec as P

ITERS = 4
TRIALS = 4
ALL = ("gx", "gy_0", "gy_1", "gz")
GY = ("gy_0", "gy_1")
NGX, NGY, NGZ = 8, 8, 4
NDEV = 256
NZB = 32
NX, NY, NZ = 64, 128, 512
M = 12
B = 16
NB = 40
F32 = jnp.float32
INTERPRET = False
H = 20
LIMIT = 26 * 1024 * 1024

THETA = 1.15
DELTA = 0.85
SIGMA = THETA / DELTA
RHO0 = 1.0 / SIGMA
RHO1 = 1.0 / (2.0 * SIGMA - RHO0)
RHO2 = 1.0 / (2.0 * SIGMA - RHO1)
C1U = RHO1 * RHO0
C1R = 2.0 * RHO1 / DELTA
C2U = RHO2 * RHO1
C2R = 2.0 * RHO2 / DELTA


def roll(v, shift, axis):
    return pltpu.roll(v, shift % v.shape[axis], axis)


def up_z(v, s=1):
    return roll(v, -s, 0)


def dn_z(v, s=1):
    return roll(v, s, 0)


def up_x(v, s=1):
    return roll(v, -s, 1)


def dn_x(v, s=1):
    return roll(v, s, 1)


def swap(v):
    return roll(v, NX, 1)


def ziota():
    return lax.broadcasted_iota(jnp.int32, (NB, 128), 0)


def xiota():
    return lax.broadcasted_iota(jnp.int32, (NB, 128), 1)


def even(iota, s):
    return (iota // s) % 2 == 0


def sum_z(v, s):
    return v + jnp.where(even(ziota(), s), up_z(v, s), dn_z(v, s))


def sum_x(v, s):
    return v + jnp.where(even(xiota(), s), up_x(v, s), dn_x(v, s))


def odd_z(v, s):
    return jnp.where(even(ziota(), s), up_z(v, s), v)


def odd_x(v, s):
    return jnp.where(even(xiota(), s), up_x(v, s), v)


class Level:
    def __init__(self, wx, wy, wz, c, dinv, s):
        self.wx, self.wy, self.wz, self.c, self.dinv, self.s = wx, wy, wz, c, dinv, s

    def y_flux(self, y, low, high):
        return self.wy[y] * (high - low)

    def apply(self, y, u, high, flux_low):
        s = self.s
        flux_y = self.wy[y] * (high - u)
        flux_x = self.wx[y] * (up_x(u, s) - u)
        flux_z = self.wz[y] * (up_z(u, s) - u)
        image = self.c[y] * u - ((flux_x - dn_x(flux_x, s)) + (flux_y - flux_low) + (flux_z - dn_z(flux_z, s)))
        return image, flux_y


def rows(lo, hi, body, carry, step=4):
    def group(start, carry):
        stores = []
        for k in range(step):
            carry, more = body(start + k, carry)
            stores += more
        for ref, at, value in stores:
            ref[at] = value
        return carry

    count = (hi - lo) // step
    if count:
        carry = lax.fori_loop(0, count, lambda i, carry: group(lo + i * step, carry), carry)
    for y in range(lo + count * step, hi):
        carry, stores = body(y, carry)
        for ref, at, value in stores:
            ref[at] = value
    return carry


def sweep(level, lo, n, field, store):
    first = field(lo)
    flux = level.y_flux(lo - 1, field(lo - 1), first)

    def row(y, carry):
        u, flux_low = carry
        high = field(y + 1)
        image, flux_y = level.apply(y, u, high, flux_low)
        return (high, flux_y), store(y, u, image)

    u, flux_low = rows(lo, n - 1, row, (first, flux))
    image, _ = level.apply(n - 1, u, swap(u), flux_low)
    for ref, at, value in store(n - 1, u, image):
        ref[at] = value


def smooth_down(level, lo, n, r, r1, u1, x, r2):
    def start(y):
        return level.dinv[y] * r[y] * (1.0 / THETA)

    def first(y, u, image):
        rest = r[y] - image
        after = C1U * u + C1R * (level.dinv[y] * rest)
        return [(r1, y, rest), (u1, y, after), (x, y, u + after)]

    sweep(level, lo, n, start, first)
    sweep(level, lo + 1, n, lambda y: u1[y], lambda y, u, image: [(r2, y, r1[y] - image)])


def smooth_up(level, lo, n, e, r2, r3, u, x, finish):
    def first(y, own, image):
        rest = r2[y] - image
        return [(r3, y, rest), (u, y, level.dinv[y] * rest * (1.0 / THETA))]

    sweep(level, lo, n, e, first)

    def second(y, own, image):
        rest = r3[y] - image
        after = C1U * own + C1R * (level.dinv[y] * rest)
        return finish(y, (x[y] + e(y)) + (own + after))

    sweep(level, lo + 1, n, lambda y: u[y], second)


def down(fine, mid, r, x, r2, xm, r2m, r1, u1, b1, r1m, u1m):
    smooth_down(fine, 3, H, r, r1, u1, x, r2)
    rows(2, H // 2, lambda y, c: (c, [(b1, y, sum_x(sum_z(r2[2 * y] + r2[2 * y + 1], 1), 1))]), 0)
    smooth_down(mid, 3, H // 2, b1, r1m, u1m, xm, r2m)
    return [sum_x(sum_z(r2m[2 * k + 6] + r2m[2 * k + 7], 2), 2) for k in range(2)]


def to_line(folded):
    to = lax.broadcasted_iota(jnp.int32, (128, 256), 1)
    spread = to % 16 * 4 + to // 128 * NX == lax.broadcasted_iota(jnp.int32, (128, 256), 0)
    spread = jnp.where(spread, 1.0, 0.0)
    at = lax.broadcasted_iota(jnp.int32, (NB, 256), 1) // 16
    y = at // 4
    z = lax.broadcasted_iota(jnp.int32, (NB, 256), 0) == M + 4 * (at % 4)
    line = jnp.zeros((1, 256), F32)
    for k in range(2):
        wide = jnp.dot(folded[k], spread, precision=lax.Precision.HIGHEST, preferred_element_type=F32)
        line = line + jnp.sum(jnp.where(((y == k) | (y == 3 - k)) & z, wide, 0.0), axis=0, keepdims=True)
    return line


def levels_of(coef, coef1):
    return Level(*(coef.at[k] for k in range(5)), 1), Level(*(coef1.at[k] for k in range(5)), 2)


def cycle_of(cycle, cycle1):
    return cycle.at[0], cycle.at[1], cycle1.at[0], cycle1.at[1]


def setup_kernel(pos, fields, coef, coef1, rq, cycle, cycle1, kept, pay, *scratch):
    it, src, rea, r = fields.at[0], fields.at[1], fields.at[2], rq.at[0]
    fine, mid = levels_of(coef, coef1)
    wx, wy, wz, c, dinv = fine.wx, fine.wy, fine.wz, fine.c, fine.dinv
    wx1, wy1, wz1, c1, dinv1 = mid.wx, mid.wy, mid.wz, mid.c, mid.dinv
    for k in range(3):
        kept[k] = fields[k, M - 1 : H]
    gy, zb = pos[0], pos[1]
    zg = ziota() + (zb * B - M)
    lane = xiota()
    xg = lane % NX
    inside_z = (zg >= 0) & (zg < NZ)
    at_edge = ((lane < NX) & (gy == 0)) | ((lane >= NX) & (gy == NGY - 1))

    def weight(g):
        square = g * g
        root = jnp.sqrt(1.0 + square)
        return (1.0 + 2.0 * square) / root, g * root

    def row(y, carry, high=None):
        here, flow_low, wy_low, wym_low = carry
        high = it[y + 1] if high is None else high
        w_x, p_x = weight(jnp.where(xg == NX - 1, 0.0, up_x(here)) - here)
        w_0, p_0 = weight(here)
        w_y, p_y = weight(high - here)
        w_z, p_z = weight(up_z(here) - here)
        inside = inside_z & jnp.logical_not(at_edge & (y < M))
        low_x = jnp.where(xg == 0, p_0, dn_x(p_x))
        rest = src[y] - rea[y] * here + ((p_x - low_x) + (p_y - flow_low) + (p_z - dn_z(p_z)))
        outer = rea[y] + jnp.where(xg == 0, w_0, 0.0) + jnp.where(xg == NX - 1, w_x, 0.0)
        outer = outer + jnp.where(zg == 0, dn_z(w_z), 0.0) + jnp.where(zg == NZ - 1, w_z, 0.0)
        outer = outer + jnp.where(at_edge & (y == M), wy_low, 0.0)
        outer = jnp.where(inside, outer, 0.0)
        m_x = jnp.where(inside & (xg < NX - 1), w_x, 0.0)
        m_y = jnp.where(inside, w_y, 0.0)
        m_z = jnp.where(inside & (zg < NZ - 1), w_z, 0.0)
        diagonal = outer + m_x + dn_x(m_x) + m_y + wym_low + m_z + dn_z(m_z)
        good = diagonal > 0.0
        inverse = jnp.where(good, 1.0 / jnp.where(good, diagonal, 1.0), 0.0)
        stores = [(r, y, jnp.where(inside, rest, 0.0)), (wx, y, m_x), (wy, y, m_y), (wz, y, m_z), (c, y, outer)]
        return (high, p_y, w_y, m_y), stores + [(dinv, y, inverse)]

    zero = jnp.zeros((NB, 128), F32)
    carry = rows(1, H - 1, row, (it[1], zero, zero, zero), 2)
    for ref, at, value in row(H - 1, carry, swap(carry[0]))[1]:
        ref[at] = value
    for ref in (wx, wy, wz, c, dinv, r):
        ref[0] = zero

    def row1(y, low):
        a, b = 2 * y, 2 * y + 1
        m_x = sum_z(odd_x(wx[a] + wx[b], 1), 1)
        m_y = sum_x(sum_z(wy[b], 1), 1)
        m_z = sum_x(odd_z(wz[a] + wz[b], 1), 1)
        m_c = sum_x(sum_z(c[a] + c[b], 1), 1)
        diagonal = m_c + m_x + dn_x(m_x, 2) + m_y + low + m_z + dn_z(m_z, 2)
        good = diagonal > 0.0
        inverse = jnp.where(good, 1.0 / jnp.where(good, diagonal, 1.0), 0.0)
        return m_y, [(wx1, y, m_x), (wy1, y, m_y), (wz1, y, m_z), (c1, y, m_c), (dinv1, y, inverse)]

    rows(0, H // 2, row1, zero, 2)

    pay[:, 0:256] = to_line(down(fine, mid, r, *cycle_of(cycle, cycle1), *scratch))
    pair = [(2 * k + 6, 2 * k + 7) for k in range(2)]
    pay[:, 256:512] = to_line([sum_z(odd_x(wx1[a] + wx1[b], 2), 2) for a, b in pair])
    half = lane < NX
    pay[:, 512:768] = to_line([sum_x(sum_z(jnp.where(half, wy1[b], wy1[b - 2]), 2), 2) for a, b in pair])
    pay[:, 768:1024] = to_line([sum_x(odd_z(wz1[a] + wz1[b], 2), 2) for a, b in pair])
    pay[:, 1024:1280] = to_line([sum_x(sum_z(c1[a] + c1[b], 2), 2) for a, b in pair])


def lane_ids():
    return lax.broadcasted_iota(jnp.int32, (16, NDEV), 1)


def next_z(v):
    lanes = lane_ids()
    ahead = jnp.where(lanes < 224, roll(v, -32, 1), roll(v, -1, 1))
    back = jnp.where(lanes >= 32, roll(v, 32, 1), roll(v, -1, 1))
    return jnp.where(lanes % 2 == 0, ahead, back)


def prev_z(v):
    lanes = lane_ids()
    back = jnp.where(lanes >= 32, roll(v, 32, 1), jnp.where(lanes == 0, 0.0, roll(v, 1, 1)))
    ahead = jnp.where(lanes < 224, roll(v, -32, 1), roll(v, 1, 1))
    return jnp.where(lanes % 2 == 0, back, ahead)


def next_y(v):
    return roll(v, -4, 1)


def prev_y(v):
    return roll(v, 4, 1)


def coarse_apply(n, s, u, wx, wy, wz, c):
    flux_y = [[None] * n for _ in range(n)]
    flux_z = [[None] * n for _ in range(n)]
    for y in range(n):
        for z in range(n):
            here = u[y][z]
            high_y = u[y + 1][z] if y + 1 < n else next_y(u[0][z])
            high_z = u[y][z + 1] if z + 1 < n else next_z(u[y][0])
            flux_y[y][z] = wy(y, z) * (high_y - here)
            flux_z[y][z] = wz(y, z) * (high_z - here)
    image = [[None] * n for _ in range(n)]
    for y in range(n):
        for z in range(n):
            here = u[y][z]
            flux_x = wx(y, z) * (roll(here, -s, 0) - here)
            low_y = flux_y[y - 1][z] if y else prev_y(flux_y[n - 1][z])
            low_z = flux_z[y][z - 1] if z else prev_z(flux_z[y][n - 1])
            image[y][z] = c(y, z) * here - (
                (flux_x - roll(flux_x, s, 0)) + (flux_y[y][z] - low_y) + (flux_z[y][z] - low_z)
            )
    return image


def planes(n, f):
    return [[f(y, z) for z in range(n)] for y in range(n)]


def pair_x(v):
    iota = lax.broadcasted_iota(jnp.int32, (16, NDEV), 0)
    return v + jnp.where(even(iota, 1), roll(v, -1, 0), roll(v, 1, 0))


def odd_pair_x(v):
    iota = lax.broadcasted_iota(jnp.int32, (16, NDEV), 0)
    return jnp.where(even(iota, 1), roll(v, -1, 0), v)


def inverse_diagonal(n, s, wx, wy, wz, c):
    def one(y, z):
        low_y = wy(y - 1, z) if y else prev_y(wy(n - 1, z))
        low_z = wz(y, z - 1) if z else prev_z(wz(y, n - 1))
        diagonal = c(y, z) + wx(y, z) + roll(wx(y, z), s, 0) + wy(y, z) + low_y + wz(y, z) + low_z
        return 1.0 / diagonal

    return planes(n, one)


def coefficients(got, k2, k3):
    for f in range(4):
        k2[f] = got[:, 256 * (f + 1) : 256 * (f + 2)].T

    def field(f):
        return lambda y, z: k2[f, pl.ds((y * 4 + z) * 16, 16), :]

    wx, wy, wz, c = (field(f) for f in range(4))
    inverse = inverse_diagonal(4, 1, wx, wy, wz, c)
    for y in range(4):
        for z in range(4):
            k2[4, pl.ds((y * 4 + z) * 16, 16), :] = inverse[y][z]
    for y in range(2):
        for z in range(2):
            a, b, e, f = (2 * y, 2 * z), (2 * y, 2 * z + 1), (2 * y + 1, 2 * z), (2 * y + 1, 2 * z + 1)
            at = pl.ds((y * 2 + z) * 16, 16)
            k3[0, at, :] = odd_pair_x((wx(*a) + wx(*b)) + (wx(*e) + wx(*f)))
            k3[1, at, :] = pair_x(wy(*e) + wy(*f))
            k3[2, at, :] = pair_x(wz(*b) + wz(*f))
            k3[3, at, :] = pair_x((c(*a) + c(*b)) + (c(*e) + c(*f)))

    def field3(f):
        return lambda y, z: k3[f, pl.ds((y * 2 + z) * 16, 16), :]

    inverse = inverse_diagonal(2, 2, *(field3(f) for f in range(4)))
    for y in range(2):
        for z in range(2):
            k3[4, pl.ds((y * 2 + z) * 16, 16), :] = inverse[y][z]


def combine(n, f, *lists):
    return planes(n, lambda y, z: f(*(a[y][z] for a in lists)))


def coarse_solve(k2, k3, b2t):
    def field(ref, n, f):
        return lambda y, z: ref[f, pl.ds((y * n + z) * 16, 16), :]

    a2 = tuple(field(k2, 4, f) for f in range(4))
    dinv = planes(4, field(k2, 4, 4))
    a3 = tuple(field(k3, 2, f) for f in range(4))
    dinv3 = planes(2, field(k3, 2, 4))
    r = planes(4, lambda y, z: b2t[pl.ds((y * 4 + z) * 16, 16), :])
    u = combine(4, lambda d, b: d * b / THETA, dinv, r)
    r = combine(4, lambda a, b: a - b, r, coarse_apply(4, 1, u, *a2))
    u1 = combine(4, lambda u, d, r: C1U * u + C1R * (d * r), u, dinv, r)
    x = combine(4, lambda a, b: a + b, u, u1)
    r = combine(4, lambda a, b: a - b, r, coarse_apply(4, 1, u1, *a2))
    r3 = planes(
        2,
        lambda y, z: pair_x(
            (r[2 * y][2 * z] + r[2 * y][2 * z + 1]) + (r[2 * y + 1][2 * z] + r[2 * y + 1][2 * z + 1])
        ),
    )
    u = combine(2, lambda d, b: d * b / THETA, dinv3, r3)
    x3 = u
    for cu, cr in ((C1U, C1R), (C2U, C2R)):
        r3 = combine(2, lambda a, b: a - b, r3, coarse_apply(2, 2, u, *a3))
        u = combine(2, lambda u, d, r: cu * u + cr * (d * r), u, dinv3, r3)
        x3 = combine(2, lambda a, b: a + b, x3, u)
    e = planes(4, lambda y, z: x3[y // 2][z // 2])
    x = combine(4, lambda a, b: a + b, x, e)
    r = combine(4, lambda a, b: a - b, r, coarse_apply(4, 1, e, *a2))
    u = combine(4, lambda d, b: d * b / THETA, dinv, r)
    r = combine(4, lambda a, b: a - b, r, coarse_apply(4, 1, u, *a2))
    u1 = combine(4, lambda u, d, r: C1U * u + C1R * (d * r), u, dinv, r)
    return combine(4, lambda x, a, b: x + (a + b), x, u, u1)


def place_coarse(pos, x2, e2):
    gy, zb = pos[0], pos[1]
    lanes = lane_ids()
    picked = {}
    for dy in (-1, 0, 1):
        for dz in (-1, 0, 1):
            at_y = jnp.clip(gy + dy, 0, NGY - 1)
            at_z = jnp.clip(zb + dz, 0, NZB - 1)
            gz, k = at_z // NGX, at_z % NGX
            picked[dy, dz] = lanes == (jnp.where(gz % 2 == 0, k, NGX - 1 - k) * NGY + at_y) * NGZ + gz
    lane = lax.broadcasted_iota(jnp.int32, (16, 128), 1)
    spread = lane % NX // 4 == lax.broadcasted_iota(jnp.int32, (16, 128), 0)
    rows_z = ziota() // 4

    def column(y2, z2):
        mine = picked[(y2 - 3) // 4, (z2 - 3) // 4]
        return jnp.sum(jnp.where(mine, x2[(y2 - 3) % 4][(z2 - 3) % 4], 0.0), axis=1, keepdims=True)

    for k in range(1, 5):
        plane = jnp.zeros((NB, 128), F32)
        for z2 in range(1, 9):
            both = jnp.where(lane < NX, column(k, z2), column(9 - k, z2))
            line = jnp.sum(jnp.where(spread, both, 0.0), axis=0, keepdims=True)
            plane = jnp.where(rows_z == z2, line, plane)
        e2[k] = plane


def up(pos, k2, k3, b2t, fine, mid, x, r2, xm, r2m, out, e2, r3, u, x1, r3m, um):
    place_coarse(pos, coarse_solve(k2, k3, b2t), e2)
    smooth_up(mid, 4, H // 2, lambda y: e2[y // 2], r2m, r3m, um, xm, lambda y, value: [(x1, y, value)])

    def result(y, value):
        return [(out, y - M, dn_z(value, -M)[:B])]

    smooth_up(fine, M - 1, H, lambda y: x1[y // 2], r2, r3, u, x, result)


def first_kernel(pos, got, coef, coef1, cycle, cycle1, out, k2, k3, b2t, *scratch):
    fine, mid = levels_of(coef, coef1)
    coefficients(got, k2, k3)
    b2t[...] = got[:, 0:256].T
    up(pos, k2, k3, b2t, fine, mid, *cycle_of(cycle, cycle1), out, *scratch)


def image_kernel(last, centre, *refs):
    if last:
        before, after, edge, rq, coef, coef1, z_kept, w, pay, z, *scratch = refs
        z[M - 1] = edge[0]
        blank = jnp.zeros((8, 128), F32)
        for k in range(8):
            z[M + k] = roll(jnp.concatenate([before[k], centre[k], after[k], blank], axis=0), 4, 0)
    else:
        low, high, rq, coef, coef1, z_kept, w, pay, z, *scratch = refs
        half = xiota() < NX
        z[M:H] = centre[...]
        for k in range(4):
            z[k] = jnp.where(half, low[k + 4], high[k + 4])
        for k in range(4, M):
            z[k] = swap(jnp.where(half, high[11 - k], low[11 - k]))
    fine, mid = levels_of(coef, coef1)
    z_kept[...] = z[M - 1 : H]
    sweep(fine, M if last else 2, H, lambda y: z[y], lambda y, u, image: [(w, y, image)])
    own = (ziota() >= M) & (ziota() < M + B)

    def row(y, carry):
        a, b = carry
        here = jnp.where(own, z[y], 0.0)
        return (a + rq[0, y] * here, b + here * w[y]), []

    zero = jnp.zeros((NB, 128), F32)
    a, b = rows(M, H, row, (zero, zero))
    lane = lax.broadcasted_iota(jnp.int32, (1, 128), 1)
    pay[:, 0:128] = jnp.where(lane == 0, jnp.sum(a), jnp.where(lane == 1, jnp.sum(b), 0.0))
    if not last:
        cycle, cycle1 = scratch[:2]
        pay[:, 128:384] = to_line(down(fine, mid, w, *cycle_of(cycle, cycle1), *scratch[2:]))


def step_sizes(got, old, scal, first):
    total = jnp.sum(got[:, 0:128], axis=0, keepdims=True)
    lane = lax.broadcasted_iota(jnp.int32, (1, 128), 1)

    def pick(v, k):
        return jnp.sum(jnp.where(lane == k, v, 0.0))

    one = jnp.ones((1, 128), F32)
    gamma, delta = pick(total, 0) * one, pick(total, 1) * one
    if first:
        beta = jnp.zeros((1, 128), F32)
        alpha = gamma / delta
    else:
        was = old[0:1]
        gamma_old, alpha_old = pick(was, 0) * one, pick(was, 1) * one
        beta = gamma / gamma_old
        alpha = gamma / (delta - beta * gamma / alpha_old)
    if scal is not None:
        scal[...] = jnp.broadcast_to(jnp.where(lane == 0, gamma, alpha), (8, 128))
    return alpha, beta


def step_kernel(first, again, pos, got, old, z, w, b2_was, rq, *refs):
    pd, refs = (None, refs) if first else (refs[0], refs[1:])
    coef, coef1, k2, k3, scal, rq_o, pd_o, out, b2, *refs = refs
    (pay, refs) = (refs[0], refs[1:]) if first else (None, refs)
    cycle, cycle1, e2, *scratch = refs
    b2q, b2t = b2.at[0], b2.at[1]
    fine, mid = levels_of(coef, coef1)
    alpha, beta = step_sizes(got, old, scal, first)

    def row(y, carry):
        q = w[y] if first else w[y] + beta * rq[1, y]
        return carry, [(rq_o, (1, y), q), (rq_o, (0, y), rq[0, y] - alpha * q)]

    rows(2, H, row, 0)

    def row_d(y, carry):
        p = z[y] if first else z[y] + beta * pd[0, y]
        return carry, [(pd_o, (0, y), p), (pd_o, (1, y), alpha * p if first else pd[1, y] + alpha * p)]

    rows(0, 9, row_d, 0)
    x, r2, xm, r2m = cycle_of(cycle, cycle1)
    folded = down(fine, mid, rq_o.at[0], x, r2, xm, r2m, *scratch)
    if first:
        pay[...] = to_line(folded)
    alpha2 = jnp.concatenate([alpha, alpha], axis=1)
    if first:
        b2q[...] = got[:, 128:384].T
        b2t[...] = b2_was[...] - alpha2 * b2q[...]
    else:
        beta2 = jnp.concatenate([beta, beta], axis=1)
        b2q[...] = got[:, 128:384].T + beta2 * b2_was[0]
        b2t[...] = (got[:, 384:640].T if again else b2_was[1]) - alpha2 * b2q[...]
    up(pos, k2, k3, b2t, fine, mid, x, r2, xm, r2m, out, e2, *scratch)


def finish_kernel(pos, steps, got, old, z, w, rq, pd, kept, d_out, r_out, layers, d_all):
    alpha, beta = step_sizes(got, old, None, False)
    gy, zb = pos[0], pos[1]
    rows(0, 9, lambda y, c: (c, [(d_all, y, pd[1, y] + alpha * (z[y] + beta * pd[0, y]))]), 0)

    def row(y, carry):
        r = rq[0, y + M] - alpha * (w[y + M] + beta * rq[1, y + M])
        return carry, [(r_out, y, dn_z(r, -M)[:B]), (d_out, y, dn_z(d_all[y + 1], -M)[:B])]

    rows(0, 8, row, 0)
    zi = ziota()
    own = (zi >= M) & (zi < M + B)
    own_z = own | ((zi == M + B) & (zb == NZB - 1))
    lane = xiota()
    x = lane % NX
    edge = own & ((lane < NX) | (gy == NGY - 1))

    def energy(g):
        square = 1.0 + g * g
        return (square * jnp.sqrt(square) - 1.0) / 3.0

    zero = jnp.zeros((NB, 128), F32)
    for k in range(TRIALS):
        step = steps[k]

        def trial(y):
            return kept[0, y] + step * d_all[y]

        def part(y, low, acc, outer):
            v = trial(y)
            acc = acc + jnp.where(outer, energy(v - low), 0.0) + jnp.where(own_z, energy(v - dn_z(v)), 0.0)
            inner = energy(v - jnp.where(x == 0, 0.0, dn_x(v))) + jnp.where(x == NX - 1, energy(v), 0.0)
            inner = inner + (0.5 * kept[2, y] * v * v - kept[1, y] * v)
            return v, acc + jnp.where(own, inner, 0.0)

        def row(y, carry):
            return part(y, *carry, own), []

        v, acc = rows(2, 9, row, part(1, trial(0), zero, edge), 2)
        acc = acc + jnp.where(own & (lane < NX), energy(swap(v) - v), 0.0)
        total = jnp.broadcast_to(jnp.sum(acc, axis=0, keepdims=True), (8, 128))
        layers[k] = total + swap(total)


VM = pl.BlockSpec(memory_space=pltpu.VMEM)
SM = pl.BlockSpec(memory_space=pltpu.SMEM)


def call(kernel, n_scalar, outs, scratch, name, aliases={}):
    def run(*args):
        return pl.pallas_call(
            kernel,
            in_specs=[SM] * n_scalar + [VM] * (len(args) - n_scalar),
            out_specs=[VM] * len(outs),
            out_shape=[jax.ShapeDtypeStruct(s, F32) for s in outs],
            scratch_shapes=[pltpu.VMEM(s, F32) for s in scratch],
            input_output_aliases=aliases,
            compiler_params=pltpu.CompilerParams(vmem_limit_bytes=LIMIT),
            interpret=INTERPRET,
            name=name,
        )(*args)

    return run


FINE = (H, NB, 128)
MID = (H // 2, NB, 128)
KEPT = (9, NB, 128)
SCRATCH = [FINE, FINE, MID, MID, MID]
CYCLE = [(2, *FINE), (2, *MID)]
COEFS = [(5, *FINE), (5, *MID)]
COARSE = (H // 4, NB, 128)
PLANES = (256, NDEV)


def device_of(gy, zb):
    gz, k = zb // NGX, zb % NGX
    return ((k if gz % 2 == 0 else NGX - 1 - k) * NGY + gy) * NGZ + gz


def shift_pairs(dy, dz):
    pairs = []
    for gy in range(NGY):
        for zb in range(NZB):
            ty, tz = gy + dy, zb + dz
            if 0 <= ty < NGY and 0 <= tz < NZB:
                pairs.append((device_of(gy, zb), device_of(ty, tz)))
    return pairs


def exchange_z(own):
    low = lax.ppermute(own, ALL, shift_pairs(0, 1))
    high = lax.ppermute(own, ALL, shift_pairs(0, -1))
    return jnp.concatenate([low[..., B - M :, :], own, high[..., :M, :]], axis=-2)


def exchange_y(own):
    return lax.ppermute(own, ALL, shift_pairs(1, 0)), lax.ppermute(own, ALL, shift_pairs(-1, 0))


def exchange_faces(own):
    low = lax.ppermute(own[:, 8:], ALL, shift_pairs(0, 1))
    high = lax.ppermute(own[:, :8], ALL, shift_pairs(0, -1))
    below, above = exchange_y(own[:1])
    edge = jnp.concatenate([below[..., NX:], above[..., :NX]], axis=-1)
    return own, low, high, jnp.pad(edge, ((0, 0), (M, M), (0, 0)))


def unfold_margin(own, low, high):
    outer = jnp.concatenate([low[..., 4:, :, :NX], high[..., 4:, :, NX:]], axis=-1)
    inner = jnp.concatenate([low[..., ::-1, :, NX:], high[..., ::-1, :, :NX]], axis=-1)
    return jnp.concatenate([outer, inner, own], axis=-3)


def to_everyone(x):
    copies = jnp.broadcast_to(x, (NDEV, *x.shape))
    return lax.all_to_all(copies, ALL, split_axis=0, concat_axis=0, tiled=True)


def to_everyone_by_axes(line):
    n = line.shape[1]
    copies = jnp.broadcast_to(line, (NGX, 1, n))
    got = lax.all_to_all(copies, "gx", split_axis=0, concat_axis=0, tiled=True)
    copies = jnp.broadcast_to(got.reshape(NGX, n), (NDEV // NGX, NGX, n))
    got = lax.all_to_all(copies, (*GY, "gz"), split_axis=0, concat_axis=0, tiled=True)
    return got.transpose(1, 0, 2).reshape(NDEV, n)


def on_device(iterate, source, reaction, trial_powers):
    gx = lax.axis_index("gx")
    gy = lax.axis_index(GY)
    gz = lax.axis_index("gz")
    down_gx = gz % 2 == 1
    zb = gz * NGX + jnp.where(down_gx, NGX - 1 - gx, gx)
    pos = jnp.stack([gy, zb]).astype(jnp.int32)
    pos, steps = lax.optimization_barrier((pos, jnp.exp2(-trial_powers.astype(F32))))
    fields = jnp.stack([iterate, source, reaction])
    fields = fields.reshape(3, 8, 16, 8, 16).transpose(3, 1, 0, 2, 4).reshape(8, 8, 3, 256)
    fields = jnp.where(down_gx, fields[::-1], fields)
    fields = lax.all_to_all(fields, "gx", split_axis=0, concat_axis=0, tiled=True)
    fields = fields.reshape(NX, 3 * 256).T.reshape(3, 16, 16, NX)
    fields = jnp.concatenate([fields[:, :8], fields[:, :7:-1]], axis=-1)
    fields = exchange_z(fields)
    fields = unfold_margin(fields, *exchange_y(fields))
    coef, coef1, rq, cycle, cycle1, kept, pay = call(
        setup_kernel, 1, COEFS + [(2, *FINE)] + CYCLE + [(3, *KEPT), (1, 1280)], SCRATCH, "setup"
    )(pos, fields)
    own = (8, B, 128)
    z, k2, k3, b2 = call(
        first_kernel, 1, [own, (5, 256, NDEV), (5, 64, NDEV), PLANES], [COARSE] + SCRATCH, "first"
    )(pos, to_everyone_by_axes(pay), coef, coef1, cycle, cycle1)
    scal = jnp.zeros((8, 128), F32)
    pd = None
    for i in range(ITERS):
        first, last = i == 0, i + 1 == ITERS
        if last:
            around = exchange_faces(z)
        else:
            centre = exchange_z(z)
            around = (centre, *exchange_y(centre))
        z, w, line = call(
            functools.partial(image_kernel, last), 0, [KEPT, FINE, (1, 128 if last else 384)],
            [FINE] + ([] if last else CYCLE + SCRATCH), "image",
        )(*around, rq, coef, coef1)
        if last:
            break
        if i == 1:
            line = jnp.concatenate([line, pay], axis=1)
        else:
            line = jnp.pad(line, ((0, 0), (0, 128)))
        got = to_everyone(line)[:, 0]
        state = (rq,) if first else (rq, pd)
        scal, rq, pd, z, b2, *rest = call(
            functools.partial(step_kernel, first, i == 1), 1,
            [(8, 128), (2, *FINE), (2, *KEPT), own, (2, *PLANES)] + ([(1, 256)] if first else []),
            CYCLE + [COARSE] + SCRATCH, "step", {6: 1} if first else {6: 1, 7: 2},
        )(pos, got, scal, z, w, b2, *state, coef, coef1, k2, k3)
        if first:
            (pay,) = rest
    dots = to_everyone(line)[:, 0]
    d_own, r_own, layers = call(finish_kernel, 2, [own, own, (TRIALS, 8, 128)], [KEPT], "finish")(
        pos, steps, dots, scal, z, w, rq, pd, kept
    )
    both = jnp.stack([d_own, r_own])
    both = jnp.concatenate([both[..., :NX], both[:, ::-1, :, NX:]], axis=1).reshape(512, NX).T
    copies = jnp.broadcast_to(layers[:, 0, :NX].reshape(1, 256), (NDEV, 1, 256))
    copies, both = lax.optimization_barrier((copies, both.reshape(8, 8, 512)))
    layers = lax.all_to_all(copies, ALL, split_axis=0, concat_axis=0, tiled=True)
    both = lax.all_to_all(both, "gx", split_axis=0, concat_axis=0, tiled=True)
    both = jnp.where(down_gx, both[::-1], both)
    both = both.reshape(8, 8, 2, 16, 16).transpose(2, 1, 3, 0, 4).reshape(2, 8, 16, 128)
    layers = layers.sum(axis=0).reshape(TRIALS, NX) / (NY * NZ)
    energies = jnp.sum(layers, axis=1) / NX
    mine = lax.dynamic_slice_in_dim(layers, gx * 8, 8, axis=1)
    return both[0], both[1], mine, energies


def solution(mesh):
    torus = Mesh(mesh.devices.reshape(8, 4, 2, 4), ALL)
    placed = P("gx", GY, "gz")
    return jax.shard_map(
        on_device,
        mesh=torus,
        in_specs=(placed, placed, placed, P()),
        out_specs=(placed, placed, P(None, "gx"), P()),
        check_vma=False,
    )
```

```python
import functools

import jax
import jax.numpy as jnp
from jax import lax
from jax.experimental import pallas as pl
from jax.experimental.pallas import tpu as pltpu
from jax.sharding import Mesh
from jax.sharding import PartitionSpec as P

ITERS = 4
TRIALS = 4
ALL = ("gx", "gy_0", "gy_1", "gz")
GY = ("gy_0", "gy_1")
NGX, NGY, NGZ = 8, 8, 4
NDEV = 256
NZB = 32
NX, NY, NZ = 64, 128, 512
M = 12
B = 16
NB = 40
F32 = jnp.float32
INTERPRET = False
H = 20
LIMIT = 26 * 1024 * 1024

THETA = 1.15
DELTA = 0.85
SIGMA = THETA / DELTA
RHO0 = 1.0 / SIGMA
RHO1 = 1.0 / (2.0 * SIGMA - RHO0)
RHO2 = 1.0 / (2.0 * SIGMA - RHO1)
C1U = RHO1 * RHO0
C1R = 2.0 * RHO1 / DELTA
C2U = RHO2 * RHO1
C2R = 2.0 * RHO2 / DELTA


def roll(v, shift, axis):
    return pltpu.roll(v, shift % v.shape[axis], axis)


def up_z(v, s=1):
    return roll(v, -s, 0)


def dn_z(v, s=1):
    return roll(v, s, 0)


def up_x(v, s=1):
    return roll(v, -s, 1)


def dn_x(v, s=1):
    return roll(v, s, 1)


def swap(v):
    return roll(v, NX, 1)


def ziota():
    return lax.broadcasted_iota(jnp.int32, (NB, 128), 0)


def xiota():
    return lax.broadcasted_iota(jnp.int32, (NB, 128), 1)


def even(iota, s):
    return (iota // s) % 2 == 0


def sum_z(v, s):
    return v + jnp.where(even(ziota(), s), up_z(v, s), dn_z(v, s))


def sum_x(v, s):
    return v + jnp.where(even(xiota(), s), up_x(v, s), dn_x(v, s))


def odd_z(v, s):
    return jnp.where(even(ziota(), s), up_z(v, s), v)


def odd_x(v, s):
    return jnp.where(even(xiota(), s), up_x(v, s), v)


class Level:
    def __init__(self, wx, wy, wz, c, dinv, s):
        self.wx, self.wy, self.wz, self.c, self.dinv, self.s = wx, wy, wz, c, dinv, s

    def y_flux(self, y, low, high):
        return self.wy[y] * (high - low)

    def apply(self, y, u, high, flux_low):
        s = self.s
        flux_y = self.wy[y] * (high - u)
        flux_x = self.wx[y] * (up_x(u, s) - u)
        flux_z = self.wz[y] * (up_z(u, s) - u)
        image = self.c[y] * u - ((flux_x - dn_x(flux_x, s)) + (flux_y - flux_low) + (flux_z - dn_z(flux_z, s)))
        return image, flux_y


def rows(lo, hi, body, carry, step=8):
    def group(start, carry):
        stores = []
        for k in range(step):
            carry, more = body(start + k, carry)
            stores += more
        for ref, at, value in stores:
            ref[at] = value
        return carry

    count = (hi - lo) // step
    if count:
        carry = lax.fori_loop(0, count, lambda i, carry: group(lo + i * step, carry), carry)
    for y in range(lo + count * step, hi):
        carry, stores = body(y, carry)
        for ref, at, value in stores:
            ref[at] = value
    return carry


def sweep(level, lo, n, field, store):
    first = field(lo)
    flux = level.y_flux(lo - 1, field(lo - 1), first)

    def row(y, carry):
        u, flux_low = carry
        high = field(y + 1)
        image, flux_y = level.apply(y, u, high, flux_low)
        return (high, flux_y), store(y, u, image)

    u, flux_low = rows(lo, n - 1, row, (first, flux))
    image, _ = level.apply(n - 1, u, swap(u), flux_low)
    for ref, at, value in store(n - 1, u, image):
        ref[at] = value


def smooth_down(level, lo, n, r, r1, u1, x, r2):
    def start(y):
        return level.dinv[y] * r[y] * (1.0 / THETA)

    def first(y, u, image):
        rest = r[y] - image
        after = C1U * u + C1R * (level.dinv[y] * rest)
        return [(r1, y, rest), (u1, y, after), (x, y, u + after)]

    sweep(level, lo, n, start, first)
    sweep(level, lo + 1, n, lambda y: u1[y], lambda y, u, image: [(r2, y, r1[y] - image)])


def smooth_up(level, lo, n, e, r2, r3, u, x, finish):
    def first(y, own, image):
        rest = r2[y] - image
        return [(r3, y, rest), (u, y, level.dinv[y] * rest * (1.0 / THETA))]

    sweep(level, lo, n, e, first)

    def second(y, own, image):
        rest = r3[y] - image
        after = C1U * own + C1R * (level.dinv[y] * rest)
        return finish(y, (x[y] + e(y)) + (own + after))

    sweep(level, lo + 1, n, lambda y: u[y], second)


def down(fine, mid, r, x, r2, xm, r2m, r1, u1, b1, r1m, u1m):
    smooth_down(fine, 3, H, r, r1, u1, x, r2)
    rows(2, H // 2, lambda y, c: (c, [(b1, y, sum_x(sum_z(r2[2 * y] + r2[2 * y + 1], 1), 1))]), 0)
    smooth_down(mid, 3, H // 2, b1, r1m, u1m, xm, r2m)
    return [sum_x(sum_z(r2m[2 * k + 6] + r2m[2 * k + 7], 2), 2) for k in range(2)]


def to_line(folded):
    to = lax.broadcasted_iota(jnp.int32, (128, 256), 1)
    spread = to % 16 * 4 + to // 128 * NX == lax.broadcasted_iota(jnp.int32, (128, 256), 0)
    spread = jnp.where(spread, 1.0, 0.0)
    at = lax.broadcasted_iota(jnp.int32, (NB, 256), 1) // 16
    y = at // 4
    z = lax.broadcasted_iota(jnp.int32, (NB, 256), 0) == M + 4 * (at % 4)
    line = jnp.zeros((1, 256), F32)
    for k in range(2):
        wide = jnp.dot(folded[k], spread, precision=lax.Precision.HIGHEST, preferred_element_type=F32)
        line = line + jnp.sum(jnp.where(((y == k) | (y == 3 - k)) & z, wide, 0.0), axis=0, keepdims=True)
    return line


def levels_of(coef, coef1):
    return Level(*(coef.at[k] for k in range(5)), 1), Level(*(coef1.at[k] for k in range(5)), 2)


def cycle_of(cycle, cycle1):
    return cycle.at[0], cycle.at[1], cycle1.at[0], cycle1.at[1]


def setup_kernel(pos, fields, coef, coef1, rq, cycle, cycle1, kept, pay, *scratch):
    it, src, rea, r = fields.at[0], fields.at[1], fields.at[2], rq.at[0]
    fine, mid = levels_of(coef, coef1)
    wx, wy, wz, c, dinv = fine.wx, fine.wy, fine.wz, fine.c, fine.dinv
    wx1, wy1, wz1, c1, dinv1 = mid.wx, mid.wy, mid.wz, mid.c, mid.dinv
    for k in range(3):
        kept[k] = fields[k, M - 1 : H]
    gy, zb = pos[0], pos[1]
    zg = ziota() + (zb * B - M)
    lane = xiota()
    xg = lane % NX
    inside_z = (zg >= 0) & (zg < NZ)
    at_edge = ((lane < NX) & (gy == 0)) | ((lane >= NX) & (gy == NGY - 1))

    def weight(g):
        square = g * g
        root = jnp.sqrt(1.0 + square)
        return (1.0 + 2.0 * square) / root, g * root

    def row(y, carry, high=None):
        here, flow_low, wy_low, wym_low = carry
        high = it[y + 1] if high is None else high
        w_x, p_x = weight(jnp.where(xg == NX - 1, 0.0, up_x(here)) - here)
        w_0, p_0 = weight(here)
        w_y, p_y = weight(high - here)
        w_z, p_z = weight(up_z(here) - here)
        inside = inside_z & jnp.logical_not(at_edge & (y < M))
        low_x = jnp.where(xg == 0, p_0, dn_x(p_x))
        rest = src[y] - rea[y] * here + ((p_x - low_x) + (p_y - flow_low) + (p_z - dn_z(p_z)))
        outer = rea[y] + jnp.where(xg == 0, w_0, 0.0) + jnp.where(xg == NX - 1, w_x, 0.0)
        outer = outer + jnp.where(zg == 0, dn_z(w_z), 0.0) + jnp.where(zg == NZ - 1, w_z, 0.0)
        outer = outer + jnp.where(at_edge & (y == M), wy_low, 0.0)
        outer = jnp.where(inside, outer, 0.0)
        m_x = jnp.where(inside & (xg < NX - 1), w_x, 0.0)
        m_y = jnp.where(inside, w_y, 0.0)
        m_z = jnp.where(inside & (zg < NZ - 1), w_z, 0.0)
        diagonal = outer + m_x + dn_x(m_x) + m_y + wym_low + m_z + dn_z(m_z)
        good = diagonal > 0.0
        inverse = jnp.where(good, 1.0 / jnp.where(good, diagonal, 1.0), 0.0)
        stores = [(r, y, jnp.where(inside, rest, 0.0)), (wx, y, m_x), (wy, y, m_y), (wz, y, m_z), (c, y, outer)]
        return (high, p_y, w_y, m_y), stores + [(dinv, y, inverse)]

    zero = jnp.zeros((NB, 128), F32)
    carry = rows(1, H - 1, row, (it[1], zero, zero, zero), 2)
    for ref, at, value in row(H - 1, carry, swap(carry[0]))[1]:
        ref[at] = value
    for ref in (wx, wy, wz, c, dinv, r):
        ref[0] = zero

    def row1(y, low):
        a, b = 2 * y, 2 * y + 1
        m_x = sum_z(odd_x(wx[a] + wx[b], 1), 1)
        m_y = sum_x(sum_z(wy[b], 1), 1)
        m_z = sum_x(odd_z(wz[a] + wz[b], 1), 1)
        m_c = sum_x(sum_z(c[a] + c[b], 1), 1)
        diagonal = m_c + m_x + dn_x(m_x, 2) + m_y + low + m_z + dn_z(m_z, 2)
        good = diagonal > 0.0
        inverse = jnp.where(good, 1.0 / jnp.where(good, diagonal, 1.0), 0.0)
        return m_y, [(wx1, y, m_x), (wy1, y, m_y), (wz1, y, m_z), (c1, y, m_c), (dinv1, y, inverse)]

    rows(0, H // 2, row1, zero, 2)

    pay[:, 0:256] = to_line(down(fine, mid, r, *cycle_of(cycle, cycle1), *scratch))
    pair = [(2 * k + 6, 2 * k + 7) for k in range(2)]
    pay[:, 256:512] = to_line([sum_z(odd_x(wx1[a] + wx1[b], 2), 2) for a, b in pair])
    half = lane < NX
    pay[:, 512:768] = to_line([sum_x(sum_z(jnp.where(half, wy1[b], wy1[b - 2]), 2), 2) for a, b in pair])
    pay[:, 768:1024] = to_line([sum_x(odd_z(wz1[a] + wz1[b], 2), 2) for a, b in pair])
    pay[:, 1024:1280] = to_line([sum_x(sum_z(c1[a] + c1[b], 2), 2) for a, b in pair])


def lane_ids():
    return lax.broadcasted_iota(jnp.int32, (16, NDEV), 1)


def next_z(v):
    lanes = lane_ids()
    ahead = jnp.where(lanes < 224, roll(v, -32, 1), roll(v, -1, 1))
    back = jnp.where(lanes >= 32, roll(v, 32, 1), roll(v, -1, 1))
    return jnp.where(lanes % 2 == 0, ahead, back)


def prev_z(v):
    lanes = lane_ids()
    back = jnp.where(lanes >= 32, roll(v, 32, 1), jnp.where(lanes == 0, 0.0, roll(v, 1, 1)))
    ahead = jnp.where(lanes < 224, roll(v, -32, 1), roll(v, 1, 1))
    return jnp.where(lanes % 2 == 0, back, ahead)


def next_y(v):
    return roll(v, -4, 1)


def prev_y(v):
    return roll(v, 4, 1)


def coarse_apply(n, s, u, wx, wy, wz, c):
    flux_y = [[None] * n for _ in range(n)]
    flux_z = [[None] * n for _ in range(n)]
    for y in range(n):
        for z in range(n):
            here = u[y][z]
            high_y = u[y + 1][z] if y + 1 < n else next_y(u[0][z])
            high_z = u[y][z + 1] if z + 1 < n else next_z(u[y][0])
            flux_y[y][z] = wy(y, z) * (high_y - here)
            flux_z[y][z] = wz(y, z) * (high_z - here)
    image = [[None] * n for _ in range(n)]
    for y in range(n):
        for z in range(n):
            here = u[y][z]
            flux_x = wx(y, z) * (roll(here, -s, 0) - here)
            low_y = flux_y[y - 1][z] if y else prev_y(flux_y[n - 1][z])
            low_z = flux_z[y][z - 1] if z else prev_z(flux_z[y][n - 1])
            image[y][z] = c(y, z) * here - (
                (flux_x - roll(flux_x, s, 0)) + (flux_y[y][z] - low_y) + (flux_z[y][z] - low_z)
            )
    return image


def planes(n, f):
    return [[f(y, z) for z in range(n)] for y in range(n)]


def pair_x(v):
    iota = lax.broadcasted_iota(jnp.int32, (16, NDEV), 0)
    return v + jnp.where(even(iota, 1), roll(v, -1, 0), roll(v, 1, 0))


def odd_pair_x(v):
    iota = lax.broadcasted_iota(jnp.int32, (16, NDEV), 0)
    return jnp.where(even(iota, 1), roll(v, -1, 0), v)


def inverse_diagonal(n, s, wx, wy, wz, c):
    def one(y, z):
        low_y = wy(y - 1, z) if y else prev_y(wy(n - 1, z))
        low_z = wz(y, z - 1) if z else prev_z(wz(y, n - 1))
        diagonal = c(y, z) + wx(y, z) + roll(wx(y, z), s, 0) + wy(y, z) + low_y + wz(y, z) + low_z
        return 1.0 / diagonal

    return planes(n, one)


def coefficients(got, k2, k3):
    for f in range(4):
        k2[f] = got[:, 256 * (f + 1) : 256 * (f + 2)].T

    def field(f):
        return lambda y, z: k2[f, pl.ds((y * 4 + z) * 16, 16), :]

    wx, wy, wz, c = (field(f) for f in range(4))
    inverse = inverse_diagonal(4, 1, wx, wy, wz, c)
    for y in range(4):
        for z in range(4):
            k2[4, pl.ds((y * 4 + z) * 16, 16), :] = inverse[y][z]
    for y in range(2):
        for z in range(2):
            a, b, e, f = (2 * y, 2 * z), (2 * y, 2 * z + 1), (2 * y + 1, 2 * z), (2 * y + 1, 2 * z + 1)
            at = pl.ds((y * 2 + z) * 16, 16)
            k3[0, at, :] = odd_pair_x((wx(*a) + wx(*b)) + (wx(*e) + wx(*f)))
            k3[1, at, :] = pair_x(wy(*e) + wy(*f))
            k3[2, at, :] = pair_x(wz(*b) + wz(*f))
            k3[3, at, :] = pair_x((c(*a) + c(*b)) + (c(*e) + c(*f)))

    def field3(f):
        return lambda y, z: k3[f, pl.ds((y * 2 + z) * 16, 16), :]

    inverse = inverse_diagonal(2, 2, *(field3(f) for f in range(4)))
    for y in range(2):
        for z in range(2):
            k3[4, pl.ds((y * 2 + z) * 16, 16), :] = inverse[y][z]


def combine(n, f, *lists):
    return planes(n, lambda y, z: f(*(a[y][z] for a in lists)))


def coarse_solve(k2, k3, b2t):
    def field(ref, n, f):
        return lambda y, z: ref[f, pl.ds((y * n + z) * 16, 16), :]

    a2 = tuple(field(k2, 4, f) for f in range(4))
    dinv = planes(4, field(k2, 4, 4))
    a3 = tuple(field(k3, 2, f) for f in range(4))
    dinv3 = planes(2, field(k3, 2, 4))
    r = planes(4, lambda y, z: b2t[pl.ds((y * 4 + z) * 16, 16), :])
    u = combine(4, lambda d, b: d * b / THETA, dinv, r)
    r = combine(4, lambda a, b: a - b, r, coarse_apply(4, 1, u, *a2))
    u1 = combine(4, lambda u, d, r: C1U * u + C1R * (d * r), u, dinv, r)
    x = combine(4, lambda a, b: a + b, u, u1)
    r = combine(4, lambda a, b: a - b, r, coarse_apply(4, 1, u1, *a2))
    r3 = planes(
        2,
        lambda y, z: pair_x(
            (r[2 * y][2 * z] + r[2 * y][2 * z + 1]) + (r[2 * y + 1][2 * z] + r[2 * y + 1][2 * z + 1])
        ),
    )
    u = combine(2, lambda d, b: d * b / THETA, dinv3, r3)
    x3 = u
    for cu, cr in ((C1U, C1R), (C2U, C2R)):
        r3 = combine(2, lambda a, b: a - b, r3, coarse_apply(2, 2, u, *a3))
        u = combine(2, lambda u, d, r: cu * u + cr * (d * r), u, dinv3, r3)
        x3 = combine(2, lambda a, b: a + b, x3, u)
    e = planes(4, lambda y, z: x3[y // 2][z // 2])
    x = combine(4, lambda a, b: a + b, x, e)
    r = combine(4, lambda a, b: a - b, r, coarse_apply(4, 1, e, *a2))
    u = combine(4, lambda d, b: d * b / THETA, dinv, r)
    r = combine(4, lambda a, b: a - b, r, coarse_apply(4, 1, u, *a2))
    u1 = combine(4, lambda u, d, r: C1U * u + C1R * (d * r), u, dinv, r)
    return combine(4, lambda x, a, b: x + (a + b), x, u, u1)


def place_coarse(pos, x2, e2):
    gy, zb = pos[0], pos[1]
    lanes = lane_ids()
    picked = {}
    for dy in (-1, 0, 1):
        for dz in (-1, 0, 1):
            at_y = jnp.clip(gy + dy, 0, NGY - 1)
            at_z = jnp.clip(zb + dz, 0, NZB - 1)
            gz, k = at_z // NGX, at_z % NGX
            picked[dy, dz] = lanes == (jnp.where(gz % 2 == 0, k, NGX - 1 - k) * NGY + at_y) * NGZ + gz
    lane = lax.broadcasted_iota(jnp.int32, (16, 128), 1)
    spread = lane % NX // 4 == lax.broadcasted_iota(jnp.int32, (16, 128), 0)
    rows_z = ziota() // 4

    def column(y2, z2):
        mine = picked[(y2 - 3) // 4, (z2 - 3) // 4]
        return jnp.sum(jnp.where(mine, x2[(y2 - 3) % 4][(z2 - 3) % 4], 0.0), axis=1, keepdims=True)

    for k in range(1, 5):
        plane = jnp.zeros((NB, 128), F32)
        for z2 in range(1, 9):
            both = jnp.where(lane < NX, column(k, z2), column(9 - k, z2))
            line = jnp.sum(jnp.where(spread, both, 0.0), axis=0, keepdims=True)
            plane = jnp.where(rows_z == z2, line, plane)
        e2[k] = plane


def up(pos, k2, k3, b2t, fine, mid, x, r2, xm, r2m, out, e2, r3, u, x1, r3m, um):
    place_coarse(pos, coarse_solve(k2, k3, b2t), e2)
    smooth_up(mid, 4, H // 2, lambda y: e2[y // 2], r2m, r3m, um, xm, lambda y, value: [(x1, y, value)])

    def result(y, value):
        return [(out, y - M, dn_z(value, -M)[:B])]

    smooth_up(fine, M - 1, H, lambda y: x1[y // 2], r2, r3, u, x, result)


def first_kernel(pos, got, coef, coef1, cycle, cycle1, out, k2, k3, b2t, *scratch):
    fine, mid = levels_of(coef, coef1)
    coefficients(got, k2, k3)
    b2t[...] = got[:, 0:256].T
    up(pos, k2, k3, b2t, fine, mid, *cycle_of(cycle, cycle1), out, *scratch)


def image_kernel(last, centre, *refs):
    if last:
        before, after, edge, rq, coef, coef1, z_kept, w, pay, z, *scratch = refs
        z[M - 1] = edge[0]
        blank = jnp.zeros((8, 128), F32)
        for k in range(8):
            z[M + k] = roll(jnp.concatenate([before[k], centre[k], after[k], blank], axis=0), 4, 0)
    else:
        low, high, rq, coef, coef1, z_kept, w, pay, z, *scratch = refs
        half = xiota() < NX
        z[M:H] = centre[...]
        for k in range(4):
            z[k] = jnp.where(half, low[k + 4], high[k + 4])
        for k in range(4, M):
            z[k] = swap(jnp.where(half, high[11 - k], low[11 - k]))
    fine, mid = levels_of(coef, coef1)
    z_kept[...] = z[M - 1 : H]
    sweep(fine, M if last else 2, H, lambda y: z[y], lambda y, u, image: [(w, y, image)])
    own = (ziota() >= M) & (ziota() < M + B)

    def row(y, carry):
        a, b = carry
        here = jnp.where(own, z[y], 0.0)
        return (a + rq[0, y] * here, b + here * w[y]), []

    zero = jnp.zeros((NB, 128), F32)
    a, b = rows(M, H, row, (zero, zero))
    lane = lax.broadcasted_iota(jnp.int32, (1, 128), 1)
    pay[:, 0:128] = jnp.where(lane == 0, jnp.sum(a), jnp.where(lane == 1, jnp.sum(b), 0.0))
    if not last:
        cycle, cycle1 = scratch[:2]
        pay[:, 128:384] = to_line(down(fine, mid, w, *cycle_of(cycle, cycle1), *scratch[2:]))


def step_sizes(got, old, scal, first):
    total = jnp.sum(got[:, 0:128], axis=0, keepdims=True)
    lane = lax.broadcasted_iota(jnp.int32, (1, 128), 1)

    def pick(v, k):
        return jnp.sum(jnp.where(lane == k, v, 0.0))

    one = jnp.ones((1, 128), F32)
    gamma, delta = pick(total, 0) * one, pick(total, 1) * one
    if first:
        beta = jnp.zeros((1, 128), F32)
        alpha = gamma / delta
    else:
        was = old[0:1]
        gamma_old, alpha_old = pick(was, 0) * one, pick(was, 1) * one
        beta = gamma / gamma_old
        alpha = gamma / (delta - beta * gamma / alpha_old)
    if scal is not None:
        scal[...] = jnp.broadcast_to(jnp.where(lane == 0, gamma, alpha), (8, 128))
    return alpha, beta


def step_kernel(first, again, pos, got, old, z, w, b2_was, rq, *refs):
    pd, refs = (None, refs) if first else (refs[0], refs[1:])
    coef, coef1, k2, k3, scal, rq_o, pd_o, out, b2, *refs = refs
    (pay, refs) = (refs[0], refs[1:]) if first else (None, refs)
    cycle, cycle1, e2, *scratch = refs
    b2q, b2t = b2.at[0], b2.at[1]
    fine, mid = levels_of(coef, coef1)
    alpha, beta = step_sizes(got, old, scal, first)

    def row(y, carry):
        q = w[y] if first else w[y] + beta * rq[1, y]
        return carry, [(rq_o, (1, y), q), (rq_o, (0, y), rq[0, y] - alpha * q)]

    rows(2, H, row, 0)

    def row_d(y, carry):
        p = z[y] if first else z[y] + beta * pd[0, y]
        return carry, [(pd_o, (0, y), p), (pd_o, (1, y), alpha * p if first else pd[1, y] + alpha * p)]

    rows(0, 9, row_d, 0)
    x, r2, xm, r2m = cycle_of(cycle, cycle1)
    folded = down(fine, mid, rq_o.at[0], x, r2, xm, r2m, *scratch)
    if first:
        pay[...] = to_line(folded)
    alpha2 = jnp.concatenate([alpha, alpha], axis=1)
    if first:
        b2q[...] = got[:, 128:384].T
        b2t[...] = b2_was[...] - alpha2 * b2q[...]
    else:
        beta2 = jnp.concatenate([beta, beta], axis=1)
        b2q[...] = got[:, 128:384].T + beta2 * b2_was[0]
        b2t[...] = (got[:, 384:640].T if again else b2_was[1]) - alpha2 * b2q[...]
    up(pos, k2, k3, b2t, fine, mid, x, r2, xm, r2m, out, e2, *scratch)


def finish_kernel(pos, steps, got, old, z, w, rq, pd, kept, d_out, r_out, layers, d_all):
    alpha, beta = step_sizes(got, old, None, False)
    gy, zb = pos[0], pos[1]
    rows(0, 9, lambda y, c: (c, [(d_all, y, pd[1, y] + alpha * (z[y] + beta * pd[0, y]))]), 0)

    def row(y, carry):
        r = rq[0, y + M] - alpha * (w[y + M] + beta * rq[1, y + M])
        return carry, [(r_out, y, dn_z(r, -M)[:B]), (d_out, y, dn_z(d_all[y + 1], -M)[:B])]

    rows(0, 8, row, 0)
    zi = ziota()
    own = (zi >= M) & (zi < M + B)
    own_z = own | ((zi == M + B) & (zb == NZB - 1))
    lane = xiota()
    x = lane % NX
    edge = own & ((lane < NX) | (gy == NGY - 1))

    def energy(g):
        square = 1.0 + g * g
        return (square * jnp.sqrt(square) - 1.0) / 3.0

    zero = jnp.zeros((NB, 128), F32)
    for k in range(TRIALS):
        step = steps[k]

        def trial(y):
            return kept[0, y] + step * d_all[y]

        def part(y, low, acc, outer):
            v = trial(y)
            acc = acc + jnp.where(outer, energy(v - low), 0.0) + jnp.where(own_z, energy(v - dn_z(v)), 0.0)
            inner = energy(v - jnp.where(x == 0, 0.0, dn_x(v))) + jnp.where(x == NX - 1, energy(v), 0.0)
            inner = inner + (0.5 * kept[2, y] * v * v - kept[1, y] * v)
            return v, acc + jnp.where(own, inner, 0.0)

        def row(y, carry):
            return part(y, *carry, own), []

        v, acc = rows(2, 9, row, part(1, trial(0), zero, edge), 2)
        acc = acc + jnp.where(own & (lane < NX), energy(swap(v) - v), 0.0)
        total = jnp.broadcast_to(jnp.sum(acc, axis=0, keepdims=True), (8, 128))
        layers[k] = total + swap(total)


VM = pl.BlockSpec(memory_space=pltpu.VMEM)
SM = pl.BlockSpec(memory_space=pltpu.SMEM)


def call(kernel, n_scalar, outs, scratch, name, aliases={}):
    def run(*args):
        return pl.pallas_call(
            kernel,
            in_specs=[SM] * n_scalar + [VM] * (len(args) - n_scalar),
            out_specs=[VM] * len(outs),
            out_shape=[jax.ShapeDtypeStruct(s, F32) for s in outs],
            scratch_shapes=[pltpu.VMEM(s, F32) for s in scratch],
            input_output_aliases=aliases,
            compiler_params=pltpu.CompilerParams(vmem_limit_bytes=LIMIT),
            interpret=INTERPRET,
            name=name,
        )(*args)

    return run


FINE = (H, NB, 128)
MID = (H // 2, NB, 128)
KEPT = (9, NB, 128)
SCRATCH = [FINE, FINE, MID, MID, MID]
CYCLE = [(2, *FINE), (2, *MID)]
COEFS = [(5, *FINE), (5, *MID)]
COARSE = (H // 4, NB, 128)
PLANES = (256, NDEV)


def device_of(gy, zb):
    gz, k = zb // NGX, zb % NGX
    return ((k if gz % 2 == 0 else NGX - 1 - k) * NGY + gy) * NGZ + gz


def shift_pairs(dy, dz):
    pairs = []
    for gy in range(NGY):
        for zb in range(NZB):
            ty, tz = gy + dy, zb + dz
            if 0 <= ty < NGY and 0 <= tz < NZB:
                pairs.append((device_of(gy, zb), device_of(ty, tz)))
    return pairs


def exchange_z(own):
    low = lax.ppermute(own, ALL, shift_pairs(0, 1))
    high = lax.ppermute(own, ALL, shift_pairs(0, -1))
    return jnp.concatenate([low[..., B - M :, :], own, high[..., :M, :]], axis=-2)


def exchange_y(own):
    return lax.ppermute(own, ALL, shift_pairs(1, 0)), lax.ppermute(own, ALL, shift_pairs(-1, 0))


def exchange_faces(own):
    low = lax.ppermute(own[:, 8:], ALL, shift_pairs(0, 1))
    high = lax.ppermute(own[:, :8], ALL, shift_pairs(0, -1))
    below, above = exchange_y(own[:1])
    edge = jnp.concatenate([below[..., NX:], above[..., :NX]], axis=-1)
    return own, low, high, jnp.pad(edge, ((0, 0), (M, M), (0, 0)))


def unfold_margin(own, low, high):
    outer = jnp.concatenate([low[..., 4:, :, :NX], high[..., 4:, :, NX:]], axis=-1)
    inner = jnp.concatenate([low[..., ::-1, :, NX:], high[..., ::-1, :, :NX]], axis=-1)
    return jnp.concatenate([outer, inner, own], axis=-3)


def to_everyone(x):
    copies = jnp.broadcast_to(x, (NDEV, *x.shape))
    return lax.all_to_all(copies, ALL, split_axis=0, concat_axis=0, tiled=True)


def to_everyone_by_axes(line):
    n = line.shape[1]
    copies = jnp.broadcast_to(line, (NGX, 1, n))
    got = lax.all_to_all(copies, "gx", split_axis=0, concat_axis=0, tiled=True)
    copies = jnp.broadcast_to(got.reshape(NGX, n), (NDEV // NGX, NGX, n))
    got = lax.all_to_all(copies, (*GY, "gz"), split_axis=0, concat_axis=0, tiled=True)
    return got.transpose(1, 0, 2).reshape(NDEV, n)


def on_device(iterate, source, reaction, trial_powers):
    gx = lax.axis_index("gx")
    gy = lax.axis_index(GY)
    gz = lax.axis_index("gz")
    down_gx = gz % 2 == 1
    zb = gz * NGX + jnp.where(down_gx, NGX - 1 - gx, gx)
    pos = jnp.stack([gy, zb]).astype(jnp.int32)
    pos, steps = lax.optimization_barrier((pos, jnp.exp2(-trial_powers.astype(F32))))
    fields = jnp.stack([iterate, source, reaction])
    fields = fields.reshape(3, 8, 16, 8, 16).transpose(3, 1, 0, 2, 4).reshape(8, 8, 3, 256)
    fields = jnp.where(down_gx, fields[::-1], fields)
    fields = lax.all_to_all(fields, "gx", split_axis=0, concat_axis=0, tiled=True)
    fields = fields.reshape(NX, 3 * 256).T.reshape(3, 16, 16, NX)
    fields = jnp.concatenate([fields[:, :8], fields[:, :7:-1]], axis=-1)
    fields = exchange_z(fields)
    fields = unfold_margin(fields, *exchange_y(fields))
    coef, coef1, rq, cycle, cycle1, kept, pay = call(
        setup_kernel, 1, COEFS + [(2, *FINE)] + CYCLE + [(3, *KEPT), (1, 1280)], SCRATCH, "setup"
    )(pos, fields)
    own = (8, B, 128)
    z, k2, k3, b2 = call(
        first_kernel, 1, [own, (5, 256, NDEV), (5, 64, NDEV), PLANES], [COARSE] + SCRATCH, "first"
    )(pos, to_everyone_by_axes(pay), coef, coef1, cycle, cycle1)
    scal = jnp.zeros((8, 128), F32)
    pd = None
    for i in range(ITERS):
        first, last = i == 0, i + 1 == ITERS
        if last:
            around = exchange_faces(z)
        else:
            centre = exchange_z(z)
            around = (centre, *exchange_y(centre))
        z, w, line = call(
            functools.partial(image_kernel, last), 0, [KEPT, FINE, (1, 128 if last else 384)],
            [FINE] + ([] if last else CYCLE + SCRATCH), "image",
        )(*around, rq, coef, coef1)
        if last:
            break
        if i == 1:
            line = jnp.concatenate([line, pay], axis=1)
        else:
            line = jnp.pad(line, ((0, 0), (0, 128)))
        got = to_everyone(line)[:, 0]
        state = (rq,) if first else (rq, pd)
        scal, rq, pd, z, b2, *rest = call(
            functools.partial(step_kernel, first, i == 1), 1,
            [(8, 128), (2, *FINE), (2, *KEPT), own, (2, *PLANES)] + ([(1, 256)] if first else []),
            CYCLE + [COARSE] + SCRATCH, "step", {6: 1} if first else {6: 1, 7: 2},
        )(pos, got, scal, z, w, b2, *state, coef, coef1, k2, k3)
        if first:
            (pay,) = rest
    dots = to_everyone(line)[:, 0]
    d_own, r_own, layers = call(finish_kernel, 2, [own, own, (TRIALS, 8, 128)], [KEPT], "finish")(
        pos, steps, dots, scal, z, w, rq, pd, kept
    )
    both = jnp.stack([d_own, r_own])
    both = jnp.concatenate([both[..., :NX], both[:, ::-1, :, NX:]], axis=1).reshape(512, NX).T
    copies = jnp.broadcast_to(layers[:, 0, :NX].reshape(1, 256), (NDEV, 1, 256))
    copies, both = lax.optimization_barrier((copies, both.reshape(8, 8, 512)))
    layers = lax.all_to_all(copies, ALL, split_axis=0, concat_axis=0, tiled=True)
    both = lax.all_to_all(both, "gx", split_axis=0, concat_axis=0, tiled=True)
    both = jnp.where(down_gx, both[::-1], both)
    both = both.reshape(8, 8, 2, 16, 16).transpose(2, 1, 3, 0, 4).reshape(2, 8, 16, 128)
    layers = layers.sum(axis=0).reshape(TRIALS, NX) / (NY * NZ)
    energies = jnp.sum(layers, axis=1) / NX
    mine = lax.dynamic_slice_in_dim(layers, gx * 8, 8, axis=1)
    return both[0], both[1], mine, energies


def solution(mesh):
    torus = Mesh(mesh.devices.reshape(8, 4, 2, 4), ALL)
    placed = P("gx", GY, "gz")
    return jax.shard_map(
        on_device,
        mesh=torus,
        in_specs=(placed, placed, placed, P()),
        out_specs=(placed, placed, P(None, "gx"), P()),
        check_vma=False,
    )
```
